128 devices in a mesh: rows: 16 (over x, y), cols: 8 (over z, core).
Axes of the slice: x: 4, y: 4, z: 4, core: 2. Of those that a mesh axis runs over, the one named last changes fastest.
Arguments:
- coarse: float32 [1024, 1024], P('rows', 'cols'), may hold values from -6 to 6
- detail4: float32 [3, 1024, 1024], P(None, 'rows', 'cols'), may hold values from -6 to 6
- detail3: float32 [3, 2048, 2048], P(None, 'rows', 'cols'), may hold values from -6 to 6
- detail2: float32 [3, 4096, 4096], P(None, 'rows', 'cols'), may hold values from -6 to 6
- detail1: float32 [3, 8192, 8192], P(None, 'rows', 'cols'), may hold values from -6 to 6
Outputs:
- image: float32 [16384, 16384], P('rows', 'cols')
The draws below stay inside these ranges and needn't reach their ends.
All inputs are finite; a program needn't handle non-finite values.
Results may differ from the reference program's by a relative error of at most 0.00013.
Values sent between devices are 32-bit elements; how exact they have to be, the bound alone decides.
A program may use at most 128 MiB of HBM per device.

```python
import jax
import jax.numpy as jnp

NR = 16384
NC = 16384


def steps_of(rng, dims, shards, smallest, high):
    def one(position, blocks):
        draws = jax.random.uniform(jax.random.fold_in(jax.random.fold_in(rng, 6), position), (blocks,), jnp.float32, smallest / len(shards), high / len(shards))
        return jnp.repeat(jnp.exp(draws), dims[position] // blocks).reshape((-1,) + (1,) * (len(dims) - position - 1))

    loudness = one(*shards[0])
    for cut in shards[1:]:
        loudness = loudness * one(*cut)
    return loudness


def noise(own_key, extent, deviation, reach, cuts=(), kind=jnp.bfloat16):
    result = deviation * jax.random.normal(own_key, extent, jnp.float32)
    if cuts:
        result = result * steps_of(own_key, extent, cuts, -0.22, 0.18)
    return jnp.clip(result, -reach, reach).astype(kind)


def setup_inputs(seed: int = 0) -> dict:
    splits = jax.random.split(jax.random.key(seed), 6)
    coarse = noise(splits[0], (NR // 16, NC // 16), 1.0, 6.0, ((0, 16), (1, 8)), jnp.float32)
    detail4 = noise(splits[1], (3, NR // 16, NC // 16), 1.0, 6.0, ((1, 16), (2, 8)), jnp.float32)
    detail3 = noise(splits[2], (3, NR // 8, NC // 8), 1.0, 6.0, ((1, 16), (2, 8)), jnp.float32)
    detail2 = noise(splits[3], (3, NR // 4, NC // 4), 1.0, 6.0, ((1, 16), (2, 8)), jnp.float32)
    detail1 = noise(splits[4], (3, NR // 2, NC // 2), 1.0, 6.0, ((1, 16), (2, 8)), jnp.float32)
    return {"coarse": coarse, "detail4": detail4, "detail3": detail3, "detail2": detail2, "detail1": detail1}


lift_alpha = -1.586134342059924
lift_beta = -0.052980118572961
lift_gamma = 0.882911075530934
lift_delta = 0.443506852043971
lift_scale = 1.149604398860241


def phase_join(smooth, rough, along):
    target = list(smooth.shape)
    target[along] = 2 * target[along]
    return jnp.stack((smooth, rough), axis=along + 1).reshape(target)


def lift_roll(smooth, rough, along):
    smooth = smooth * lift_scale
    rough = rough / lift_scale
    smooth = smooth - lift_delta * (rough + jnp.roll(rough, 1, along))
    rough = rough - lift_gamma * (smooth + jnp.roll(smooth, -1, along))
    smooth = smooth - lift_beta * (rough + jnp.roll(rough, 1, along))
    rough = rough - lift_alpha * (smooth + jnp.roll(smooth, -1, along))
    return phase_join(smooth, rough, along)


def whole_synth(lowband, detail):
    smooth = jnp.stack((lowband, detail[1]), 0)
    rough = jnp.stack((detail[0], detail[2]), 0)
    halves = lift_roll(smooth, rough, 2)
    return lift_roll(halves[0], halves[1], 0)


def reference(coarse, detail4, detail3, detail2, detail1):
    lowband = coarse
    for detail in (detail4, detail3, detail2, detail1):
        lowband = whole_synth(lowband, detail)
    return lowband
```

```python
import functools

import jax
import jax.numpy as jnp
from jax import lax
from jax.experimental import pallas as pl
from jax.experimental.pallas import tpu as pltpu
from jax.sharding import PartitionSpec as P

ALPHA = -1.586134342059924
BETA = -0.052980118572961
GAMMA = 0.882911075530934
DELTA = 0.443506852043971
SCALE = 1.149604398860241

LANES = 128
HALO = 8
F32 = jnp.float32
MESH = pl.DeviceIdType.MESH

DIRS = ((-1, 0), (1, 0), (0, -1), (0, 1), (-1, -1), (-1, 1), (1, -1), (1, 1))


def lane_iota():
    return lax.broadcasted_iota(jnp.int32, (8, LANES), 1)


def turn(x, amount):
    amount = amount % LANES
    return x if amount == 0 else pltpu.roll(x, amount, axis=1)


def row_plan(levels):
    plan, at = [], 0
    for k, (arrays, blocks, h) in enumerate(levels):
        depth = 2 if k == len(levels) - 1 else 4
        for a in range(arrays):
            for b in range(blocks):
                plan.append((k, a, b, at, depth))
                at += depth
    return plan, -(-at // 8) * 8


def column_plan(levels):
    tiles = []
    for k, (arrays, blocks, h) in enumerate(levels):
        here = [(k, a, j) for a in range(arrays) for j in range(h // 8)]
        for i in range(0, len(here), 32):
            tiles.append(here[i : i + 32])
    return tiles


def exchange_kernel(levels, coarse, d4, d3, d2, d1, s4, s3, s2, s1, rows_out, cols_out, corners_out,
                    rows_in, cols_in, corners_in, load_sem, send_sem, recv_sem):
    bands = (s4, s3, s2, s1)
    nr, nc = lax.axis_size("rows"), lax.axis_size("cols")
    r, c = lax.axis_index("rows"), lax.axis_index("cols")

    def neighbour(step):
        return (lax.rem(r + step[0] + nr, nr), lax.rem(c + step[1] + nc, nc))

    barrier = pltpu.get_barrier_semaphore()
    for step in DIRS:
        pl.semaphore_signal(barrier, inc=1, device_id=neighbour(step), device_id_type=MESH)

    loads = []

    def load(src, dst):
        copy = pltpu.make_async_copy(src, dst, load_sem.at[len(loads)])
        copy.start()
        loads.append(copy)

    h = levels[0][2]
    load(coarse, s4.at[3, 0, pl.ds(HALO, h), :])
    for k, src in enumerate((d4, d3, d2, d1)):
        _, blocks, h = levels[k]
        for b in range(blocks):
            load(src.at[:, :, pl.ds(b * LANES, LANES)], bands[k].at[pl.ds(0, 3), b, pl.ds(HALO, h), :])
    for copy in loads:
        copy.wait()

    lane = lane_iota()
    group = lane // 4
    low = lane < 64

    plan, _ = row_plan(levels)
    for k, a, b, at, depth in plan:
        h = levels[k][2]
        rows_out[0, pl.ds(at, depth), :] = bands[k][a, b, pl.ds(HALO, depth), :]
        rows_out[1, pl.ds(at, depth), :] = bands[k][a, b, pl.ds(HALO + h - depth, depth), :]
    tiles = column_plan(levels)
    for p, members in enumerate(tiles):
        left = jnp.zeros((8, LANES), F32)
        right = jnp.zeros((8, LANES), F32)
        for q, (k, a, j) in enumerate(members):
            last = levels[k][1] - 1
            at = pl.ds(HALO + 8 * j, 8)
            left = jnp.where(group == q, turn(bands[k][a, 0, at, :], 4 * q), left)
            right = jnp.where(group == 31 - q, turn(bands[k][a, last, at, :], -4 * q), right)
        cols_out[0, pl.ds(8 * p, 8), :] = left
        cols_out[1, pl.ds(8 * p, 8), :] = right
    arrays = [(k, a) for k in range(4) for a in range(levels[k][0])]
    for d in range(4):
        step = DIRS[4 + d]
        packed = jnp.zeros((8, LANES), F32)
        for q, (k, a) in enumerate(arrays):
            _, blocks, h = levels[k]
            at = pl.ds(HALO if step[0] < 0 else h, 8)
            if step[1] < 0:
                packed = jnp.where(group == q, turn(bands[k][a, 0, at, :], 4 * q), packed)
            else:
                packed = jnp.where(group == 31 - q, turn(bands[k][a, blocks - 1, at, :], -4 * q), packed)
        corners_out[d] = packed

    pl.semaphore_wait(barrier, len(DIRS))
    sends = []
    for d, step in enumerate(DIRS):
        if d < 2:
            src, dst = rows_out.at[d], rows_in.at[d]
        elif d < 4:
            src, dst = cols_out.at[d - 2], cols_in.at[d - 2]
        else:
            src, dst = corners_out.at[d - 4], corners_in.at[d - 4]
        sends.append(pltpu.make_async_remote_copy(
            src_ref=src, dst_ref=dst, send_sem=send_sem.at[d], recv_sem=recv_sem.at[d],
            device_id=neighbour(step), device_id_type=MESH))
    for d in (4, 5, 6, 7, 0, 1, 2, 3):
        sends[d].start()
    for copy in sends:
        copy.wait()

    for k, a, b, at, depth in plan:
        h = levels[k][2]
        bands[k][a, b, pl.ds(HALO + h, depth), :] = rows_in[0, pl.ds(at, depth), :]
        bands[k][a, b, pl.ds(HALO - depth, depth), :] = rows_in[1, pl.ds(at, depth), :]
    for p, members in enumerate(tiles):
        from_right = cols_in[0, pl.ds(8 * p, 8), :]
        from_left = cols_in[1, pl.ds(8 * p, 8), :]
        for q, (k, a, j) in enumerate(members):
            edge = levels[k][1]
            bands[k][a, edge, pl.ds(HALO + 8 * j, 8), :] = jnp.where(
                low, turn(from_right, -4 * q), turn(from_left, 4 * q))
    for q, (k, a) in enumerate(arrays):
        _, edge, h = levels[k]
        bands[k][a, edge, pl.ds(HALO + h, 8), :] = jnp.where(
            low, turn(corners_in[0], -4 * q), turn(corners_in[1], 4 * q))
        bands[k][a, edge, pl.ds(0, 8), :] = jnp.where(
            low, turn(corners_in[2], -4 * q), turn(corners_in[3], 4 * q))


def lift_lanes(s, r, lane, keep):
    m = len(s)
    first, last = lane == 0, lane == LANES - 1

    def before(x):
        t = [pltpu.roll(v, 1, axis=1) for v in x]
        return [jnp.where(first, t[b - 1], t[b]) for b in range(m)]

    def after(x):
        t = [pltpu.roll(v, LANES - 1, axis=1) for v in x]
        return [jnp.where(last, t[(b + 1) % m], t[b]) for b in range(m)]

    s = [a - DELTA * (b + p) for a, b, p in zip(s, r, before(r))]
    r = [a - GAMMA * (b + p) for a, b, p in zip(r, s, after(s))]
    s = [a - BETA * (b + p) for a, b, p in zip(s, r, before(r))]
    r = [a - ALPHA * (b + p) for a, b, p in zip(r, s, after(s))]
    low, even = lane < 64, (lane & 1) == 0
    spread = (lane // 2) + (lane & 1) * 64
    flip = (lane // 2) + (1 - (lane & 1)) * 64
    pairs = []
    for b in range(keep):
        x = jnp.where(low, s[b], r[b])
        y = jnp.where(low, r[b], s[b])
        px = jnp.take_along_axis(x, spread, axis=1)
        py = jnp.take_along_axis(y, flip, axis=1)
        pairs.append((jnp.where(even, px, py), jnp.where(even, py, px)))
    return pairs


def across(level, final, low_of, band, u, w, unroll):
    arrays, blocks, h = level
    lane = lane_iota()
    keep = blocks if final else blocks + 1

    def tile(i):
        at = pl.ds(pl.multiple_of(i * 8, 8), 8)
        for dst, s, r in (
            (u, [low_of(b, at) * (SCALE * SCALE) for b in range(blocks + 1)],
             [band[0, b, at, :] for b in range(blocks + 1)]),
            (w, [band[1, b, at, :] for b in range(blocks + 1)],
             [band[2, b, at, :] * (1.0 / (SCALE * SCALE)) for b in range(blocks + 1)]),
        ):
            pairs = lift_lanes(s, r, lane, keep)
            for b in range(blocks):
                dst[2 * b, at, :] = pairs[b][0]
                dst[2 * b + 1, at, :] = pairs[b][1]
            if not final:
                dst[2 * blocks, at, :] = jnp.where(lane < 64, pairs[blocks][0], pairs[blocks][1])

    count = h // 8 + 2

    def group(g, carry):
        for i in range(unroll):
            tile(g * unroll + i)
        return carry

    lax.fori_loop(0, count // unroll, group, 0)


def down(h, u, w, b, dst):
    run = -(-(h + 8) // 8)

    def rows(ref, t):
        return ref[b, pl.ds(HALO - 4 + t, 8, stride=run), :]

    r0, s1, r1, s2 = {}, {}, {}, {}
    for t in range(-2, run + 2):
        r0[t] = rows(w, t)
        if t < -1:
            continue
        s1[t] = rows(u, t) - DELTA * (r0[t] + r0[t - 1])
        if t < 0:
            continue
        r1[t - 1] = r0[t - 1] - GAMMA * (s1[t - 1] + s1[t])
        if t < 1:
            continue
        n = t - 1
        s2[n] = s1[n] - BETA * (r1[n] + r1[n - 1])
        if n < run:
            dst[b, pl.ds(2 * n, 8, stride=2 * run), :] = s2[n]
        if n >= 1:
            dst[b, pl.ds(2 * n - 1, 8, stride=2 * run), :] = r1[n - 1] - ALPHA * (s2[n - 1] + s2[n])


def synthesis_kernel(levels, s4, s3, s2, s1, out, l3, l2, l1, image, u4, w4, u3, w3, u2, w2, u1, w1, out_sem):
    bands, us, ws = (s4, s3, s2, s1), (u4, u3, u2, u1), (w4, w3, w2, w1)
    lows = (None, l3, l2, l1)
    unrolls = (5, 9, 17, 11)
    for k in range(4):
        final = k == 3
        if k == 0:
            low_of = lambda b, at: s4[3, b, at, :]
        else:
            low_of = lambda b, at, ref=lows[k]: ref[b, at, :]
        across(levels[k], final, low_of, bands[k], us[k], ws[k], unrolls[k])
        blocks, h = levels[k][1], levels[k][2]
        if not final:
            def body(b, carry, k=k, h=h):
                down(h, us[k], ws[k], b, lows[k + 1])
                return carry
            lax.fori_loop(0, 2 * blocks + 1, body, 0)
        else:
            def body(b, carry, h=h):
                down(h, u1, w1, b, image)
                pltpu.make_async_copy(
                    image.at[b, pl.ds(HALO, 2 * h), :],
                    out.at[:, pl.ds(pl.multiple_of(b * LANES, LANES), LANES)],
                    out_sem.at[b]).start()
                return carry
            lax.fori_loop(0, 2 * blocks, body, 0)
            for b in range(2 * blocks):
                pltpu.make_async_copy(
                    image.at[b, pl.ds(HALO, 2 * h), :], out.at[:, pl.ds(b * LANES, LANES)], out_sem.at[b]).wait()


def per_device(coarse, d4, d3, d2, d1):
    levels = []
    for k, x in enumerate((d4, d3, d2, d1)):
        levels.append((4 if k == 0 else 3, x.shape[2] // LANES, x.shape[1]))
    levels = tuple(levels)
    shapes = [(a, b + 1, h + 2 * HALO, LANES) for a, b, h in levels]
    _, row_count = row_plan(levels)
    col_count = 8 * len(column_plan(levels))
    loads = 1 + sum(b for _, b, _ in levels)
    anywhere = pl.BlockSpec(memory_space=pl.ANY)
    vmem = pl.BlockSpec(memory_space=pltpu.VMEM)
    bands = pl.pallas_call(
        functools.partial(exchange_kernel, levels),
        out_shape=[pltpu.VMEM(s, F32) for s in shapes],
        in_specs=[anywhere] * 5,
        out_specs=[vmem] * 4,
        scratch_shapes=[
            pltpu.VMEM((2, row_count, LANES), F32),
            pltpu.VMEM((2, col_count, LANES), F32),
            pltpu.VMEM((4, 8, LANES), F32),
            pltpu.VMEM((2, row_count, LANES), F32),
            pltpu.VMEM((2, col_count, LANES), F32),
            pltpu.VMEM((4, 8, LANES), F32),
            pltpu.SemaphoreType.DMA((loads,)),
            pltpu.SemaphoreType.DMA((8,)),
            pltpu.SemaphoreType.DMA((8,)),
        ],
        compiler_params=pltpu.CompilerParams(
            collective_id=0, has_side_effects=True, vmem_limit_bytes=16 * 2**20),
    )(coarse, d4, d3, d2, d1)
    blocks, h = levels[3][1], levels[3][2]
    scratch = [pltpu.VMEM((levels[k][1] + 1, levels[k][2] + 2 * HALO, LANES), F32) for k in (1, 2, 3)]
    scratch.append(pltpu.VMEM((2 * blocks, 2 * h + 2 * HALO, LANES), F32))
    for k in range(4):
        wide = 2 * levels[k][1] + (0 if k == 3 else 1)
        scratch += [pltpu.VMEM((wide, levels[k][2] + 2 * HALO, LANES), F32)] * 2
    scratch.append(pltpu.SemaphoreType.DMA((2 * blocks,)))
    return pl.pallas_call(
        functools.partial(synthesis_kernel, levels),
        out_shape=jax.ShapeDtypeStruct((2 * h, 2 * blocks * LANES), F32),
        in_specs=[vmem] * 4,
        out_specs=anywhere,
        scratch_shapes=scratch,
        compiler_params=pltpu.CompilerParams(vmem_limit_bytes=40 * 2**20),
    )(*bands)


def solution(mesh):
    return jax.shard_map(
        per_device,
        mesh=mesh,
        in_specs=(
            P("rows", "cols"),
            P(None, "rows", "cols"),
            P(None, "rows", "cols"),
            P(None, "rows", "cols"),
            P(None, "rows", "cols"),
        ),
        out_specs=P("rows", "cols"),
        check_vma=False,
    )
```

```python
import functools

import jax
import jax.numpy as jnp
from jax import lax
from jax.experimental import pallas as pl
from jax.experimental.pallas import tpu as pltpu
from jax.sharding import PartitionSpec as P

ALPHA = -1.586134342059924
BETA = -0.052980118572961
GAMMA = 0.882911075530934
DELTA = 0.443506852043971
SCALE = 1.149604398860241
UP2 = SCALE * SCALE
DOWN2 = 1.0 / (SCALE * SCALE)

B = 128
HALO = 8
F32 = jnp.float32
MESH = pl.DeviceIdType.MESH

DIRS = ((-1, 0), (1, 0), (0, -1), (0, 1), (-1, -1), (-1, 1), (1, -1), (1, 1))


def iota(axis):
    return lax.broadcasted_iota(jnp.int32, (8, B), axis)


def turn(x, amount):
    amount = amount % B
    return x if amount == 0 else pltpu.roll(x, amount, axis=1)


def row_blocks(level):
    return -(-level[2] // B)


def depth_of(levels, k):
    return 2 if k == len(levels) - 1 else 4


def row_plan(levels):
    plan, at = [], 0
    for k, (arrays, blocks, h) in enumerate(levels):
        for a in range(arrays):
            for b in range(blocks):
                plan.append((k, a, b, at))
                at += depth_of(levels, k)
    return plan, -(-at // 8) * 8


def column_plan(levels):
    plan, at = [], 0
    for k, level in enumerate(levels):
        for a in range(level[0]):
            for n in range(row_blocks(level)):
                plan.append((k, a, n, at))
                at += depth_of(levels, k)
    return plan, -(-at // 8) * 8


def stack_offsets(levels):
    offsets, at = [], 0
    for _, blocks, _ in levels:
        offsets.append(at)
        at += 8 * blocks
    return offsets


def lift_rows(count, s, r, dst):
    run = (count + 8) // 8

    def rows(ref, t):
        return ref[pl.ds(HALO - 4 + t, 8, stride=run), :]

    r0, s1, r1, s2 = {}, {}, {}, {}
    for t in range(-2, run + 2):
        r0[t] = rows(r, t)
        if t < -1:
            continue
        s1[t] = rows(s, t) - DELTA * (r0[t] + r0[t - 1])
        if t < 0:
            continue
        r1[t - 1] = r0[t - 1] - GAMMA * (s1[t - 1] + s1[t])
        if t < 1:
            continue
        n = t - 1
        s2[n] = s1[n] - BETA * (r1[n] + r1[n - 1])
        if n < run:
            dst[pl.ds(2 * n, 8, stride=2 * run), :] = s2[n]
        if n >= 1:
            dst[pl.ds(2 * n - 1, 8, stride=2 * run), :] = r1[n - 1] - ALPHA * (s2[n - 1] + s2[n])


def scaled(x, scale):
    return x if scale is None else x * scale


def turn_back(level, final, n, lifted, edge, dst):
    _, blocks, h = level
    count = min(B, h)
    at = pl.ds(HALO + n * B, count)
    for j in range(2 * blocks):
        dst[j, at, :] = lifted[pl.ds(HALO + j * B, B), :].T[:count]
    if not final:
        edge[0:8, :] = lifted[pl.ds(HALO + 2 * blocks * B, 8), :]
        edge[B - 8 : B, :] = lifted[0:8, :]
        dst[2 * blocks, at, :] = edge[...].T[:count]


def halo_transpose(levels, hn, cn, scale, dst):
    group = iota(1) // 8
    offsets = stack_offsets(levels)
    first = last = None
    for off, (_, blocks, _) in zip(offsets, levels):
        f, l = group == off // 8, group == off // 8 + blocks - 1
        first = f if first is None else first | f
        last = l if last is None else last | l
    t = scaled(hn[...].T, scale)
    ct = scaled(cn[...].T, scale)
    dst[pl.ds(HALO, B), :] = t
    dst[pl.ds(0, 8), :] = jnp.where(first, ct[B - 8 :], turn(t[B - 8 :], 8))
    dst[pl.ds(HALO + B, 8), :] = jnp.where(last, ct[:8], turn(t[:8], -8))


def halo_back(levels, which, lifted, edge, dsts):
    low = iota(1) < 64
    offsets = stack_offsets(levels)
    for j in range(2):
        y = lifted[pl.ds(HALO + j * B, B), :].T
        for k in which:
            _, blocks, h = levels[k]
            for b in range(blocks):
                tile = y[offsets[k] + 8 * b : offsets[k] + 8 * b + 8]
                dsts[k][2 * b + j, pl.ds(0, 8), :] = tile
                dsts[k][2 * b + j, pl.ds(HALO + h, 8), :] = tile
    which = [k for k in which if k < len(levels) - 1]
    if which:
        edge[0:8, :] = lifted[pl.ds(HALO + 2 * B, 8), :]
        edge[B - 8 : B, :] = lifted[0:8, :]
        y = edge[...].T
        for k in which:
            _, blocks, h = levels[k]
            end = offsets[k] + 8 * (blocks - 1)
            tile = jnp.where(low, y[end : end + 8], y[offsets[k] : offsets[k] + 8])
            dsts[k][2 * blocks, pl.ds(0, 8), :] = tile
            dsts[k][2 * blocks, pl.ds(HALO + h, 8), :] = tile


def exchange_kernel(levels, *refs):
    coarse, d4, d3, d2, d1 = refs[:5]
    ws, zs = refs[5:9], refs[9:13]
    zh, c4, ch = refs[13:16]
    ns, xs = refs[16:20], refs[20:24]
    (hn, cn, sh, rh, hd, lifted, edge, rows_out, cols_out, corners_out, rows_in, cols_in, corners_in,
     load_sem, send_sem, recv_sem) = refs[24:]
    nr, nc = lax.axis_size("rows"), lax.axis_size("cols")
    r, c = lax.axis_index("rows"), lax.axis_index("cols")
    top = len(levels) - 1

    def neighbour(step):
        return (lax.rem(r + step[0] + nr, nr), lax.rem(c + step[1] + nc, nc))

    barrier = pltpu.get_barrier_semaphore()
    for step in DIRS:
        pl.semaphore_signal(barrier, inc=1, device_id=neighbour(step), device_id_type=MESH)

    loads = []

    def load(src, dst):
        copy = pltpu.make_async_copy(src, dst, load_sem.at[len(loads)])
        copy.start()
        loads.append(copy)

    h = levels[0][2]
    load(coarse, ns[0].at[3, pl.ds(0, h), :])
    load(d4, ns[0].at[pl.ds(0, 3), pl.ds(0, h), :])
    load(d3, ns[1])
    load(d2, ns[2])
    _, blocks, h = levels[top]
    w = blocks * B
    for at in (pl.ds(0, 8), pl.ds(h - 8, 8)):
        load(d1.at[:, at, :], ns[top].at[:, at, :])
    inner = pl.ds(8, h - 16)
    for at in (pl.ds(0, B), pl.ds(w - B, B)):
        load(d1.at[:, inner, at], ns[top].at[:, inner, at])
    for a in range(3):
        at = pl.ds(B, w - 2 * B)
        load(d1.at[a, inner, at], ns[top].at[a, inner, at])

    def columns_of(k, a):
        return c4 if a == 3 else zs[k] if a == 0 else xs[k].at[a - 1]

    def transpose(k, a, n, b):
        scale = (None, None, DOWN2, UP2)[a]
        columns_of(k, a)[n, pl.ds(HALO + b * B, B), :] = scaled(
            ns[k][a, pl.ds(n * B, B), pl.ds(b * B, B)].T, scale)

    for copy in loads[:4]:
        copy.wait()
    for k in range(top):
        for a in range(levels[k][0]):
            for n in range(row_blocks(levels[k])):
                for b in range(levels[k][1]):
                    transpose(k, a, n, b)
    for copy in loads[4:8]:
        copy.wait()
    for a in range(3):
        for n in range(row_blocks(levels[top])):
            for b in (0, levels[top][1] - 1):
                transpose(top, a, n, b)

    rows, _ = row_plan(levels)
    for k, a, b, at in rows:
        depth, h = depth_of(levels, k), levels[k][2]
        here = pl.ds(b * B, B)
        rows_out[0, pl.ds(at, depth), :] = ns[k][a, pl.ds(0, depth), here]
        rows_out[1, pl.ds(at, depth), :] = ns[k][a, pl.ds(h - depth, depth), here]
    group = iota(1) // 4
    arrays = [(k, a) for k in range(top + 1) for a in range(levels[k][0])]
    for d in range(4):
        step = DIRS[4 + d]
        packed = jnp.zeros((8, B), F32)
        for q, (k, a) in enumerate(arrays):
            _, blocks, h = levels[k]
            at = pl.ds(0 if step[0] < 0 else h - 8, 8)
            if step[1] < 0:
                packed = jnp.where(group == q, turn(ns[k][a, at, pl.ds(0, B)], 4 * q), packed)
            else:
                packed = jnp.where(
                    group == 31 - q, turn(ns[k][a, at, pl.ds((blocks - 1) * B, B)], -4 * q), packed)
        corners_out[d] = packed
    columns, _ = column_plan(levels)
    for k, a, n, at in columns:
        depth, w = depth_of(levels, k), levels[k][1] * B
        cols_out[0, pl.ds(at, depth), :] = columns_of(k, a)[n, pl.ds(HALO, depth), :]
        cols_out[1, pl.ds(at, depth), :] = columns_of(k, a)[n, pl.ds(HALO + w - depth, depth), :]

    pl.semaphore_wait(barrier, len(DIRS))
    sends = []
    for d, step in enumerate(DIRS):
        if d < 2:
            src, dst = rows_out.at[d], rows_in.at[d]
        elif d < 4:
            src, dst = cols_out.at[d - 2], cols_in.at[d - 2]
        else:
            src, dst = corners_out.at[d - 4], corners_in.at[d - 4]
        sends.append(pltpu.make_async_remote_copy(
            src_ref=src, dst_ref=dst, send_sem=send_sem.at[d], recv_sem=recv_sem.at[d],
            device_id=neighbour(step), device_id_type=MESH))
    for d in (4, 5, 6, 7, 0, 1, 2, 3):
        sends[d].start()

    for copy in loads[8:]:
        copy.wait()

    def middle(a, carry):
        for n in range(row_blocks(levels[top])):
            for b in range(1, levels[top][1] - 1):
                at = pl.ds(HALO + b * B, B)
                block = ns[top][a, pl.ds(n * B, B), pl.ds(b * B, B)].T
                xs[top][a - 1, n, at, :] = block * jnp.where(a == 2, F32(DOWN2), F32(1.0))
        return carry

    for n in range(row_blocks(levels[top])):
        for b in range(1, levels[top][1] - 1):
            transpose(top, 0, n, b)
    lax.fori_loop(1, 3, middle, 0)

    sends[2].wait()
    sends[3].wait()
    for k, a, n, at in columns:
        depth, w = depth_of(levels, k), levels[k][1] * B
        columns_of(k, a)[n, pl.ds(HALO + w, depth), :] = cols_in[0, pl.ds(at, depth), :]
        columns_of(k, a)[n, pl.ds(HALO - depth, depth), :] = cols_in[1, pl.ds(at, depth), :]
    for k in (3, 2, 1, 0):
        for n in range(row_blocks(levels[k])):
            part = lifted.at[n, pl.ds(0, 2 * levels[k][1] * B + 16), :]
            lift_rows(levels[k][1] * B, xs[k].at[0, n], xs[k].at[1, n], part)
            turn_back(levels[k], k == top, n, part, edge, ws[k])

    for d in (0, 1, 4, 5, 6, 7):
        sends[d].wait()
    offsets = stack_offsets(levels)
    for k, a, b, at in rows:
        depth, base = depth_of(levels, k), offsets[k] + 8 * b
        hn[a, pl.ds(base, depth), :] = rows_in[0, pl.ds(at, depth), :]
        hn[a, pl.ds(base + 8 - depth, depth), :] = rows_in[1, pl.ds(at, depth), :]
    low, bottom = iota(1) < 64, iota(0) < 4
    for q, (k, a) in enumerate(arrays):
        tile = jnp.where(
            bottom,
            jnp.where(low, turn(corners_in[0], -4 * q), turn(corners_in[1], 4 * q)),
            jnp.where(low, turn(corners_in[2], -4 * q), turn(corners_in[3], 4 * q)))
        cn[a, pl.ds(offsets[k], 8), :] = tile
        cn[a, pl.ds(offsets[k] + 8 * (levels[k][1] - 1), 8), :] = tile
    halo_transpose(levels, hn.at[1], cn.at[1], None, sh)
    halo_transpose(levels, hn.at[2], cn.at[2], DOWN2, rh)
    halo_transpose(levels, hn.at[0], cn.at[0], None, zh)
    halo_transpose(levels, hn.at[3], cn.at[3], UP2, ch)
    lift_rows(B, sh, rh, hd)
    halo_back(levels, range(top + 1), hd, edge, ws)


def synthesis_kernel(levels, *refs):
    ws, zs = refs[:4], refs[4:8]
    zh, c4, ch = refs[8:11]
    out = refs[11]
    lows = (None,) + refs[12:15]
    image = refs[15]
    us, ts = refs[16:20], (c4,) + refs[20:23]
    hn, cn, th, hd, lifted, edge, out_sem = refs[23:]
    top = len(levels) - 1
    offsets = stack_offsets(levels)
    bottom = iota(0) < 4

    for k, level in enumerate(levels):
        _, blocks, h = level
        w = blocks * B
        final = k == top
        n_rows = row_blocks(level)
        if k == 0:
            halo = ch
        else:
            halo = th
            low = lows[k]
            for b in range(blocks + 1):
                tile = jnp.where(bottom, low[b, pl.ds(HALO + h, 8), :], low[b, pl.ds(0, 8), :])
                if b < blocks:
                    hn[pl.ds(offsets[k] + 8 * b, 8), :] = tile
                else:
                    cn[pl.ds(offsets[k], 8), :] = tile
                    cn[pl.ds(offsets[k] + 8 * (blocks - 1), 8), :] = tile
            halo_transpose(levels, hn, cn, UP2, th)
            for n in range(n_rows):
                at = pl.ds(HALO + n * B, B)
                for b in range(blocks):
                    ts[k][n, pl.ds(HALO + b * B, B), :] = low[b, at, :].T * UP2
                side = low[blocks, at, :].T * UP2
                ts[k][n, pl.ds(0, 8), :] = side[B - 8 :]
                ts[k][n, pl.ds(HALO + w, 8), :] = side[:8]
        lift_rows(B, halo, zh, hd)
        halo_back(levels, (k,), hd, edge, {k: us[k]})
        for n in range(n_rows):
            part = lifted.at[n, pl.ds(0, 2 * w + 16), :]
            lift_rows(w, ts[k].at[n], zs[k].at[n], part)
            turn_back(level, final, n, part, edge, us[k])
        if not final:
            for j in range(2 * blocks + 1):
                lift_rows(h, us[k].at[j], ws[k].at[j], lows[k + 1].at[j])
        else:
            def body(j, carry, h=h):
                lift_rows(h, us[top].at[j], ws[top].at[j], image.at[j])
                pltpu.make_async_copy(
                    image.at[j, pl.ds(HALO, 2 * h), :],
                    out.at[:, pl.ds(pl.multiple_of(j * B, B), B)], out_sem.at[j]).start()
                return carry

            lax.fori_loop(0, 2 * blocks, body, 0)
            for j in range(2 * blocks):
                pltpu.make_async_copy(
                    image.at[j, pl.ds(HALO, 2 * h), :], out.at[:, pl.ds(j * B, B)], out_sem.at[j]).wait()


def per_device(coarse, d4, d3, d2, d1):
    levels = []
    for k, x in enumerate((d4, d3, d2, d1)):
        levels.append((4 if k == 0 else 3, x.shape[2] // B, x.shape[1]))
    levels = tuple(levels)
    top = len(levels) - 1
    _, row_count = row_plan(levels)
    _, col_count = column_plan(levels)
    hbm = pl.BlockSpec(memory_space=pltpu.HBM)
    vmem = pl.BlockSpec(memory_space=pltpu.VMEM)
    wide = [2 * b + (0 if k == top else 1) for k, (_, b, _) in enumerate(levels)]
    across = [(row_blocks(l), l[1] * B + 2 * HALO, B) for l in levels]
    strips = [(n, l[2] + 2 * HALO, B) for n, l in zip(wide, levels)]
    stack = (B + 2 * HALO, B)
    lifted = pltpu.VMEM((across[top][0], 2 * levels[top][1] * B + 2 * HALO, B), F32)
    between = pl.pallas_call(
        functools.partial(exchange_kernel, levels),
        out_shape=[pltpu.VMEM(s, F32) for s in strips + across + [stack, across[0], stack]],
        in_specs=[hbm] * 5,
        out_specs=[vmem] * 11,
        scratch_shapes=[
            *[pltpu.VMEM((a, max(B, h), b * B), F32) for a, b, h in levels],
            *[pltpu.VMEM((2,) + s, F32) for s in across],
            pltpu.VMEM((4, B, B), F32),
            pltpu.VMEM((4, B, B), F32),
            pltpu.VMEM(stack, F32),
            pltpu.VMEM(stack, F32),
            pltpu.VMEM((2 * B + 2 * HALO, B), F32),
            lifted,
            pltpu.VMEM((B, B), F32),
            pltpu.VMEM((2, row_count, B), F32),
            pltpu.VMEM((2, col_count, B), F32),
            pltpu.VMEM((4, 8, B), F32),
            pltpu.VMEM((2, row_count, B), F32),
            pltpu.VMEM((2, col_count, B), F32),
            pltpu.VMEM((4, 8, B), F32),
            pltpu.SemaphoreType.DMA((11,)),
            pltpu.SemaphoreType.DMA((8,)),
            pltpu.SemaphoreType.DMA((8,)),
        ],
        compiler_params=pltpu.CompilerParams(
            collective_id=0, has_side_effects=True, vmem_limit_bytes=26 * 2**20),
    )(*[pltpu.with_memory_space_constraint(x, pltpu.HBM) for x in (coarse, d4, d3, d2, d1)])
    blocks, h = levels[top][1], levels[top][2]
    return pl.pallas_call(
        functools.partial(synthesis_kernel, levels),
        out_shape=jax.ShapeDtypeStruct((2 * h, 2 * blocks * B), F32),
        in_specs=[vmem] * 11,
        out_specs=pl.BlockSpec(memory_space=pl.ANY),
        scratch_shapes=[
            *[pltpu.VMEM((levels[k][1] + 1, levels[k][2] + 2 * HALO, B), F32) for k in (1, 2, 3)],
            pltpu.VMEM((2 * blocks, 2 * h + 2 * HALO, B), F32),
            *[pltpu.VMEM(s, F32) for s in strips],
            *[pltpu.VMEM(s, F32) for s in across[1:]],
            pltpu.VMEM((B, B), F32),
            pltpu.VMEM((B, B), F32),
            pltpu.VMEM(stack, F32),
            pltpu.VMEM((2 * B + 2 * HALO, B), F32),
            lifted,
            pltpu.VMEM((B, B), F32),
            pltpu.SemaphoreType.DMA((2 * blocks,)),
        ],
        compiler_params=pltpu.CompilerParams(vmem_limit_bytes=28 * 2**20),
    )(*between)


def solution(mesh):
    return jax.shard_map(
        per_device,
        mesh=mesh,
        in_specs=(
            P("rows", "cols"),
            P(None, "rows", "cols"),
            P(None, "rows", "cols"),
            P(None, "rows", "cols"),
            P(None, "rows", "cols"),
        ),
        out_specs=P("rows", "cols"),
        check_vma=False,
    )
```

```python
import functools

import jax
import jax.numpy as jnp
from jax import lax
from jax.experimental import pallas as pl
from jax.experimental.pallas import tpu as pltpu
from jax.sharding import PartitionSpec as P

ALPHA = -1.586134342059924
BETA = -0.052980118572961
GAMMA = 0.882911075530934
DELTA = 0.443506852043971
SCALE = 1.149604398860241
UP2 = SCALE * SCALE
DOWN2 = 1.0 / (SCALE * SCALE)

B = 128
HALO = 8
F32 = jnp.float32
MESH = pl.DeviceIdType.MESH

DIRS = ((-1, 0), (1, 0), (0, -1), (0, 1), (-1, -1), (-1, 1), (1, -1), (1, 1))


def iota(axis):
    return lax.broadcasted_iota(jnp.int32, (8, B), axis)


def turn(x, amount):
    amount = amount % B
    return x if amount == 0 else pltpu.roll(x, amount, axis=1)


def row_blocks(level):
    return -(-level[2] // B)


def depth_of(levels, k):
    return 2 if k == len(levels) - 1 else 4


def row_plan(levels):
    plan, at = [], 0
    for k, (arrays, blocks, h) in enumerate(levels):
        for a in range(arrays):
            for b in range(blocks):
                plan.append((k, a, b, at))
                at += depth_of(levels, k)
    return plan, -(-at // 8) * 8


def column_plan(levels):
    plan, at = [], 0
    for k, level in enumerate(levels):
        for a in range(level[0]):
            for n in range(row_blocks(level)):
                plan.append((k, a, n, at))
                at += depth_of(levels, k)
    return plan, -(-at // 8) * 8


def stack_offsets(levels):
    offsets, at = [], 0
    for _, blocks, _ in levels:
        offsets.append(at)
        at += 8 * blocks
    return offsets


def lift_rows(count, s, r, dst):
    lift_runs((count + 8) // 8, s, HALO - 4, r, HALO - 4, dst)


def lift_runs(run, s, s_at, r, r_at, dst):
    def rows(ref, t):
        at = s_at if ref is s else r_at
        return ref[pl.ds(at + t, 8, stride=run), :]

    r0, s1, r1, s2 = {}, {}, {}, {}
    for t in range(-2, run + 2):
        r0[t] = rows(r, t)
        if t < -1:
            continue
        s1[t] = rows(s, t) - DELTA * (r0[t] + r0[t - 1])
        if t < 0:
            continue
        r1[t - 1] = r0[t - 1] - GAMMA * (s1[t - 1] + s1[t])
        if t < 1:
            continue
        n = t - 1
        s2[n] = s1[n] - BETA * (r1[n] + r1[n - 1])
        if n < run:
            dst[pl.ds(2 * n, 8, stride=2 * run), :] = s2[n]
        if n >= 1:
            dst[pl.ds(2 * n - 1, 8, stride=2 * run), :] = r1[n - 1] - ALPHA * (s2[n - 1] + s2[n])


def scaled(x, scale):
    return x if scale is None else x * scale


def turn_back(level, final, n, lifted, edge, dst):
    _, blocks, h = level
    count = min(B, h)
    at = pl.ds(HALO + n * B, count)
    for j in range(2 * blocks):
        dst[j, at, :] = lifted[pl.ds(HALO + j * B, B), :].T[:count]
    if not final:
        edge[0:8, :] = lifted[pl.ds(HALO + 2 * blocks * B, 8), :]
        edge[B - 8 : B, :] = lifted[0:8, :]
        dst[2 * blocks, at, :] = edge[...].T[:count]


def halo_transpose(levels, hn, cn, scale, dst):
    group = iota(1) // 8
    offsets = stack_offsets(levels)
    first = last = None
    for off, (_, blocks, _) in zip(offsets, levels):
        f, l = group == off // 8, group == off // 8 + blocks - 1
        first = f if first is None else first | f
        last = l if last is None else last | l
    t = scaled(hn[...].T, scale)
    ct = scaled(cn[...].T, scale)
    dst[pl.ds(HALO, B), :] = t
    dst[pl.ds(0, 8), :] = jnp.where(first, ct[B - 8 :], turn(t[B - 8 :], 8))
    dst[pl.ds(HALO + B, 8), :] = jnp.where(last, ct[:8], turn(t[:8], -8))


def halo_back(levels, which, lifted, edge, dsts):
    low = iota(1) < 64
    offsets = stack_offsets(levels)
    for j in range(2):
        y = lifted[pl.ds(HALO + j * B, B), :].T
        for k in which:
            _, blocks, h = levels[k]
            for b in range(blocks):
                tile = y[offsets[k] + 8 * b : offsets[k] + 8 * b + 8]
                dsts[k][2 * b + j, pl.ds(0, 8), :] = tile
                dsts[k][2 * b + j, pl.ds(HALO + h, 8), :] = tile
    which = [k for k in which if k < len(levels) - 1]
    if which:
        edge[0:8, :] = lifted[pl.ds(HALO + 2 * B, 8), :]
        edge[B - 8 : B, :] = lifted[0:8, :]
        y = edge[...].T
        for k in which:
            _, blocks, h = levels[k]
            end = offsets[k] + 8 * (blocks - 1)
            tile = jnp.where(low, y[end : end + 8], y[offsets[k] : offsets[k] + 8])
            dsts[k][2 * blocks, pl.ds(0, 8), :] = tile
            dsts[k][2 * blocks, pl.ds(HALO + h, 8), :] = tile


def strip_rows(k):
    return (16, 16, 24, 40)[k]


def strip_sides(levels, k, main, ct, dst):
    _, blocks, h = levels[k]
    keep, off = strip_rows(k), stack_offsets(levels)[k]
    lane = iota(1)
    n = row_blocks(levels[k])
    start = h - keep - B * (n - 1)
    w = blocks * B
    for at, corner, shift in ((0, ct[B - 8 :], off), (HALO + w, ct[:8], off + 8 * (blocks - 1))):
        here = pl.ds(at, 8)
        dst[here, :] = jnp.where(
            lane < 8, turn(corner, -shift),
            jnp.where(
                lane < 8 + keep, turn(main[0, here, :], 8),
                jnp.where(lane < 8 + 2 * keep, turn(main[n - 1, here, :], 8 + keep - start),
                          turn(corner, 8 + 2 * keep - shift))))


def at_of(levels, k, a, b):
    return b if a == 3 else 1 + sum(l[1] for l in levels[:k]) + b


def columns_from(level, low, dst):
    _, blocks, _ = level
    for n in range(row_blocks(level)):
        at = pl.ds(HALO + n * B, B)
        for b in range(blocks):
            dst[n, pl.ds(HALO + b * B, B), :] = low[b, at, :].T * UP2
        side = low[blocks, at, :].T * UP2
        dst[n, pl.ds(0, 8), :] = side[B - 8 :]
        dst[n, pl.ds(HALO + blocks * B, 8), :] = side[:8]


def exchange_kernel(levels, *refs):
    coarse, d4, d3, d2, d1 = refs[:5]
    ws, zts, ct_out, image = refs[5:9], refs[9:13], refs[13], refs[14]
    ns, xs, zs, us = refs[15:19], refs[19:23], refs[23:27], refs[27:31]
    lows, ts = (None,) + refs[31:34], refs[34:38]
    c4 = ts[0]
    (hn, cn, sh, rh, hd, lifted, edge, ds, rows_out, cols_out, corners_out, rows_in, cols_in, corners_in,
     load_sem, send_sem, recv_sem) = refs[38:]
    nr, nc = lax.axis_size("rows"), lax.axis_size("cols")
    r, c = lax.axis_index("rows"), lax.axis_index("cols")
    top = len(levels) - 1

    def neighbour(step):
        return (lax.rem(r + step[0] + nr, nr), lax.rem(c + step[1] + nc, nc))

    barrier = pltpu.get_barrier_semaphore()
    for step in DIRS:
        pl.semaphore_signal(barrier, inc=1, device_id=neighbour(step), device_id_type=MESH)

    loads = []

    def load(src, dst):
        copy = pltpu.make_async_copy(src, dst, load_sem.at[len(loads)])
        copy.start()
        loads.append(copy)

    h = levels[0][2]
    load(coarse, ns[0].at[3, pl.ds(0, h), :])
    load(d4, ns[0].at[pl.ds(0, 3), pl.ds(0, h), :])
    load(d3, ns[1])
    load(d2, ns[2])
    _, blocks, h = levels[top]
    w = blocks * B
    for at in (pl.ds(0, 8), pl.ds(h - 8, 8)):
        load(d1.at[:, at, :], ns[top].at[:, at, :])
    inner = pl.ds(8, h - 16)
    for at in (pl.ds(0, B), pl.ds(w - B, B)):
        load(d1.at[:, inner, at], ns[top].at[:, inner, at])
    for a in range(3):
        at = pl.ds(B, w - 2 * B)
        load(d1.at[a, inner, at], ns[top].at[a, inner, at])

    def columns_of(k, a):
        return c4 if a == 3 else zs[k] if a == 0 else xs[k].at[a - 1]

    def transpose(k, a, n, b):
        scale = (None, None, DOWN2, UP2)[a]
        columns_of(k, a)[n, pl.ds(HALO + b * B, B), :] = scaled(
            ns[k][a, pl.ds(n * B, B), pl.ds(b * B, B)].T, scale)

    for copy in loads[:4]:
        copy.wait()
    for k in range(top):
        for a in range(levels[k][0]):
            for n in range(row_blocks(levels[k])):
                for b in range(levels[k][1]):
                    transpose(k, a, n, b)
    for copy in loads[4:8]:
        copy.wait()
    for a in range(3):
        for n in range(row_blocks(levels[top])):
            for b in (0, levels[top][1] - 1):
                transpose(top, a, n, b)

    rows, _ = row_plan(levels)
    for k, a, b, at in rows:
        depth, h = depth_of(levels, k), levels[k][2]
        here = pl.ds(b * B, B)
        rows_out[0, pl.ds(at, depth), :] = ns[k][a, pl.ds(0, depth), here]
        rows_out[1, pl.ds(at, depth), :] = ns[k][a, pl.ds(h - depth, depth), here]
    group = iota(1) // 4
    arrays = [(k, a) for k in range(top + 1) for a in range(levels[k][0])]
    for d in range(4):
        step = DIRS[4 + d]
        packed = jnp.zeros((8, B), F32)
        for q, (k, a) in enumerate(arrays):
            _, blocks, h = levels[k]
            at = pl.ds(0 if step[0] < 0 else h - 8, 8)
            if step[1] < 0:
                packed = jnp.where(group == q, turn(ns[k][a, at, pl.ds(0, B)], 4 * q), packed)
            else:
                packed = jnp.where(
                    group == 31 - q, turn(ns[k][a, at, pl.ds((blocks - 1) * B, B)], -4 * q), packed)
        corners_out[d] = packed
    columns, _ = column_plan(levels)
    for k, a, n, at in columns:
        depth, w = depth_of(levels, k), levels[k][1] * B
        cols_out[0, pl.ds(at, depth), :] = columns_of(k, a)[n, pl.ds(HALO, depth), :]
        cols_out[1, pl.ds(at, depth), :] = columns_of(k, a)[n, pl.ds(HALO + w - depth, depth), :]

    pl.semaphore_wait(barrier, len(DIRS))
    sends = []
    for d, step in enumerate(DIRS):
        if d < 2:
            src, dst = rows_out.at[d], rows_in.at[d]
        elif d < 4:
            src, dst = cols_out.at[d - 2], cols_in.at[d - 2]
        else:
            src, dst = corners_out.at[d - 4], corners_in.at[d - 4]
        sends.append(pltpu.make_async_remote_copy(
            src_ref=src, dst_ref=dst, send_sem=send_sem.at[d], recv_sem=recv_sem.at[d],
            device_id=neighbour(step), device_id_type=MESH))
    for d in (4, 5, 6, 7, 0, 1, 2, 3):
        sends[d].start()

    for copy in loads[8:]:
        copy.wait()

    def middle(a, carry):
        for n in range(row_blocks(levels[top])):
            for b in range(1, levels[top][1] - 1):
                at = pl.ds(HALO + b * B, B)
                block = ns[top][a, pl.ds(n * B, B), pl.ds(b * B, B)].T
                xs[top][a - 1, n, at, :] = block * jnp.where(a == 2, F32(DOWN2), F32(1.0))
        return carry

    for n in range(row_blocks(levels[top])):
        for b in range(1, levels[top][1] - 1):
            transpose(top, 0, n, b)
    lax.fori_loop(1, 3, middle, 0)

    sends[2].wait()
    sends[3].wait()
    for k, a, n, at in columns:
        depth, w = depth_of(levels, k), levels[k][1] * B
        columns_of(k, a)[n, pl.ds(HALO + w, depth), :] = cols_in[0, pl.ds(at, depth), :]
        columns_of(k, a)[n, pl.ds(HALO - depth, depth), :] = cols_in[1, pl.ds(at, depth), :]
    for k in (3, 2, 1, 0):
        for n in range(row_blocks(levels[k])):
            part = lifted.at[n, pl.ds(0, 2 * levels[k][1] * B + 16), :]
            lift_rows(levels[k][1] * B, xs[k].at[0, n], xs[k].at[1, n], part)
            turn_back(levels[k], k == top, n, part, edge, ws[k])

    for k, level in enumerate(levels):
        _, blocks, h = level
        w = blocks * B
        if k > 0:
            columns_from(level, lows[k], ts[k])
        for n in range(row_blocks(level)):
            part = lifted.at[n, pl.ds(0, 2 * w + 16), :]
            lift_rows(w, ts[k].at[n], zs[k].at[n], part)
            turn_back(level, k == top, n, part, edge, us[k])
        if k < top:
            for j in range(2 * blocks + 1):
                lift_rows(h, us[k].at[j], ws[k].at[j], lows[k + 1].at[j])
        else:
            def body(j, carry, h=h):
                lift_rows(h, us[top].at[j], ws[top].at[j], image.at[j])
                return carry

            lax.fori_loop(0, 2 * blocks, body, 0)

    for k, (_, blocks, h) in enumerate(levels):
        keep = strip_rows(k)
        for a in (0, 3) if k == 0 else (0,):
            for b in range(blocks):
                at = pl.ds(b * B, B)
                ds[at_of(levels, k, a, b), pl.ds(8, keep), :] = ns[k][a, pl.ds(0, keep), at]
                ds[at_of(levels, k, a, b), pl.ds(8 + keep, keep), :] = ns[k][a, pl.ds(h - keep, keep), at]

    for d in (0, 1, 4, 5, 6, 7):
        sends[d].wait()
    offsets = stack_offsets(levels)
    for k, a, b, at in rows:
        depth, base = depth_of(levels, k), offsets[k] + 8 * b
        hn[a, pl.ds(base, depth), :] = rows_in[0, pl.ds(at, depth), :]
        hn[a, pl.ds(base + 8 - depth, depth), :] = rows_in[1, pl.ds(at, depth), :]
    low, bottom = iota(1) < 64, iota(0) < 4
    for q, (k, a) in enumerate(arrays):
        tile = jnp.where(
            bottom,
            jnp.where(low, turn(corners_in[0], -4 * q), turn(corners_in[1], 4 * q)),
            jnp.where(low, turn(corners_in[2], -4 * q), turn(corners_in[3], 4 * q)))
        cn[a, pl.ds(offsets[k], 8), :] = tile
        cn[a, pl.ds(offsets[k] + 8 * (levels[k][1] - 1), 8), :] = tile
    halo_transpose(levels, hn.at[1], cn.at[1], None, sh)
    halo_transpose(levels, hn.at[2], cn.at[2], DOWN2, rh)
    for k, a, b, at in rows:
        if a in (0, 3):
            depth, keep = depth_of(levels, k), strip_rows(k)
            strip = at_of(levels, k, a, b)
            ds[strip, pl.ds(8 + 2 * keep, depth), :] = rows_in[0, pl.ds(at, depth), :]
            ds[strip, pl.ds(8 - depth, depth), :] = rows_in[1, pl.ds(at, depth), :]
            (ct_out if a == 3 else zts[k])[pl.ds(HALO + b * B, B), :] = scaled(
                ds[strip].T, UP2 if a == 3 else None)
    side = cn[0].T
    for k in range(top + 1):
        strip_sides(levels, k, zs[k], side, zts[k])
    strip_sides(levels, 0, c4, cn[3].T * UP2, ct_out)
    lift_rows(B, sh, rh, hd)
    halo_back(levels, range(top + 1), hd, edge, ws)


def strip_kernel(levels, *refs):
    ws, zts, ct, image = refs[:4], refs[4:8], refs[8], refs[9]
    out = refs[10]
    lows = (None,) + refs[11:14]
    ends, us, lifted, edge, th, out_sem, end_sem = refs[14:]
    top = len(levels) - 1
    _, blocks, h = levels[top]
    rows = 2 * h
    cut = 64

    def main(j, start):
        at = pl.ds(cut, rows - 2 * cut)
        return pltpu.make_async_copy(
            image.at[j, pl.ds(HALO + cut, rows - 2 * cut), :], out.at[at, pl.ds(start, B)], out_sem.at[j])

    def send(j, carry):
        main(j, pl.multiple_of(j * B, B)).start()
        return carry

    lax.fori_loop(0, 2 * blocks, send, 0)

    for k, level in enumerate(levels):
        _, nb, h = level
        w = nb * B
        final = k == top
        keep = strip_rows(k)
        size = 2 * keep + 16
        if k == 0:
            t = ct
        else:
            t = th
            for b in range(nb):
                t[pl.ds(HALO + b * B, B), :] = lows[k][b].T * UP2
            side = lows[k][nb].T * UP2
            t[pl.ds(0, 8), :] = side[B - 8 :]
            t[pl.ds(HALO + w, 8), :] = side[:8]
        part = lifted.at[pl.ds(0, 2 * w + 16), :]
        lift_rows(w, t, zts[k], part)
        for j in range(2 * nb):
            us[j] = lifted[pl.ds(HALO + j * B, B), :].T
        if not final:
            edge[0:8, :] = lifted[pl.ds(HALO + 2 * w, 8), :]
            edge[B - 8 : B, :] = lifted[0:8, :]
            us[2 * nb] = edge[...].T
        run = keep // 8

        def strips(j, first, second, level=level, k=k):
            _, _, h = level
            keep = strip_rows(k)
            run = keep // 8
            lift_runs(run, us.at[j], 4, ws[k].at[j], 4, first)
            lift_runs(run, us.at[j], 8 + 2 * keep + 4 - 8 * run, ws[k].at[j], HALO + h + 4 - 8 * run, second)

        if not final:
            following = strip_rows(k + 1)
            made = 16 * run
            for j in range(2 * nb + 1):
                strips(j, ends.at[0, j, pl.ds(0, made), :], ends.at[1, j, pl.ds(0, made), :])
                lows[k + 1][j, pl.ds(0, 8 + following), :] = ends[0, j, pl.ds(0, 8 + following), :]
                lows[k + 1][j, pl.ds(8 + following, 8 + following), :] = ends[
                    1, j, pl.ds(made - 8 - following, 8 + following), :]
        else:
            made = 16 * run

            def end(j, side, start):
                row = (HALO, made - 8 - cut)[side]
                return pltpu.make_async_copy(
                    ends.at[side, j, pl.ds(row, cut), :],
                    out.at[pl.ds((0, rows - cut)[side], cut), pl.ds(start, B)], end_sem.at[side, j])

            def body(j, carry):
                strips(j, ends.at[0, j, pl.ds(0, made), :], ends.at[1, j, pl.ds(0, made), :])
                for side in range(2):
                    end(j, side, pl.multiple_of(j * B, B)).start()
                return carry

            lax.fori_loop(0, 2 * nb, body, 0)
            for j in range(2 * nb):
                main(j, j * B).wait()
                for side in range(2):
                    end(j, side, j * B).wait()


def per_device(coarse, d4, d3, d2, d1):
    levels = []
    for k, x in enumerate((d4, d3, d2, d1)):
        levels.append((4 if k == 0 else 3, x.shape[2] // B, x.shape[1]))
    levels = tuple(levels)
    top = len(levels) - 1
    _, row_count = row_plan(levels)
    _, col_count = column_plan(levels)
    hbm = pl.BlockSpec(memory_space=pltpu.HBM)
    vmem = pl.BlockSpec(memory_space=pltpu.VMEM)
    wide = [2 * b + (0 if k == top else 1) for k, (_, b, _) in enumerate(levels)]
    across = [(row_blocks(l), l[1] * B + 2 * HALO, B) for l in levels]
    strips = [(n, l[2] + 2 * HALO, B) for n, l in zip(wide, levels)]
    stack = (B + 2 * HALO, B)
    blocks, h = levels[top][1], levels[top][2]
    long = 2 * blocks * B + 2 * HALO
    bands = [(l[1] + 1, l[2] + 2 * HALO, B) for l in levels[1:]]
    between = pl.pallas_call(
        functools.partial(exchange_kernel, levels),
        out_shape=[pltpu.VMEM(s, F32) for s in (
            strips + [s[1:] for s in across] + [across[0][1:], (2 * blocks, 2 * h + 2 * HALO, B)])],
        in_specs=[hbm] * 5,
        out_specs=[vmem] * 10,
        scratch_shapes=[
            *[pltpu.VMEM((a, max(B, h), b * B), F32) for a, b, h in levels],
            *[pltpu.VMEM((2,) + s, F32) for s in across],
            *[pltpu.VMEM(s, F32) for s in across],
            *[pltpu.VMEM(s, F32) for s in strips],
            *[pltpu.VMEM(s, F32) for s in bands],
            *[pltpu.VMEM(s, F32) for s in across],
            pltpu.VMEM((4, B, B), F32),
            pltpu.VMEM((4, B, B), F32),
            pltpu.VMEM(stack, F32),
            pltpu.VMEM(stack, F32),
            pltpu.VMEM((2 * B + 2 * HALO, B), F32),
            pltpu.VMEM((across[top][0], long, B), F32),
            pltpu.VMEM((B, B), F32),
            pltpu.VMEM((1 + sum(l[1] for l in levels), B, B), F32),
            pltpu.VMEM((2, row_count, B), F32),
            pltpu.VMEM((2, col_count, B), F32),
            pltpu.VMEM((4, 8, B), F32),
            pltpu.VMEM((2, row_count, B), F32),
            pltpu.VMEM((2, col_count, B), F32),
            pltpu.VMEM((4, 8, B), F32),
            pltpu.SemaphoreType.DMA((11,)),
            pltpu.SemaphoreType.DMA((8,)),
            pltpu.SemaphoreType.DMA((8,)),
        ],
        compiler_params=pltpu.CompilerParams(
            collective_id=0, has_side_effects=True, vmem_limit_bytes=40 * 2**20),
    )(*[pltpu.with_memory_space_constraint(x, pltpu.HBM) for x in (coarse, d4, d3, d2, d1)])
    return pl.pallas_call(
        functools.partial(strip_kernel, levels),
        out_shape=jax.ShapeDtypeStruct((2 * h, 2 * blocks * B), F32),
        in_specs=[vmem] * 10,
        out_specs=pl.BlockSpec(memory_space=pl.ANY),
        scratch_shapes=[
            *[pltpu.VMEM((l[1] + 1, B, B), F32) for l in levels[1:]],
            pltpu.VMEM((2, 2 * blocks, 16 * (strip_rows(top) // 8), B), F32),
            pltpu.VMEM((2 * blocks, B, B), F32),
            pltpu.VMEM((long, B), F32),
            pltpu.VMEM((B, B), F32),
            pltpu.VMEM(across[top][1:], F32),
            pltpu.SemaphoreType.DMA((2 * blocks,)),
            pltpu.SemaphoreType.DMA((2, 2 * blocks)),
        ],
        compiler_params=pltpu.CompilerParams(vmem_limit_bytes=12 * 2**20),
    )(*between)


def solution(mesh):
    return jax.shard_map(
        per_device,
        mesh=mesh,
        in_specs=(
            P("rows", "cols"),
            P(None, "rows", "cols"),
            P(None, "rows", "cols"),
            P(None, "rows", "cols"),
            P(None, "rows", "cols"),
        ),
        out_specs=P("rows", "cols"),
        check_vma=False,
    )
```

```python
import functools

import jax
import jax.numpy as jnp
from jax import lax
from jax.experimental import pallas as pl
from jax.experimental.pallas import tpu as pltpu
from jax.sharding import PartitionSpec as P

ALPHA = -1.586134342059924
BETA = -0.052980118572961
GAMMA = 0.882911075530934
DELTA = 0.443506852043971
SCALE = 1.149604398860241
UP2 = SCALE * SCALE
DOWN2 = 1.0 / (SCALE * SCALE)

B = 128
HALO = 8
F32 = jnp.float32
MESH = pl.DeviceIdType.MESH

DIRS = ((-1, 0), (1, 0), (0, -1), (0, 1), (-1, -1), (-1, 1), (1, -1), (1, 1))


def iota(axis):
    return lax.broadcasted_iota(jnp.int32, (8, B), axis)


def turn(x, amount):
    amount = amount % B
    return x if amount == 0 else pltpu.roll(x, amount, axis=1)


def row_blocks(level):
    return -(-level[2] // B)


def depth_of(levels, k):
    return 2 if k == len(levels) - 1 else 4


def row_plan(levels):
    plan, at = [], 0
    for k, (arrays, blocks, h) in enumerate(levels):
        for a in range(arrays):
            for b in range(blocks):
                plan.append((k, a, b, at))
                at += depth_of(levels, k)
    return plan, -(-at // 8) * 8


def column_plan(levels):
    plan, at = [], 0
    for k, level in enumerate(levels):
        for a in range(level[0]):
            for n in range(row_blocks(level)):
                plan.append((k, a, n, at))
                at += depth_of(levels, k)
    return plan, -(-at // 8) * 8


def stack_offsets(levels):
    offsets, at = [], 0
    for _, blocks, _ in levels:
        offsets.append(at)
        at += 8 * blocks
    return offsets


def lift_rows(count, s, r, dst):
    run = (count + 8) // 8

    def rows(ref, t):
        return ref[pl.ds(HALO - 4 + t, 8, stride=run), :]

    r0, s1, r1, s2 = {}, {}, {}, {}
    for t in range(-2, run + 2):
        r0[t] = rows(r, t)
        if t < -1:
            continue
        s1[t] = rows(s, t) - DELTA * (r0[t] + r0[t - 1])
        if t < 0:
            continue
        r1[t - 1] = r0[t - 1] - GAMMA * (s1[t - 1] + s1[t])
        if t < 1:
            continue
        n = t - 1
        s2[n] = s1[n] - BETA * (r1[n] + r1[n - 1])
        if n < run:
            dst[pl.ds(2 * n, 8, stride=2 * run), :] = s2[n]
        if n >= 1:
            dst[pl.ds(2 * n - 1, 8, stride=2 * run), :] = r1[n - 1] - ALPHA * (s2[n - 1] + s2[n])


def scaled(x, scale):
    return x if scale is None else x * scale


def turn_back(level, final, n, lifted, edge, dst):
    _, blocks, h = level
    count = min(B, h)
    at = pl.ds(HALO + n * B, count)
    for j in range(2 * blocks):
        dst[j, at, :] = lifted[pl.ds(HALO + j * B, B), :].T[:count]
    if not final:
        edge[0:8, :] = lifted[pl.ds(HALO + 2 * blocks * B, 8), :]
        edge[B - 8 : B, :] = lifted[0:8, :]
        dst[2 * blocks, at, :] = edge[...].T[:count]


def halo_transpose(levels, hn, cn, scale, dst):
    group = iota(1) // 8
    offsets = stack_offsets(levels)
    first = last = None
    for off, (_, blocks, _) in zip(offsets, levels):
        f, l = group == off // 8, group == off // 8 + blocks - 1
        first = f if first is None else first | f
        last = l if last is None else last | l
    t = scaled(hn[...].T, scale)
    ct = scaled(cn[...].T, scale)
    dst[pl.ds(HALO, B), :] = t
    dst[pl.ds(0, 8), :] = jnp.where(first, ct[B - 8 :], turn(t[B - 8 :], 8))
    dst[pl.ds(HALO + B, 8), :] = jnp.where(last, ct[:8], turn(t[:8], -8))


def halo_back(levels, which, lifted, edge, dsts):
    low = iota(1) < 64
    offsets = stack_offsets(levels)
    for j in range(2):
        y = lifted[pl.ds(HALO + j * B, B), :].T
        for k in which:
            _, blocks, h = levels[k]
            for b in range(blocks):
                tile = y[offsets[k] + 8 * b : offsets[k] + 8 * b + 8]
                dsts[k][2 * b + j, pl.ds(0, 8), :] = tile
                dsts[k][2 * b + j, pl.ds(HALO + h, 8), :] = tile
    which = [k for k in which if k < len(levels) - 1]
    if which:
        edge[0:8, :] = lifted[pl.ds(HALO + 2 * B, 8), :]
        edge[B - 8 : B, :] = lifted[0:8, :]
        y = edge[...].T
        for k in which:
            _, blocks, h = levels[k]
            end = offsets[k] + 8 * (blocks - 1)
            tile = jnp.where(low, y[end : end + 8], y[offsets[k] : offsets[k] + 8])
            dsts[k][2 * blocks, pl.ds(0, 8), :] = tile
            dsts[k][2 * blocks, pl.ds(HALO + h, 8), :] = tile


def exchange_kernel(levels, *refs):
    coarse, d4, d3, d2, d1 = refs[:5]
    ws, zs = refs[5:9], refs[9:13]
    zh, c4, ch = refs[13:16]
    ns, xs = refs[16:20], refs[20:24]
    (hn, cn, sh, rh, hd, lifted, edge, rows_out, cols_out, corners_out, rows_in, cols_in, corners_in,
     load_sem, send_sem, recv_sem) = refs[24:]
    nr, nc = lax.axis_size("rows"), lax.axis_size("cols")
    r, c = lax.axis_index("rows"), lax.axis_index("cols")
    top = len(levels) - 1

    def neighbour(step):
        return (lax.rem(r + step[0] + nr, nr), lax.rem(c + step[1] + nc, nc))

    barrier = pltpu.get_barrier_semaphore()
    for step in DIRS:
        pl.semaphore_signal(barrier, inc=1, device_id=neighbour(step), device_id_type=MESH)

    loads = []

    def load(src, dst):
        copy = pltpu.make_async_copy(src, dst, load_sem.at[len(loads)])
        copy.start()
        loads.append(copy)

    h = levels[0][2]
    load(coarse, ns[0].at[3, pl.ds(0, h), :])
    load(d4, ns[0].at[pl.ds(0, 3), pl.ds(0, h), :])
    for k, src in ((1, d3), (2, d2), (3, d1)):
        h = levels[k][2]
        for at in (pl.ds(0, 8), pl.ds(h - 8, 8)):
            load(src.at[:, at, :], ns[k].at[:, at, :])
    edge_loads = len(loads)
    for k, src in ((1, d3), (2, d2)):
        inner = pl.ds(8, levels[k][2] - 16)
        load(src.at[:, inner, :], ns[k].at[:, inner, :])
    _, blocks, h = levels[top]
    w = blocks * B
    inner = pl.ds(8, h - 16)
    for at in (pl.ds(0, B), pl.ds(w - B, B)):
        load(d1.at[:, inner, at], ns[top].at[:, inner, at])
    side_loads = len(loads)
    for a in range(3):
        at = pl.ds(B, w - 2 * B)
        load(d1.at[a, inner, at], ns[top].at[a, inner, at])

    def columns_of(k, a):
        return c4 if a == 3 else zs[k] if a == 0 else xs[k].at[a - 1]

    def transpose(k, a, n, b):
        scale = (None, None, DOWN2, UP2)[a]
        columns_of(k, a)[n, pl.ds(HALO + b * B, B), :] = scaled(
            ns[k][a, pl.ds(n * B, B), pl.ds(b * B, B)].T, scale)

    for copy in loads[:edge_loads]:
        copy.wait()
    rows, _ = row_plan(levels)
    for k, a, b, at in rows:
        depth, h = depth_of(levels, k), levels[k][2]
        here = pl.ds(b * B, B)
        rows_out[0, pl.ds(at, depth), :] = ns[k][a, pl.ds(0, depth), here]
        rows_out[1, pl.ds(at, depth), :] = ns[k][a, pl.ds(h - depth, depth), here]
    group = iota(1) // 4
    arrays = [(k, a) for k in range(top + 1) for a in range(levels[k][0])]
    for d in range(4):
        step = DIRS[4 + d]
        packed = jnp.zeros((8, B), F32)
        for q, (k, a) in enumerate(arrays):
            _, blocks, h = levels[k]
            at = pl.ds(0 if step[0] < 0 else h - 8, 8)
            if step[1] < 0:
                packed = jnp.where(group == q, turn(ns[k][a, at, pl.ds(0, B)], 4 * q), packed)
            else:
                packed = jnp.where(
                    group == 31 - q, turn(ns[k][a, at, pl.ds((blocks - 1) * B, B)], -4 * q), packed)
        corners_out[d] = packed

    sends = []
    for d, step in enumerate(DIRS):
        if d < 2:
            src, dst = rows_out.at[d], rows_in.at[d]
        elif d < 4:
            src, dst = cols_out.at[d - 2], cols_in.at[d - 2]
        else:
            src, dst = corners_out.at[d - 4], corners_in.at[d - 4]
        sends.append(pltpu.make_async_remote_copy(
            src_ref=src, dst_ref=dst, send_sem=send_sem.at[d], recv_sem=recv_sem.at[d],
            device_id=neighbour(step), device_id_type=MESH))

    def enter():
        pl.semaphore_wait(barrier, len(DIRS))
        for d in (4, 5, 6, 7, 0, 1):
            sends[d].start()

    early = jnp.logical_or(r < 1, c < 2)
    pl.when(jnp.logical_not(early))(enter)

    for copy in loads[edge_loads : edge_loads + 2]:
        copy.wait()
    for k in range(top):
        for a in range(levels[k][0]):
            for n in range(row_blocks(levels[k])):
                for b in range(levels[k][1]):
                    transpose(k, a, n, b)
    for copy in loads[edge_loads + 2 : side_loads]:
        copy.wait()
    for a in range(3):
        for n in range(row_blocks(levels[top])):
            for b in (0, levels[top][1] - 1):
                transpose(top, a, n, b)
    columns, _ = column_plan(levels)
    for k, a, n, at in columns:
        depth, w = depth_of(levels, k), levels[k][1] * B
        cols_out[0, pl.ds(at, depth), :] = columns_of(k, a)[n, pl.ds(HALO, depth), :]
        cols_out[1, pl.ds(at, depth), :] = columns_of(k, a)[n, pl.ds(HALO + w - depth, depth), :]

    pl.when(early)(enter)
    sends[2].start()
    sends[3].start()

    for copy in loads[side_loads:]:
        copy.wait()

    def middle(a, carry):
        for n in range(row_blocks(levels[top])):
            for b in range(1, levels[top][1] - 1):
                at = pl.ds(HALO + b * B, B)
                block = ns[top][a, pl.ds(n * B, B), pl.ds(b * B, B)].T
                xs[top][a - 1, n, at, :] = block * jnp.where(a == 2, F32(DOWN2), F32(1.0))
        return carry

    for n in range(row_blocks(levels[top])):
        for b in range(1, levels[top][1] - 1):
            transpose(top, 0, n, b)
    lax.fori_loop(1, 3, middle, 0)

    sends[2].wait()
    sends[3].wait()
    for k, a, n, at in columns:
        depth, w = depth_of(levels, k), levels[k][1] * B
        columns_of(k, a)[n, pl.ds(HALO + w, depth), :] = cols_in[0, pl.ds(at, depth), :]
        columns_of(k, a)[n, pl.ds(HALO - depth, depth), :] = cols_in[1, pl.ds(at, depth), :]
    for k in (3, 2, 1, 0):
        for n in range(row_blocks(levels[k])):
            part = lifted.at[n, pl.ds(0, 2 * levels[k][1] * B + 16), :]
            lift_rows(levels[k][1] * B, xs[k].at[0, n], xs[k].at[1, n], part)
            turn_back(levels[k], k == top, n, part, edge, ws[k])

    for d in (0, 1):
        sends[d].wait()
    offsets = stack_offsets(levels)
    for k, a, b, at in rows:
        depth, base = depth_of(levels, k), offsets[k] + 8 * b
        hn[a, pl.ds(base, depth), :] = rows_in[0, pl.ds(at, depth), :]
        hn[a, pl.ds(base + 8 - depth, depth), :] = rows_in[1, pl.ds(at, depth), :]
    for d in (4, 5, 6, 7):
        sends[d].wait()
    low, bottom = iota(1) < 64, iota(0) < 4
    for q, (k, a) in enumerate(arrays):
        tile = jnp.where(
            bottom,
            jnp.where(low, turn(corners_in[0], -4 * q), turn(corners_in[1], 4 * q)),
            jnp.where(low, turn(corners_in[2], -4 * q), turn(corners_in[3], 4 * q)))
        cn[a, pl.ds(offsets[k], 8), :] = tile
        cn[a, pl.ds(offsets[k] + 8 * (levels[k][1] - 1), 8), :] = tile
    halo_transpose(levels, hn.at[1], cn.at[1], None, sh)
    halo_transpose(levels, hn.at[2], cn.at[2], DOWN2, rh)
    halo_transpose(levels, hn.at[0], cn.at[0], None, zh)
    halo_transpose(levels, hn.at[3], cn.at[3], UP2, ch)
    lift_rows(B, sh, rh, hd)
    halo_back(levels, range(top + 1), hd, edge, ws)


def synthesis_kernel(levels, *refs):
    ws, zs = refs[:4], refs[4:8]
    zh, c4, ch = refs[8:11]
    out = refs[11]
    lows = (None,) + refs[12:15]
    image = refs[15]
    us, ts = refs[16:20], (c4,) + refs[20:23]
    hn, cn, th, hd, lifted, edge, even, odd, out_sem = refs[23:]
    top = len(levels) - 1
    offsets = stack_offsets(levels)
    bottom = iota(0) < 4

    for k, level in enumerate(levels):
        _, blocks, h = level
        w = blocks * B
        final = k == top
        n_rows = row_blocks(level)
        if k == 0:
            halo = ch
        else:
            halo = th
            low = lows[k]
            for b in range(blocks + 1):
                tile = jnp.where(bottom, low[b, pl.ds(HALO + h, 8), :], low[b, pl.ds(0, 8), :])
                if b < blocks:
                    hn[pl.ds(offsets[k] + 8 * b, 8), :] = tile
                else:
                    cn[pl.ds(offsets[k], 8), :] = tile
                    cn[pl.ds(offsets[k] + 8 * (blocks - 1), 8), :] = tile
            halo_transpose(levels, hn, cn, UP2, th)
            for n in range(n_rows):
                at = pl.ds(HALO + n * B, B)
                for b in range(blocks):
                    ts[k][n, pl.ds(HALO + b * B, B), :] = low[b, at, :].T * UP2
                side = low[blocks, at, :].T * UP2
                ts[k][n, pl.ds(0, 8), :] = side[B - 8 :]
                ts[k][n, pl.ds(HALO + w, 8), :] = side[:8]
        lift_rows(B, halo, zh, hd)
        halo_back(levels, (k,), hd, edge, {k: us[k]})
        for n in range(n_rows):
            part = lifted.at[n, pl.ds(0, 2 * w + 16), :]
            lift_rows(w, ts[k].at[n], zs[k].at[n], part)
            if not final:
                turn_back(level, final, n, part, edge, us[k])
        if not final:
            for j in range(2 * blocks + 1):
                lift_rows(h, us[k].at[j], ws[k].at[j], lows[k + 1].at[j])
        else:
            def fill(j, dst):
                dst[pl.ds(0, 8), :] = us[top][j, pl.ds(0, 8), :]
                dst[pl.ds(HALO + h, 8), :] = us[top][j, pl.ds(HALO + h, 8), :]
                at = pl.ds(pl.multiple_of(HALO + j * B, 8), B)
                for n in range(n_rows):
                    dst[pl.ds(HALO + n * B, B), :] = lifted[n, at, :].T

            def finish(j, src, dst):
                lift_rows(h, src, ws[top].at[j], dst)

            def send(j, slot, src):
                pltpu.make_async_copy(
                    src.at[j, pl.ds(HALO, 2 * h), :],
                    out.at[:, pl.ds(pl.multiple_of((2 * j + slot) * B, B), B)], out_sem.at[slot, j]).start()

            last = 2 * blocks - 1
            fill(0, even)

            def body(i, carry):
                j = 2 * i
                fill(j + 1, odd)
                finish(j, even, image.at[0, i])
                send(i, 0, image.at[0])
                fill(jnp.minimum(j + 2, last), even)
                finish(j + 1, odd, image.at[1, i])
                send(i, 1, image.at[1])
                return carry

            lax.fori_loop(0, blocks, body, 0)
            for i in range(blocks):
                for slot in range(2):
                    pltpu.make_async_copy(
                        image.at[slot, i, pl.ds(HALO, 2 * h), :],
                        out.at[:, pl.ds((2 * i + slot) * B, B)], out_sem.at[slot, i]).wait()


def per_device(coarse, d4, d3, d2, d1):
    levels = []
    for k, x in enumerate((d4, d3, d2, d1)):
        levels.append((4 if k == 0 else 3, x.shape[2] // B, x.shape[1]))
    levels = tuple(levels)
    top = len(levels) - 1
    _, row_count = row_plan(levels)
    _, col_count = column_plan(levels)
    hbm = pl.BlockSpec(memory_space=pltpu.HBM)
    vmem = pl.BlockSpec(memory_space=pltpu.VMEM)
    wide = [2 * b + (0 if k == top else 1) for k, (_, b, _) in enumerate(levels)]
    across = [(row_blocks(l), l[1] * B + 2 * HALO, B) for l in levels]
    strips = [(n, l[2] + 2 * HALO, B) for n, l in zip(wide, levels)]
    stack = (B + 2 * HALO, B)
    lifted = pltpu.VMEM((across[top][0], 2 * levels[top][1] * B + 2 * HALO, B), F32)
    between = pl.pallas_call(
        functools.partial(exchange_kernel, levels),
        out_shape=[pltpu.VMEM(s, F32) for s in strips + across + [stack, across[0], stack]],
        in_specs=[hbm] * 5,
        out_specs=[vmem] * 11,
        scratch_shapes=[
            *[pltpu.VMEM((a, max(B, h), b * B), F32) for a, b, h in levels],
            *[pltpu.VMEM((2,) + s, F32) for s in across],
            pltpu.VMEM((4, B, B), F32),
            pltpu.VMEM((4, B, B), F32),
            pltpu.VMEM(stack, F32),
            pltpu.VMEM(stack, F32),
            pltpu.VMEM((2 * B + 2 * HALO, B), F32),
            lifted,
            pltpu.VMEM((B, B), F32),
            pltpu.VMEM((2, row_count, B), F32),
            pltpu.VMEM((2, col_count, B), F32),
            pltpu.VMEM((4, 8, B), F32),
            pltpu.VMEM((2, row_count, B), F32),
            pltpu.VMEM((2, col_count, B), F32),
            pltpu.VMEM((4, 8, B), F32),
            pltpu.SemaphoreType.DMA((15,)),
            pltpu.SemaphoreType.DMA((8,)),
            pltpu.SemaphoreType.DMA((8,)),
        ],
        compiler_params=pltpu.CompilerParams(
            collective_id=0, has_side_effects=True, vmem_limit_bytes=26 * 2**20),
    )(*[pltpu.with_memory_space_constraint(x, pltpu.HBM) for x in (coarse, d4, d3, d2, d1)])
    blocks, h = levels[top][1], levels[top][2]
    return pl.pallas_call(
        functools.partial(synthesis_kernel, levels),
        out_shape=jax.ShapeDtypeStruct((2 * h, 2 * blocks * B), F32),
        in_specs=[vmem] * 11,
        out_specs=pl.BlockSpec(memory_space=pl.ANY),
        scratch_shapes=[
            *[pltpu.VMEM((levels[k][1] + 1, levels[k][2] + 2 * HALO, B), F32) for k in (1, 2, 3)],
            pltpu.VMEM((2, blocks, 2 * h + 2 * HALO, B), F32),
            *[pltpu.VMEM(s, F32) for s in strips],
            *[pltpu.VMEM(s, F32) for s in across[1:]],
            pltpu.VMEM((B, B), F32),
            pltpu.VMEM((B, B), F32),
            pltpu.VMEM(stack, F32),
            pltpu.VMEM((2 * B + 2 * HALO, B), F32),
            lifted,
            pltpu.VMEM((B, B), F32),
            pltpu.VMEM(strips[top][1:], F32),
            pltpu.VMEM(strips[top][1:], F32),
            pltpu.SemaphoreType.DMA((2, blocks)),
        ],
        compiler_params=pltpu.CompilerParams(vmem_limit_bytes=28 * 2**20),
    )(*between)


def solution(mesh):
    return jax.shard_map(
        per_device,
        mesh=mesh,
        in_specs=(
            P("rows", "cols"),
            P(None, "rows", "cols"),
            P(None, "rows", "cols"),
            P(None, "rows", "cols"),
            P(None, "rows", "cols"),
        ),
        out_specs=P("rows", "cols"),
        check_vma=False,
    )
```

```python
import functools

import jax
import jax.numpy as jnp
from jax import lax
from jax.experimental import pallas as pl
from jax.experimental.pallas import tpu as pltpu
from jax.sharding import PartitionSpec as P

ALPHA = -1.586134342059924
BETA = -0.052980118572961
GAMMA = 0.882911075530934
DELTA = 0.443506852043971
SCALE = 1.149604398860241
UP2 = SCALE * SCALE
DOWN2 = 1.0 / (SCALE * SCALE)

B = 128
HALO = 8
F32 = jnp.float32
MESH = pl.DeviceIdType.MESH

DIRS = ((-1, 0), (1, 0), (0, -1), (0, 1), (-1, -1), (-1, 1), (1, -1), (1, 1))


def iota(axis):
    return lax.broadcasted_iota(jnp.int32, (8, B), axis)


def turn(x, amount):
    amount = amount % B
    return x if amount == 0 else pltpu.roll(x, amount, axis=1)


def row_blocks(level):
    return -(-level[2] // B)


def depth_of(levels, k):
    return 2 if k == len(levels) - 1 else 4


def row_plan(levels):
    plan, at = [], 0
    for k, (arrays, blocks, h) in enumerate(levels):
        for a in range(arrays):
            for b in range(blocks):
                plan.append((k, a, b, at))
                at += depth_of(levels, k)
    return plan, -(-at // 8) * 8


def column_plan(levels):
    plan, at = [], 0
    for k, level in enumerate(levels):
        for a in range(level[0]):
            for n in range(row_blocks(level)):
                plan.append((k, a, n, at))
                at += depth_of(levels, k)
    return plan, -(-at // 8) * 8


def stack_offsets(levels):
    offsets, at = [], 0
    for _, blocks, _ in levels:
        offsets.append(at)
        at += 8 * blocks
    return offsets


def lift_rows(count, s, r, dst):
    lift_runs((count + 8) // 8, s, HALO - 4, r, HALO - 4, dst)


def lift_runs(run, s, s_at, r, r_at, dst):
    def rows(ref, t):
        at = s_at if ref is s else r_at
        return ref[pl.ds(at + t, 8, stride=run), :]

    r0, s1, r1, s2 = {}, {}, {}, {}
    for t in range(-2, run + 2):
        r0[t] = rows(r, t)
        if t < -1:
            continue
        s1[t] = rows(s, t) - DELTA * (r0[t] + r0[t - 1])
        if t < 0:
            continue
        r1[t - 1] = r0[t - 1] - GAMMA * (s1[t - 1] + s1[t])
        if t < 1:
            continue
        n = t - 1
        s2[n] = s1[n] - BETA * (r1[n] + r1[n - 1])
        if n < run:
            dst[pl.ds(2 * n, 8, stride=2 * run), :] = s2[n]
        if n >= 1:
            dst[pl.ds(2 * n - 1, 8, stride=2 * run), :] = r1[n - 1] - ALPHA * (s2[n - 1] + s2[n])


def scaled(x, scale):
    return x if scale is None else x * scale


def turn_back(level, n, lifted, dst, which):
    count = min(B, level[2])
    at = pl.ds(HALO + n * B, count)
    for j in which:
        dst[j, at, :] = lifted[pl.ds(HALO + j * B, B), :].T[:count]


def turn_back_side(level, n, lifted, edge, dst):
    _, blocks, h = level
    count = min(B, h)
    edge[0:8, :] = lifted[pl.ds(HALO + 2 * blocks * B, 8), :]
    edge[B - 8 : B, :] = lifted[0:8, :]
    dst[2 * blocks, pl.ds(HALO + n * B, count), :] = edge[...].T[:count]


def halo_transpose(levels, hn, cn, scale, dst):
    group = iota(1) // 8
    offsets = stack_offsets(levels)
    first = last = None
    for off, (_, blocks, _) in zip(offsets, levels):
        f, l = group == off // 8, group == off // 8 + blocks - 1
        first = f if first is None else first | f
        last = l if last is None else last | l
    t = scaled(hn[...].T, scale)
    ct = scaled(cn[...].T, scale)
    dst[pl.ds(HALO, B), :] = t
    dst[pl.ds(0, 8), :] = jnp.where(first, ct[B - 8 :], turn(t[B - 8 :], 8))
    dst[pl.ds(HALO + B, 8), :] = jnp.where(last, ct[:8], turn(t[:8], -8))


def halo_back(levels, which, lifted, edge, dsts):
    low = iota(1) < 64
    offsets = stack_offsets(levels)
    for j in range(2):
        y = lifted[pl.ds(HALO + j * B, B), :].T
        for k in which:
            _, blocks, h = levels[k]
            for b in range(blocks):
                tile = y[offsets[k] + 8 * b : offsets[k] + 8 * b + 8]
                dsts[k][2 * b + j, pl.ds(0, 8), :] = tile
                dsts[k][2 * b + j, pl.ds(HALO + h, 8), :] = tile
    which = [k for k in which if k < len(levels) - 1]
    if which:
        edge[0:8, :] = lifted[pl.ds(HALO + 2 * B, 8), :]
        edge[B - 8 : B, :] = lifted[0:8, :]
        y = edge[...].T
        for k in which:
            _, blocks, h = levels[k]
            end = offsets[k] + 8 * (blocks - 1)
            tile = jnp.where(low, y[end : end + 8], y[offsets[k] : offsets[k] + 8])
            dsts[k][2 * blocks, pl.ds(0, 8), :] = tile
            dsts[k][2 * blocks, pl.ds(HALO + h, 8), :] = tile


def exchange_kernel(levels, *refs):
    coarse, d4, d3, d2, d1 = refs[:5]
    ws, zs = refs[5:9], refs[9:13]
    zh, c4, ch = refs[13:16]
    ns, xs = refs[16:20], refs[20:24]
    ls = refs[24:28]
    (hn, cn, sh, rh, hd, edge, rows_out, cols_out, corners_out, rows_in, cols_in, corners_in,
     load_sem, send_sem, recv_sem) = refs[28:]
    nr, nc = lax.axis_size("rows"), lax.axis_size("cols")
    r, c = lax.axis_index("rows"), lax.axis_index("cols")
    top = len(levels) - 1

    def neighbour(step):
        return (lax.rem(r + step[0] + nr, nr), lax.rem(c + step[1] + nc, nc))

    barrier = pltpu.get_barrier_semaphore()
    for step in DIRS:
        pl.semaphore_signal(barrier, inc=1, device_id=neighbour(step), device_id_type=MESH)

    loads = []

    def load(src, dst):
        copy = pltpu.make_async_copy(src, dst, load_sem.at[len(loads)])
        copy.start()
        loads.append(copy)

    h = levels[0][2]
    load(coarse, ns[0].at[3, pl.ds(0, h), :])
    load(d4, ns[0].at[pl.ds(0, 3), pl.ds(0, h), :])
    for k, src in ((1, d3), (2, d2), (3, d1)):
        h = levels[k][2]
        for at in (pl.ds(0, 8), pl.ds(h - 8, 8)):
            load(src.at[:, at, :], ns[k].at[:, at, :])
    edge_loads = len(loads)
    for k, src in ((1, d3), (2, d2)):
        inner = pl.ds(8, levels[k][2] - 16)
        load(src.at[:, inner, :], ns[k].at[:, inner, :])
    _, blocks, h = levels[top]
    w = blocks * B
    inner = pl.ds(8, h - 16)
    for at in (pl.ds(0, B), pl.ds(w - B, B)):
        load(d1.at[:, inner, at], ns[top].at[:, inner, at])
    side_loads = len(loads)
    for a in range(3):
        at = pl.ds(B, w - 2 * B)
        load(d1.at[a, inner, at], ns[top].at[a, inner, at])

    def columns_of(k, a):
        return c4 if a == 3 else zs[k] if a == 0 else xs[k].at[a - 1]

    def transpose(k, a, n, b):
        scale = (None, None, DOWN2, UP2)[a]
        columns_of(k, a)[n, pl.ds(HALO + b * B, B), :] = scaled(
            ns[k][a, pl.ds(n * B, B), pl.ds(b * B, B)].T, scale)

    for copy in loads[:edge_loads]:
        copy.wait()
    rows, _ = row_plan(levels)
    for k, a, b, at in rows:
        depth, h = depth_of(levels, k), levels[k][2]
        here = pl.ds(b * B, B)
        rows_out[0, pl.ds(at, depth), :] = ns[k][a, pl.ds(0, depth), here]
        rows_out[1, pl.ds(at, depth), :] = ns[k][a, pl.ds(h - depth, depth), here]
    group = iota(1) // 4
    arrays = [(k, a) for k in range(top + 1) for a in range(levels[k][0])]
    for d in range(4):
        step = DIRS[4 + d]
        packed = jnp.zeros((8, B), F32)
        for q, (k, a) in enumerate(arrays):
            _, blocks, h = levels[k]
            at = pl.ds(0 if step[0] < 0 else h - 8, 8)
            if step[1] < 0:
                packed = jnp.where(group == q, turn(ns[k][a, at, pl.ds(0, B)], 4 * q), packed)
            else:
                packed = jnp.where(
                    group == 31 - q, turn(ns[k][a, at, pl.ds((blocks - 1) * B, B)], -4 * q), packed)
        corners_out[d] = packed

    sends = []
    for d, step in enumerate(DIRS):
        if d < 2:
            src, dst = rows_out.at[d], rows_in.at[d]
        elif d < 4:
            src, dst = cols_out.at[d - 2], cols_in.at[d - 2]
        else:
            src, dst = corners_out.at[d - 4], corners_in.at[d - 4]
        sends.append(pltpu.make_async_remote_copy(
            src_ref=src, dst_ref=dst, send_sem=send_sem.at[d], recv_sem=recv_sem.at[d],
            device_id=neighbour(step), device_id_type=MESH))

    def enter():
        pl.semaphore_wait(barrier, len(DIRS))
        for d in (4, 5, 6, 7, 0, 1):
            sends[d].start()

    early = jnp.logical_or(r < 1, c < 1)
    pl.when(jnp.logical_not(early))(enter)

    for copy in loads[edge_loads:side_loads]:
        copy.wait()

    def blocks_of(k, which):
        blocks = levels[k][1]
        sides = sorted({0, blocks - 1})
        return sides if which == "sides" else range(1, blocks - 1)

    for k in range(top + 1):
        for a in range(levels[k][0]):
            for n in range(row_blocks(levels[k])):
                for b in blocks_of(k, "sides"):
                    transpose(k, a, n, b)
    columns, _ = column_plan(levels)
    for k, a, n, at in columns:
        depth, w = depth_of(levels, k), levels[k][1] * B
        cols_out[0, pl.ds(at, depth), :] = columns_of(k, a)[n, pl.ds(HALO, depth), :]
        cols_out[1, pl.ds(at, depth), :] = columns_of(k, a)[n, pl.ds(HALO + w - depth, depth), :]

    def enter_sides():
        sends[2].start()
        sends[3].start()

    pl.when(jnp.logical_not(early))(enter_sides)

    for k in range(top):
        for a in range(levels[k][0]):
            for n in range(row_blocks(levels[k])):
                for b in blocks_of(k, "middle"):
                    transpose(k, a, n, b)
    for copy in loads[side_loads:]:
        copy.wait()

    def middle(a, carry):
        for n in range(row_blocks(levels[top])):
            for b in blocks_of(top, "middle"):
                at = pl.ds(HALO + b * B, B)
                block = ns[top][a, pl.ds(n * B, B), pl.ds(b * B, B)].T
                xs[top][a - 1, n, at, :] = block * jnp.where(a == 2, F32(DOWN2), F32(1.0))
        return carry

    for n in range(row_blocks(levels[top])):
        for b in blocks_of(top, "middle"):
            transpose(top, 0, n, b)
    lax.fori_loop(1, 3, middle, 0)
    for k in (3, 2, 1, 0):
        for n in range(row_blocks(levels[k])):
            lift_rows(levels[k][1] * B, xs[k].at[0, n], xs[k].at[1, n], ls[k].at[n])
            turn_back(levels[k], n, ls[k].at[n], ws[k], range(1, 2 * levels[k][1] - 1))

    def enter_late():
        enter()
        enter_sides()

    pl.when(early)(enter_late)

    sends[2].wait()
    sends[3].wait()
    for k, a, n, at in columns:
        depth, w = depth_of(levels, k), levels[k][1] * B
        columns_of(k, a)[n, pl.ds(HALO + w, depth), :] = cols_in[0, pl.ds(at, depth), :]
        columns_of(k, a)[n, pl.ds(HALO - depth, depth), :] = cols_in[1, pl.ds(at, depth), :]
    for k in (3, 2, 1, 0):
        blocks = levels[k][1]
        w = blocks * B
        for n in range(row_blocks(levels[k])):
            part = ls[k].at[n]
            for at in (HALO - 4, HALO + w - 4):
                lift_runs(1, xs[k].at[0, n], at, xs[k].at[1, n], at, ls[k].at[n, pl.ds(2 * at - HALO, 16), :])
            turn_back(levels[k], n, part, ws[k], (0, 2 * blocks - 1))
            if k < top:
                turn_back_side(levels[k], n, part, edge, ws[k])

    for d in (0, 1):
        sends[d].wait()
    offsets = stack_offsets(levels)
    for k, a, b, at in rows:
        depth, base = depth_of(levels, k), offsets[k] + 8 * b
        hn[a, pl.ds(base, depth), :] = rows_in[0, pl.ds(at, depth), :]
        hn[a, pl.ds(base + 8 - depth, depth), :] = rows_in[1, pl.ds(at, depth), :]
    for d in (4, 5, 6, 7):
        sends[d].wait()
    low, bottom = iota(1) < 64, iota(0) < 4
    for q, (k, a) in enumerate(arrays):
        tile = jnp.where(
            bottom,
            jnp.where(low, turn(corners_in[0], -4 * q), turn(corners_in[1], 4 * q)),
            jnp.where(low, turn(corners_in[2], -4 * q), turn(corners_in[3], 4 * q)))
        cn[a, pl.ds(offsets[k], 8), :] = tile
        cn[a, pl.ds(offsets[k] + 8 * (levels[k][1] - 1), 8), :] = tile
    halo_transpose(levels, hn.at[1], cn.at[1], None, sh)
    halo_transpose(levels, hn.at[2], cn.at[2], DOWN2, rh)
    halo_transpose(levels, hn.at[0], cn.at[0], None, zh)
    halo_transpose(levels, hn.at[3], cn.at[3], UP2, ch)
    lift_rows(B, sh, rh, hd)
    halo_back(levels, range(top + 1), hd, edge, ws)


def synthesis_kernel(levels, *refs):
    ws, zs = refs[:4], refs[4:8]
    zh, c4, ch = refs[8:11]
    out = refs[11]
    lows = (None,) + refs[12:15]
    image = refs[15]
    us, ts = refs[16:20], (c4,) + refs[20:23]
    hn, cn, th, hd, lifted, edge, out_sem = refs[23:]
    top = len(levels) - 1
    offsets = stack_offsets(levels)
    bottom = iota(0) < 4

    for k, level in enumerate(levels):
        _, blocks, h = level
        w = blocks * B
        final = k == top
        n_rows = row_blocks(level)
        def columns_from(n):
            at = pl.ds(HALO + n * B, B)
            for b in range(blocks):
                ts[k][n, pl.ds(HALO + b * B, B), :] = low[b, at, :].T * UP2
            side = low[blocks, at, :].T * UP2
            ts[k][n, pl.ds(0, 8), :] = side[B - 8 :]
            ts[k][n, pl.ds(HALO + w, 8), :] = side[:8]

        if k == 0:
            halo = ch
        else:
            halo = th
            low = lows[k]
            for b in range(blocks + 1):
                tile = jnp.where(bottom, low[b, pl.ds(HALO + h, 8), :], low[b, pl.ds(0, 8), :])
                if b < blocks:
                    hn[pl.ds(offsets[k] + 8 * b, 8), :] = tile
                else:
                    cn[pl.ds(offsets[k], 8), :] = tile
                    cn[pl.ds(offsets[k] + 8 * (blocks - 1), 8), :] = tile
            halo_transpose(levels, hn, cn, UP2, th)
        lift_rows(B, halo, zh, hd)
        halo_back(levels, (k,), hd, edge, {k: us[k]})
        if not final:
            for n in range(n_rows):
                if k > 0:
                    columns_from(n)
                part = lifted.at[n, pl.ds(0, 2 * w + 16), :]
                lift_rows(w, ts[k].at[n], zs[k].at[n], part)
                turn_back(level, n, part, us[k], range(2 * blocks))
                turn_back_side(level, n, part, edge, us[k])
            for j in range(2 * blocks + 1):
                lift_rows(h, us[k].at[j], ws[k].at[j], lows[k + 1].at[j])
            continue

        half = n_rows // 2
        run = half * B // 8 - 1
        seam = 8 * run - 4
        runs = (run, (h + 4 - seam) // 8)
        ats = (HALO - 4, HALO + seam)
        dsts = (pl.ds(0, 16 * run), pl.ds(16 * run, 16 * runs[1]))
        outs = (pl.ds(0, 2 * seam), pl.ds(2 * seam, 2 * (h - seam)))

        def image_copy(part, j):
            row = (HALO, HALO + 2 * seam)[part]
            return pltpu.make_async_copy(
                image.at[j, pl.ds(row, outs[part].size), :],
                out.at[outs[part], pl.ds(j * B, B)], out_sem.at[part, j])

        last = 2 * blocks - 1

        for part in range(2):
            these = (range(half), range(half, n_rows))[part]
            for n in these:
                columns_from(n)
                lift_rows(w, ts[k].at[n], zs[k].at[n], lifted.at[n])

            def fill(j, these=these):
                for n in these:
                    us[top][j, pl.ds(HALO + n * B, B), :] = lifted[n, pl.ds(HALO + j * B, B), :].T

            fill(0)
            for j in range(2 * blocks):
                if j < last:
                    fill(j + 1)
                lift_runs(runs[part], us[top].at[j], ats[part], ws[top].at[j], ats[part],
                          image.at[j, dsts[part], :])
                image_copy(part, j).start()

        for part in range(2):
            for j in range(2 * blocks):
                image_copy(part, j).wait()


def per_device(coarse, d4, d3, d2, d1):
    levels = []
    for k, x in enumerate((d4, d3, d2, d1)):
        levels.append((4 if k == 0 else 3, x.shape[2] // B, x.shape[1]))
    levels = tuple(levels)
    top = len(levels) - 1
    _, row_count = row_plan(levels)
    _, col_count = column_plan(levels)
    hbm = pl.BlockSpec(memory_space=pltpu.HBM)
    vmem = pl.BlockSpec(memory_space=pltpu.VMEM)
    wide = [2 * b + (0 if k == top else 1) for k, (_, b, _) in enumerate(levels)]
    across = [(row_blocks(l), l[1] * B + 2 * HALO, B) for l in levels]
    strips = [(n, l[2] + 2 * HALO, B) for n, l in zip(wide, levels)]
    stack = (B + 2 * HALO, B)
    lifted = pltpu.VMEM((across[top][0], 2 * levels[top][1] * B + 2 * HALO, B), F32)
    between = pl.pallas_call(
        functools.partial(exchange_kernel, levels),
        out_shape=[pltpu.VMEM(s, F32) for s in strips + across + [stack, across[0], stack]],
        in_specs=[hbm] * 5,
        out_specs=[vmem] * 11,
        scratch_shapes=[
            *[pltpu.VMEM((a, max(B, h), b * B), F32) for a, b, h in levels],
            *[pltpu.VMEM((2,) + s, F32) for s in across],
            *[pltpu.VMEM((n, 2 * l[1] * B + 2 * HALO, B), F32) for (n, _, _), l in zip(across, levels)],
            pltpu.VMEM((4, B, B), F32),
            pltpu.VMEM((4, B, B), F32),
            pltpu.VMEM(stack, F32),
            pltpu.VMEM(stack, F32),
            pltpu.VMEM((2 * B + 2 * HALO, B), F32),
            pltpu.VMEM((B, B), F32),
            pltpu.VMEM((2, row_count, B), F32),
            pltpu.VMEM((2, col_count, B), F32),
            pltpu.VMEM((4, 8, B), F32),
            pltpu.VMEM((2, row_count, B), F32),
            pltpu.VMEM((2, col_count, B), F32),
            pltpu.VMEM((4, 8, B), F32),
            pltpu.SemaphoreType.DMA((15,)),
            pltpu.SemaphoreType.DMA((8,)),
            pltpu.SemaphoreType.DMA((8,)),
        ],
        compiler_params=pltpu.CompilerParams(
            collective_id=0, has_side_effects=True, vmem_limit_bytes=30 * 2**20),
    )(*[pltpu.with_memory_space_constraint(x, pltpu.HBM) for x in (coarse, d4, d3, d2, d1)])
    blocks, h = levels[top][1], levels[top][2]
    return pl.pallas_call(
        functools.partial(synthesis_kernel, levels),
        out_shape=jax.ShapeDtypeStruct((2 * h, 2 * blocks * B), F32),
        in_specs=[vmem] * 11,
        out_specs=pl.BlockSpec(memory_space=pl.ANY),
        scratch_shapes=[
            *[pltpu.VMEM((levels[k][1] + 1, levels[k][2] + 2 * HALO, B), F32) for k in (1, 2, 3)],
            pltpu.VMEM((2 * blocks, 2 * h + 2 * HALO, B), F32),
            *[pltpu.VMEM(s, F32) for s in strips],
            *[pltpu.VMEM(s, F32) for s in across[1:]],
            pltpu.VMEM((B, B), F32),
            pltpu.VMEM((B, B), F32),
            pltpu.VMEM(stack, F32),
            pltpu.VMEM((2 * B + 2 * HALO, B), F32),
            lifted,
            pltpu.VMEM((B, B), F32),
            pltpu.SemaphoreType.DMA((2, 2 * blocks)),
        ],
        compiler_params=pltpu.CompilerParams(vmem_limit_bytes=28 * 2**20),
    )(*between)


def solution(mesh):
    return jax.shard_map(
        per_device,
        mesh=mesh,
        in_specs=(
            P("rows", "cols"),
            P(None, "rows", "cols"),
            P(None, "rows", "cols"),
            P(None, "rows", "cols"),
            P(None, "rows", "cols"),
        ),
        out_specs=P("rows", "cols"),
        check_vma=False,
    )
```

```python
import functools

import jax
import jax.numpy as jnp
from jax import lax
from jax.experimental import pallas as pl
from jax.experimental.pallas import tpu as pltpu
from jax.sharding import PartitionSpec as P

ALPHA = -1.586134342059924
BETA = -0.052980118572961
GAMMA = 0.882911075530934
DELTA = 0.443506852043971
SCALE = 1.149604398860241
UP2 = SCALE * SCALE
DOWN2 = 1.0 / (SCALE * SCALE)

B = 128
HALO = 8
F32 = jnp.float32
MESH = pl.DeviceIdType.MESH

DIRS = ((-1, 0), (1, 0), (0, -1), (0, 1), (-1, -1), (-1, 1), (1, -1), (1, 1))


def iota(axis):
    return lax.broadcasted_iota(jnp.int32, (8, B), axis)


def turn(x, amount):
    amount = amount % B
    return x if amount == 0 else pltpu.roll(x, amount, axis=1)


def row_blocks(level):
    return -(-level[2] // B)


def depth_of(levels, k):
    return 2 if k == len(levels) - 1 else 4


def row_plan(levels):
    plan, at = [], 0
    for k, (arrays, blocks, h) in enumerate(levels):
        for a in range(arrays):
            for b in range(blocks):
                plan.append((k, a, b, at))
                at += depth_of(levels, k)
    return plan, -(-at // 8) * 8


def column_plan(levels):
    plan, at = [], 0
    for k, level in enumerate(levels):
        for a in range(level[0]):
            for n in range(row_blocks(level)):
                plan.append((k, a, n, at))
                at += depth_of(levels, k)
    return plan, -(-at // 8) * 8


def stack_offsets(levels):
    offsets, at = [], 0
    for _, blocks, _ in levels:
        offsets.append(at)
        at += 8 * blocks
    return offsets


def lift_rows(count, s, r, dst):
    lift_runs((count + 8) // 8, s, HALO - 4, r, HALO - 4, dst)


def lift_runs(run, s, s_at, r, r_at, dst):
    def rows(ref, t):
        at = s_at if ref is s else r_at
        return ref[pl.ds(at + t, 8, stride=run), :]

    r0, s1, r1, s2 = {}, {}, {}, {}
    for t in range(-2, run + 2):
        r0[t] = rows(r, t)
        if t < -1:
            continue
        s1[t] = rows(s, t) - DELTA * (r0[t] + r0[t - 1])
        if t < 0:
            continue
        r1[t - 1] = r0[t - 1] - GAMMA * (s1[t - 1] + s1[t])
        if t < 1:
            continue
        n = t - 1
        s2[n] = s1[n] - BETA * (r1[n] + r1[n - 1])
        if n < run:
            dst[pl.ds(2 * n, 8, stride=2 * run), :] = s2[n]
        if n >= 1:
            dst[pl.ds(2 * n - 1, 8, stride=2 * run), :] = r1[n - 1] - ALPHA * (s2[n - 1] + s2[n])


def scaled(x, scale):
    return x if scale is None else x * scale


def turn_back(level, n, lifted, dst, which):
    count = min(B, level[2])
    at = pl.ds(HALO + n * B, count)
    for j in which:
        dst[j, at, :] = lifted[pl.ds(HALO + j * B, B), :].T[:count]


def turn_back_side(level, n, lifted, edge, dst):
    _, blocks, h = level
    count = min(B, h)
    edge[0:8, :] = lifted[pl.ds(HALO + 2 * blocks * B, 8), :]
    edge[B - 8 : B, :] = lifted[0:8, :]
    dst[2 * blocks, pl.ds(HALO + n * B, count), :] = edge[...].T[:count]


def halo_transpose(levels, hn, cn, scale, dst):
    group = iota(1) // 8
    offsets = stack_offsets(levels)
    first = last = None
    for off, (_, blocks, _) in zip(offsets, levels):
        f, l = group == off // 8, group == off // 8 + blocks - 1
        first = f if first is None else first | f
        last = l if last is None else last | l
    t = scaled(hn[...].T, scale)
    ct = scaled(cn[...].T, scale)
    dst[pl.ds(HALO, B), :] = t
    dst[pl.ds(0, 8), :] = jnp.where(first, ct[B - 8 :], turn(t[B - 8 :], 8))
    dst[pl.ds(HALO + B, 8), :] = jnp.where(last, ct[:8], turn(t[:8], -8))


def halo_back(levels, which, lifted, edge, dsts):
    low = iota(1) < 64
    offsets = stack_offsets(levels)
    for j in range(2):
        y = lifted[pl.ds(HALO + j * B, B), :].T
        for k in which:
            _, blocks, h = levels[k]
            for b in range(blocks):
                tile = y[offsets[k] + 8 * b : offsets[k] + 8 * b + 8]
                dsts[k][2 * b + j, pl.ds(0, 8), :] = tile
                dsts[k][2 * b + j, pl.ds(HALO + h, 8), :] = tile
    which = [k for k in which if k < len(levels) - 1]
    if which:
        edge[0:8, :] = lifted[pl.ds(HALO + 2 * B, 8), :]
        edge[B - 8 : B, :] = lifted[0:8, :]
        y = edge[...].T
        for k in which:
            _, blocks, h = levels[k]
            end = offsets[k] + 8 * (blocks - 1)
            tile = jnp.where(low, y[end : end + 8], y[offsets[k] : offsets[k] + 8])
            dsts[k][2 * blocks, pl.ds(0, 8), :] = tile
            dsts[k][2 * blocks, pl.ds(HALO + h, 8), :] = tile


def strip_rows(k):
    return (16, 16, 24, 40)[k]


def strip_sides(levels, k, main, ct, dst):
    _, blocks, h = levels[k]
    keep, off = strip_rows(k), stack_offsets(levels)[k]
    lane = iota(1)
    n = row_blocks(levels[k])
    start = h - keep - B * (n - 1)
    w = blocks * B
    for at, corner, shift in ((0, ct[B - 8 :], off), (HALO + w, ct[:8], off + 8 * (blocks - 1))):
        here = pl.ds(at, 8)
        dst[here, :] = jnp.where(
            lane < 8, turn(corner, -shift),
            jnp.where(
                lane < 8 + keep, turn(main[0, here, :], 8),
                jnp.where(lane < 8 + 2 * keep, turn(main[n - 1, here, :], 8 + keep - start),
                          turn(corner, 8 + 2 * keep - shift))))


def at_of(levels, k, a, b):
    return b if a == 3 else 1 + sum(l[1] for l in levels[:k]) + b


def side_takes(levels, k):
    if k == len(levels) - 1:
        return 64, 8, 72
    take = 8 + strip_rows(k + 1)
    return take, 0, take


def exchange_kernel(levels, *refs):
    coarse, d4, d3, d2, d1 = refs[:5]
    ws, zts, ct_out, image = refs[5:9], refs[9:13], refs[13], refs[14]
    zs, c4, wcs = refs[15:19], refs[19], refs[20:24]
    ns, xs, ls, us = refs[24:28], refs[28:32], refs[32:36], refs[36:40]
    lows, ts = (None,) + refs[40:43], (c4,) + refs[43:46]
    (hn, cn, sh, rh, hd, lifted, edge, ds, even, odd, rows_out, cols_out, corners_out,
     rows_in, cols_in, corners_in, load_sem, send_sem, recv_sem) = refs[46:]
    nr, nc = lax.axis_size("rows"), lax.axis_size("cols")
    r, c = lax.axis_index("rows"), lax.axis_index("cols")
    top = len(levels) - 1

    def neighbour(step):
        return (lax.rem(r + step[0] + nr, nr), lax.rem(c + step[1] + nc, nc))

    barrier = pltpu.get_barrier_semaphore()
    for step in DIRS:
        pl.semaphore_signal(barrier, inc=1, device_id=neighbour(step), device_id_type=MESH)

    loads = []

    def load(src, dst):
        copy = pltpu.make_async_copy(src, dst, load_sem.at[len(loads)])
        copy.start()
        loads.append(copy)

    h = levels[0][2]
    load(coarse, ns[0].at[3, pl.ds(0, h), :])
    load(d4, ns[0].at[pl.ds(0, 3), pl.ds(0, h), :])
    for k, src in ((1, d3), (2, d2), (3, d1)):
        h = levels[k][2]
        for at in (pl.ds(0, 8), pl.ds(h - 8, 8)):
            load(src.at[:, at, :], ns[k].at[:, at, :])
    edge_loads = len(loads)
    for k, src in ((1, d3), (2, d2)):
        inner = pl.ds(8, levels[k][2] - 16)
        load(src.at[:, inner, :], ns[k].at[:, inner, :])
    _, blocks, h = levels[top]
    w = blocks * B
    inner = pl.ds(8, h - 16)
    for at in (pl.ds(0, B), pl.ds(w - B, B)):
        load(d1.at[:, inner, at], ns[top].at[:, inner, at])
    side_loads = len(loads)
    for a in range(3):
        at = pl.ds(B, w - 2 * B)
        load(d1.at[a, inner, at], ns[top].at[a, inner, at])

    def columns_of(k, a):
        return c4 if a == 3 else zs[k] if a == 0 else xs[k].at[a - 1]

    def transpose(k, a, n, b):
        scale = (None, None, DOWN2, UP2)[a]
        columns_of(k, a)[n, pl.ds(HALO + b * B, B), :] = scaled(
            ns[k][a, pl.ds(n * B, B), pl.ds(b * B, B)].T, scale)

    for copy in loads[:edge_loads]:
        copy.wait()
    rows, _ = row_plan(levels)
    for k, a, b, at in rows:
        depth, h = depth_of(levels, k), levels[k][2]
        here = pl.ds(b * B, B)
        rows_out[0, pl.ds(at, depth), :] = ns[k][a, pl.ds(0, depth), here]
        rows_out[1, pl.ds(at, depth), :] = ns[k][a, pl.ds(h - depth, depth), here]
    group = iota(1) // 4
    arrays = [(k, a) for k in range(top + 1) for a in range(levels[k][0])]
    for d in range(4):
        step = DIRS[4 + d]
        packed = jnp.zeros((8, B), F32)
        for q, (k, a) in enumerate(arrays):
            _, blocks, h = levels[k]
            at = pl.ds(0 if step[0] < 0 else h - 8, 8)
            if step[1] < 0:
                packed = jnp.where(group == q, turn(ns[k][a, at, pl.ds(0, B)], 4 * q), packed)
            else:
                packed = jnp.where(
                    group == 31 - q, turn(ns[k][a, at, pl.ds((blocks - 1) * B, B)], -4 * q), packed)
        corners_out[d] = packed

    sends = []
    for d, step in enumerate(DIRS):
        if d < 2:
            src, dst = rows_out.at[d], rows_in.at[d]
        elif d < 4:
            src, dst = cols_out.at[d - 2], cols_in.at[d - 2]
        else:
            src, dst = corners_out.at[d - 4], corners_in.at[d - 4]
        sends.append(pltpu.make_async_remote_copy(
            src_ref=src, dst_ref=dst, send_sem=send_sem.at[d], recv_sem=recv_sem.at[d],
            device_id=neighbour(step), device_id_type=MESH))

    def enter():
        pl.semaphore_wait(barrier, len(DIRS))
        for d in (4, 5, 6, 7, 0, 1):
            sends[d].start()

    def enter_sides():
        sends[2].start()
        sends[3].start()

    def enter_all():
        enter()
        enter_sides()

    first_row = r < 1
    fourth = jnp.logical_and(first_row, c < 2)
    third = jnp.logical_or(
        jnp.logical_and(first_row, c >= 2),
        jnp.logical_and(jnp.logical_and(lax.rem(r, 4) < 1, r >= 1), c < 1))
    rest = jnp.logical_not(jnp.logical_or(third, fourth))
    quick = jnp.logical_or(jnp.logical_and(c >= 2, lax.rem(c, 2) < 1), c >= nc - 1)
    at_once = jnp.logical_and(rest, quick)
    second = jnp.logical_and(rest, jnp.logical_not(quick))
    pl.when(at_once)(enter)

    for copy in loads[edge_loads:side_loads]:
        copy.wait()

    def blocks_of(k, which):
        blocks = levels[k][1]
        sides = sorted({0, blocks - 1})
        return sides if which == "sides" else range(1, blocks - 1)

    for k in range(top + 1):
        for a in range(levels[k][0]):
            for n in range(row_blocks(levels[k])):
                for b in blocks_of(k, "sides"):
                    transpose(k, a, n, b)
    columns, _ = column_plan(levels)
    for k, a, n, at in columns:
        depth, w = depth_of(levels, k), levels[k][1] * B
        cols_out[0, pl.ds(at, depth), :] = columns_of(k, a)[n, pl.ds(HALO, depth), :]
        cols_out[1, pl.ds(at, depth), :] = columns_of(k, a)[n, pl.ds(HALO + w - depth, depth), :]

    pl.when(at_once)(enter_sides)
    pl.when(second)(enter_all)

    for k in range(top):
        for a in range(levels[k][0]):
            for n in range(row_blocks(levels[k])):
                for b in blocks_of(k, "middle"):
                    transpose(k, a, n, b)
    for copy in loads[side_loads:]:
        copy.wait()

    def middle(a, carry):
        for n in range(row_blocks(levels[top])):
            for b in blocks_of(top, "middle"):
                at = pl.ds(HALO + b * B, B)
                block = ns[top][a, pl.ds(n * B, B), pl.ds(b * B, B)].T
                xs[top][a - 1, n, at, :] = block * jnp.where(a == 2, F32(DOWN2), F32(1.0))
        return carry

    for n in range(row_blocks(levels[top])):
        for b in blocks_of(top, "middle"):
            transpose(top, 0, n, b)
    lax.fori_loop(1, 3, middle, 0)
    for k in (3, 2, 1, 0):
        for n in range(row_blocks(levels[k])):
            lift_rows(levels[k][1] * B, xs[k].at[0, n], xs[k].at[1, n], ls[k].at[n])
            turn_back(levels[k], n, ls[k].at[n], ws[k], range(2 * levels[k][1]))

    pl.when(third)(enter_all)

    for k, level in enumerate(levels):
        _, blocks, h = level
        w = blocks * B
        n_rows = row_blocks(level)
        for n in range(n_rows):
            if k > 0:
                for b in range(blocks):
                    ts[k][n, pl.ds(HALO + b * B, B), :] = lows[k][b, pl.ds(HALO + n * B, B), :].T * UP2
            part = lifted.at[n, pl.ds(0, 2 * w + 16), :]
            lift_rows(w, ts[k].at[n], zs[k].at[n], part)
            if k < top:
                turn_back(level, n, part, us[k], range(2 * blocks))
        if k < top:
            for j in range(2 * blocks):
                lift_rows(h, us[k].at[j], ws[k].at[j], lows[k + 1].at[j])
        if k == top - 1:
            pl.when(fourth)(enter_all)

    def fill(j, dst):
        at = pl.ds(pl.multiple_of(HALO + j * B, 8), B)
        for n in range(row_blocks(levels[top])):
            dst[pl.ds(HALO + n * B, B), :] = lifted[n, at, :].T

    def body(i, carry):
        j = 2 * i
        _, blocks, h = levels[top]
        fill(j + 1, odd)
        lift_rows(h, even, ws[top].at[j], image.at[j])
        fill(jnp.minimum(j + 2, 2 * blocks - 1), even)
        lift_rows(h, odd, ws[top].at[j + 1], image.at[j + 1])
        return carry

    fill(0, even)
    lax.fori_loop(0, levels[top][1], body, 0)

    for k, (_, blocks, h) in enumerate(levels):
        keep = strip_rows(k)
        for a in (0, 3) if k == 0 else (0,):
            for b in range(blocks):
                at = pl.ds(b * B, B)
                ds[at_of(levels, k, a, b), pl.ds(8, keep), :] = ns[k][a, pl.ds(0, keep), at]
                ds[at_of(levels, k, a, b), pl.ds(8 + keep, keep), :] = ns[k][a, pl.ds(h - keep, keep), at]

    sends[2].wait()
    sends[3].wait()
    for k, a, n, at in columns:
        depth, w = depth_of(levels, k), levels[k][1] * B
        columns_of(k, a)[n, pl.ds(HALO + w, depth), :] = cols_in[0, pl.ds(at, depth), :]
        columns_of(k, a)[n, pl.ds(HALO - depth, depth), :] = cols_in[1, pl.ds(at, depth), :]
    for k in (3, 2, 1, 0):
        blocks = levels[k][1]
        w = blocks * B
        for n in range(row_blocks(levels[k])):
            part = ls[k].at[n]
            for at in (HALO - 4, HALO + w - 4):
                lift_runs(1, xs[k].at[0, n], at, xs[k].at[1, n], at, ls[k].at[n, pl.ds(2 * at - HALO, 16), :])
            turn_back(levels[k], n, part, ws[k], (0, 2 * blocks - 1))
            if k < top:
                turn_back_side(levels[k], n, part, edge, ws[k])
            take, left, right = side_takes(levels, k)
            edge[pl.ds(0, take), :] = part[pl.ds(left, take), :]
            edge[pl.ds(take, take), :] = part[pl.ds(2 * w + 16 - right, take), :]
            count = min(B, levels[k][2])
            wcs[k][pl.ds(HALO + n * B, count), :] = edge[...].T[:count]

    for d in (0, 1):
        sends[d].wait()
    offsets = stack_offsets(levels)
    for k, a, b, at in rows:
        depth, base = depth_of(levels, k), offsets[k] + 8 * b
        hn[a, pl.ds(base, depth), :] = rows_in[0, pl.ds(at, depth), :]
        hn[a, pl.ds(base + 8 - depth, depth), :] = rows_in[1, pl.ds(at, depth), :]
    for d in (4, 5, 6, 7):
        sends[d].wait()
    low, bottom = iota(1) < 64, iota(0) < 4
    for q, (k, a) in enumerate(arrays):
        tile = jnp.where(
            bottom,
            jnp.where(low, turn(corners_in[0], -4 * q), turn(corners_in[1], 4 * q)),
            jnp.where(low, turn(corners_in[2], -4 * q), turn(corners_in[3], 4 * q)))
        cn[a, pl.ds(offsets[k], 8), :] = tile
        cn[a, pl.ds(offsets[k] + 8 * (levels[k][1] - 1), 8), :] = tile
    halo_transpose(levels, hn.at[1], cn.at[1], None, sh)
    halo_transpose(levels, hn.at[2], cn.at[2], DOWN2, rh)
    for k, a, b, at in rows:
        if a in (0, 3):
            depth, keep = depth_of(levels, k), strip_rows(k)
            strip = at_of(levels, k, a, b)
            ds[strip, pl.ds(8 + 2 * keep, depth), :] = rows_in[0, pl.ds(at, depth), :]
            ds[strip, pl.ds(8 - depth, depth), :] = rows_in[1, pl.ds(at, depth), :]
            (ct_out if a == 3 else zts[k])[pl.ds(HALO + b * B, B), :] = scaled(
                ds[strip].T, UP2 if a == 3 else None)
    side = cn[0].T
    for k in range(top + 1):
        strip_sides(levels, k, zs[k], side, zts[k])
    strip_sides(levels, 0, c4, cn[3].T * UP2, ct_out)
    lift_rows(B, sh, rh, hd)
    halo_back(levels, range(top + 1), hd, edge, ws)


def strip_kernel(levels, *refs):
    ws, zts, ct, image = refs[:4], refs[4:8], refs[8], refs[9]
    zs, c4, wcs = refs[10:14], refs[14], refs[15:19]
    out = refs[19]
    lows = (None,) + refs[20:23]
    sides = (None,) + refs[23:26]
    ends, us, lifted, edge, th, tc, sd, pair, uc, strip, merged, out_sem, end_sem = refs[26:]
    top = len(levels) - 1
    _, blocks, h = levels[top]
    rows = 2 * h
    cut = 64

    def main(j, start):
        at = pl.ds(cut, rows - 2 * cut)
        return pltpu.make_async_copy(
            image.at[j, pl.ds(HALO + cut, rows - 2 * cut), :], out.at[at, pl.ds(start, B)], out_sem.at[j])

    def flank(side):
        at = pl.ds(cut, rows - 2 * cut)
        start = (0, (2 * blocks - 1) * B)[side]
        return pltpu.make_async_copy(merged.at[side], out.at[at, pl.ds(start, B)],
                                     out_sem.at[(0, 2 * blocks - 1)[side]])

    def send(j, carry):
        main(j, pl.multiple_of(j * B, B)).start()
        return carry

    lax.fori_loop(1, 2 * blocks - 1, send, 0)

    for k, level in enumerate(levels):
        _, nb, h = level
        w = nb * B
        final = k == top
        keep = strip_rows(k)
        size = 2 * keep + 16
        if k == 0:
            t = ct
        else:
            t = th
            for b in range(nb):
                t[pl.ds(HALO + b * B, B), :] = lows[k][b].T * UP2
            side = lows[k][nb].T * UP2
            t[pl.ds(0, 8), :] = side[B - 8 :]
            t[pl.ds(HALO + w, 8), :] = side[:8]
        run = keep // 8
        take, left, right = side_takes(levels, k)
        for n in range(row_blocks(level)):
            if k == 0:
                side_t, second = c4.at[n], HALO + w + 4 - 8 * run
            else:
                tc[n] = sides[k][pl.ds(HALO + n * B, B), :].T * UP2
                side_t, second = tc.at[n], 8 + 2 * keep + 4 - 8 * run
            lift_runs(run, side_t, 4, zs[k].at[n], 4, sd.at[n, 0, pl.ds(0, 16 * run), :])
            lift_runs(run, side_t, second, zs[k].at[n], HALO + w + 4 - 8 * run, sd.at[n, 1, pl.ds(0, 16 * run), :])
            pair[n, pl.ds(0, take), :] = sd[n, 0, pl.ds(left, take), :]
            pair[n, pl.ds(take, take), :] = sd[n, 1, pl.ds(16 * run - right, take), :]
            count = min(B, h)
            uc[pl.ds(HALO + n * B, count), :] = pair[n].T[:count]
        lift_rows(h, uc, wcs[k], strip if final else sides[k + 1])
        if final:
            low = lax.broadcasted_iota(jnp.int32, (rows - 2 * cut, B), 1) < 64
            at = pl.ds(HALO + cut, rows - 2 * cut)
            merged[0] = jnp.where(low, strip[at, :], image[0, at, :])
            merged[1] = jnp.where(low, image[2 * nb - 1, at, :], strip[at, :])
            for side in range(2):
                flank(side).start()
        part = lifted.at[pl.ds(0, 2 * w + 16), :]
        lift_rows(w, t, zts[k], part)
        for j in range(2 * nb):
            us[j] = lifted[pl.ds(HALO + j * B, B), :].T
        if not final:
            edge[0:8, :] = lifted[pl.ds(HALO + 2 * w, 8), :]
            edge[B - 8 : B, :] = lifted[0:8, :]
            us[2 * nb] = edge[...].T
        run = keep // 8

        def strips(j, first, second, level=level, k=k):
            _, _, h = level
            keep = strip_rows(k)
            run = keep // 8
            lift_runs(run, us.at[j], 4, ws[k].at[j], 4, first)
            lift_runs(run, us.at[j], 8 + 2 * keep + 4 - 8 * run, ws[k].at[j], HALO + h + 4 - 8 * run, second)

        if not final:
            following = strip_rows(k + 1)
            made = 16 * run
            for j in range(2 * nb + 1):
                strips(j, ends.at[0, j, pl.ds(0, made), :], ends.at[1, j, pl.ds(0, made), :])
                lows[k + 1][j, pl.ds(0, 8 + following), :] = ends[0, j, pl.ds(0, 8 + following), :]
                lows[k + 1][j, pl.ds(8 + following, 8 + following), :] = ends[
                    1, j, pl.ds(made - 8 - following, 8 + following), :]
        else:
            made = 16 * run

            def end(j, side, start):
                row = (HALO, made - 8 - cut)[side]
                return pltpu.make_async_copy(
                    ends.at[side, j, pl.ds(row, cut), :],
                    out.at[pl.ds((0, rows - cut)[side], cut), pl.ds(start, B)], end_sem.at[side, j])

            def body(j, carry):
                strips(j, ends.at[0, j, pl.ds(0, made), :], ends.at[1, j, pl.ds(0, made), :])
                for side in range(2):
                    end(j, side, pl.multiple_of(j * B, B)).start()
                return carry

            lax.fori_loop(0, 2 * nb, body, 0)
            for j in range(2 * nb):
                if 0 < j < 2 * nb - 1:
                    main(j, j * B).wait()
                for side in range(2):
                    end(j, side, j * B).wait()
            for side in range(2):
                flank(side).wait()


def per_device(coarse, d4, d3, d2, d1):
    levels = []
    for k, x in enumerate((d4, d3, d2, d1)):
        levels.append((4 if k == 0 else 3, x.shape[2] // B, x.shape[1]))
    levels = tuple(levels)
    top = len(levels) - 1
    _, row_count = row_plan(levels)
    _, col_count = column_plan(levels)
    hbm = pl.BlockSpec(memory_space=pltpu.HBM)
    vmem = pl.BlockSpec(memory_space=pltpu.VMEM)
    wide = [2 * b + (0 if k == top else 1) for k, (_, b, _) in enumerate(levels)]
    across = [(row_blocks(l), l[1] * B + 2 * HALO, B) for l in levels]
    strips = [(n, l[2] + 2 * HALO, B) for n, l in zip(wide, levels)]
    stack = (B + 2 * HALO, B)
    blocks, h = levels[top][1], levels[top][2]
    mb = across[top][0]
    long = 2 * blocks * B + 2 * HALO
    tall = [(l[2] + 2 * HALO, B) for l in levels]
    between = pl.pallas_call(
        functools.partial(exchange_kernel, levels),
        out_shape=[pltpu.VMEM(s, F32) for s in (
            strips + [s[1:] for s in across] + [across[0][1:], (2 * blocks, 2 * h + 2 * HALO, B)]
            + across + [across[0]] + tall)],
        in_specs=[hbm] * 5,
        out_specs=[vmem] * 19,
        scratch_shapes=[
            *[pltpu.VMEM((a, max(B, h), b * B), F32) for a, b, h in levels],
            *[pltpu.VMEM((2,) + s, F32) for s in across],
            *[pltpu.VMEM((n, 2 * l[1] * B + 2 * HALO, B), F32) for (n, _, _), l in zip(across, levels)],
            *[pltpu.VMEM(s, F32) for s in strips[:top] + [(1, 8, B)]],
            *[pltpu.VMEM((l[1], l[2] + 2 * HALO, B), F32) for l in levels[1:]],
            *[pltpu.VMEM(s, F32) for s in across[1:]],
            pltpu.VMEM((4, B, B), F32),
            pltpu.VMEM((4, B, B), F32),
            pltpu.VMEM(stack, F32),
            pltpu.VMEM(stack, F32),
            pltpu.VMEM((2 * B + 2 * HALO, B), F32),
            pltpu.VMEM((mb, long, B), F32),
            pltpu.VMEM((B, B), F32),
            pltpu.VMEM((1 + sum(l[1] for l in levels), B, B), F32),
            pltpu.VMEM(tall[top], F32),
            pltpu.VMEM(tall[top], F32),
            pltpu.VMEM((2, row_count, B), F32),
            pltpu.VMEM((2, col_count, B), F32),
            pltpu.VMEM((4, 8, B), F32),
            pltpu.VMEM((2, row_count, B), F32),
            pltpu.VMEM((2, col_count, B), F32),
            pltpu.VMEM((4, 8, B), F32),
            pltpu.SemaphoreType.DMA((15,)),
            pltpu.SemaphoreType.DMA((8,)),
            pltpu.SemaphoreType.DMA((8,)),
        ],
        compiler_params=pltpu.CompilerParams(
            collective_id=0, has_side_effects=True, vmem_limit_bytes=41 * 2**20),
    )(*[pltpu.with_memory_space_constraint(x, pltpu.HBM) for x in (coarse, d4, d3, d2, d1)])
    return pl.pallas_call(
        functools.partial(strip_kernel, levels),
        out_shape=jax.ShapeDtypeStruct((2 * h, 2 * blocks * B), F32),
        in_specs=[vmem] * 19,
        out_specs=pl.BlockSpec(memory_space=pl.ANY),
        scratch_shapes=[
            *[pltpu.VMEM((l[1] + 1, B, B), F32) for l in levels[1:]],
            *[pltpu.VMEM(s, F32) for s in tall[1:]],
            pltpu.VMEM((2, 2 * blocks, 16 * (strip_rows(top) // 8), B), F32),
            pltpu.VMEM((2 * blocks, B, B), F32),
            pltpu.VMEM((long, B), F32),
            pltpu.VMEM((B, B), F32),
            pltpu.VMEM(across[top][1:], F32),
            pltpu.VMEM((mb, B, B), F32),
            pltpu.VMEM((mb, 2, 16 * (strip_rows(top) // 8), B), F32),
            pltpu.VMEM((mb, B, B), F32),
            pltpu.VMEM(tall[top], F32),
            pltpu.VMEM((2 * h + 2 * HALO, B), F32),
            pltpu.VMEM((2, 2 * h - 128, B), F32),
            pltpu.SemaphoreType.DMA((2 * blocks,)),
            pltpu.SemaphoreType.DMA((2, 2 * blocks)),
        ],
        compiler_params=pltpu.CompilerParams(vmem_limit_bytes=14 * 2**20),
    )(*between)


def solution(mesh):
    return jax.shard_map(
        per_device,
        mesh=mesh,
        in_specs=(
            P("rows", "cols"),
            P(None, "rows", "cols"),
            P(None, "rows", "cols"),
            P(None, "rows", "cols"),
            P(None, "rows", "cols"),
        ),
        out_specs=P("rows", "cols"),
        check_vma=False,
    )
```

```python
import functools

import jax
import jax.numpy as jnp
from jax import lax
from jax.experimental import pallas as pl
from jax.experimental.pallas import tpu as pltpu
from jax.sharding import PartitionSpec as P

ALPHA = -1.586134342059924
BETA = -0.052980118572961
GAMMA = 0.882911075530934
DELTA = 0.443506852043971
SCALE = 1.149604398860241
UP2 = SCALE * SCALE
DOWN2 = 1.0 / (SCALE * SCALE)

B = 128
HALO = 8
F32 = jnp.float32
MESH = pl.DeviceIdType.MESH

DIRS = ((-1, 0), (1, 0), (0, -1), (0, 1), (-1, -1), (-1, 1), (1, -1), (1, 1))


def iota(axis):
    return lax.broadcasted_iota(jnp.int32, (8, B), axis)


def turn(x, amount):
    amount = amount % B
    return x if amount == 0 else pltpu.roll(x, amount, axis=1)


def row_blocks(level):
    return -(-level[2] // B)


def depth_of(levels, k):
    return 2 if k == len(levels) - 1 else 4


def row_plan(levels):
    plan, at = [], 0
    for k, (arrays, blocks, h) in enumerate(levels):
        for a in range(arrays):
            for b in range(blocks):
                plan.append((k, a, b, at))
                at += depth_of(levels, k)
    return plan, -(-at // 8) * 8


def column_plan(levels):
    plan, at = [], 0
    for k, level in enumerate(levels):
        for a in range(level[0]):
            for n in range(row_blocks(level)):
                plan.append((k, a, n, at))
                at += depth_of(levels, k)
    return plan, -(-at // 8) * 8


def stack_offsets(levels):
    offsets, at = [], 0
    for _, blocks, _ in levels:
        offsets.append(at)
        at += 8 * blocks
    return offsets


def lift_rows(count, s, r, dst):
    lift_runs((count + 8) // 8, s, HALO - 4, r, HALO - 4, dst)


def lift_runs(run, s, s_at, r, r_at, dst):
    def rows(ref, t):
        at = s_at if ref is s else r_at
        return ref[pl.ds(at + t, 8, stride=run), :]

    r0, s1, r1, s2 = {}, {}, {}, {}
    for t in range(-2, run + 2):
        r0[t] = rows(r, t)
        if t < -1:
            continue
        s1[t] = rows(s, t) - DELTA * (r0[t] + r0[t - 1])
        if t < 0:
            continue
        r1[t - 1] = r0[t - 1] - GAMMA * (s1[t - 1] + s1[t])
        if t < 1:
            continue
        n = t - 1
        s2[n] = s1[n] - BETA * (r1[n] + r1[n - 1])
        if n < run:
            dst[pl.ds(2 * n, 8, stride=2 * run), :] = s2[n]
        if n >= 1:
            dst[pl.ds(2 * n - 1, 8, stride=2 * run), :] = r1[n - 1] - ALPHA * (s2[n - 1] + s2[n])


def scaled(x, scale):
    return x if scale is None else x * scale


def turn_back(level, n, lifted, dst, which):
    count = min(B, level[2])
    at = pl.ds(HALO + n * B, count)
    for j in which:
        dst[j, at, :] = lifted[pl.ds(HALO + j * B, B), :].T[:count]


def turn_back_side(level, n, lifted, edge, dst):
    _, blocks, h = level
    count = min(B, h)
    edge[0:8, :] = lifted[pl.ds(HALO + 2 * blocks * B, 8), :]
    edge[B - 8 : B, :] = lifted[0:8, :]
    dst[2 * blocks, pl.ds(HALO + n * B, count), :] = edge[...].T[:count]


def halo_transpose(levels, hn, cn, scale, dst):
    group = iota(1) // 8
    offsets = stack_offsets(levels)
    first = last = None
    for off, (_, blocks, _) in zip(offsets, levels):
        f, l = group == off // 8, group == off // 8 + blocks - 1
        first = f if first is None else first | f
        last = l if last is None else last | l
    t = scaled(hn[...].T, scale)
    ct = scaled(cn[...].T, scale)
    dst[pl.ds(HALO, B), :] = t
    dst[pl.ds(0, 8), :] = jnp.where(first, ct[B - 8 :], turn(t[B - 8 :], 8))
    dst[pl.ds(HALO + B, 8), :] = jnp.where(last, ct[:8], turn(t[:8], -8))


def halo_back(levels, which, lifted, edge, dsts):
    low = iota(1) < 64
    offsets = stack_offsets(levels)
    for j in range(2):
        y = lifted[pl.ds(HALO + j * B, B), :].T
        for k in which:
            _, blocks, h = levels[k]
            for b in range(blocks):
                tile = y[offsets[k] + 8 * b : offsets[k] + 8 * b + 8]
                dsts[k][2 * b + j, pl.ds(0, 8), :] = tile
                dsts[k][2 * b + j, pl.ds(HALO + h, 8), :] = tile
    which = [k for k in which if k < len(levels) - 1]
    if which:
        edge[0:8, :] = lifted[pl.ds(HALO + 2 * B, 8), :]
        edge[B - 8 : B, :] = lifted[0:8, :]
        y = edge[...].T
        for k in which:
            _, blocks, h = levels[k]
            end = offsets[k] + 8 * (blocks - 1)
            tile = jnp.where(low, y[end : end + 8], y[offsets[k] : offsets[k] + 8])
            dsts[k][2 * blocks, pl.ds(0, 8), :] = tile
            dsts[k][2 * blocks, pl.ds(HALO + h, 8), :] = tile


def strip_rows(k):
    return (16, 16, 24, 40)[k]


def strip_sides(levels, k, main, ct, dst):
    _, blocks, h = levels[k]
    keep, off = strip_rows(k), stack_offsets(levels)[k]
    lane = iota(1)
    n = row_blocks(levels[k])
    start = h - keep - B * (n - 1)
    w = blocks * B
    for at, corner, shift in ((0, ct[B - 8 :], off), (HALO + w, ct[:8], off + 8 * (blocks - 1))):
        here = pl.ds(at, 8)
        dst[here, :] = jnp.where(
            lane < 8, turn(corner, -shift),
            jnp.where(
                lane < 8 + keep, turn(main[0, here, :], 8),
                jnp.where(lane < 8 + 2 * keep, turn(main[n - 1, here, :], 8 + keep - start),
                          turn(corner, 8 + 2 * keep - shift))))


def at_of(levels, k, a, b):
    return b if a == 3 else 1 + sum(l[1] for l in levels[:k]) + b


def side_takes(levels, k):
    if k == len(levels) - 1:
        return 64, 8, 72
    take = 8 + strip_rows(k + 1)
    return take, 0, take


def exchange_kernel(levels, *refs):
    coarse, d4, d3, d2, d1 = refs[:5]
    ws, zts, ct_out, image = refs[5:9], refs[9:13], refs[13], refs[14]
    zs, c4, wcs = refs[15:19], refs[19], refs[20:24]
    ns, xs, ls, us = refs[24:28], refs[28:32], refs[32:36], refs[36:40]
    lows, ts = (None,) + refs[40:43], (c4,) + refs[43:46]
    (hn, cn, sh, rh, hd, lifted, edge, ds, rows_out, cols_out, corners_out,
     rows_in, cols_in, corners_in, load_sem, send_sem, recv_sem) = refs[46:]
    nr, nc = lax.axis_size("rows"), lax.axis_size("cols")
    r, c = lax.axis_index("rows"), lax.axis_index("cols")
    top = len(levels) - 1

    def neighbour(step):
        return (lax.rem(r + step[0] + nr, nr), lax.rem(c + step[1] + nc, nc))

    barrier = pltpu.get_barrier_semaphore()
    for step in DIRS:
        pl.semaphore_signal(barrier, inc=1, device_id=neighbour(step), device_id_type=MESH)

    loads = []

    def load(src, dst):
        copy = pltpu.make_async_copy(src, dst, load_sem.at[len(loads)])
        copy.start()
        loads.append(copy)

    h = levels[0][2]
    load(coarse, ns[0].at[3, pl.ds(0, h), :])
    load(d4, ns[0].at[pl.ds(0, 3), pl.ds(0, h), :])
    for k, src in ((1, d3), (2, d2), (3, d1)):
        h = levels[k][2]
        for at in (pl.ds(0, 8), pl.ds(h - 8, 8)):
            load(src.at[:, at, :], ns[k].at[:, at, :])
    edge_loads = len(loads)
    for k, src in ((1, d3), (2, d2)):
        inner = pl.ds(8, levels[k][2] - 16)
        load(src.at[:, inner, :], ns[k].at[:, inner, :])
    _, blocks, h = levels[top]
    w = blocks * B
    inner = pl.ds(8, h - 16)
    for at in (pl.ds(0, B), pl.ds(w - B, B)):
        load(d1.at[:, inner, at], ns[top].at[:, inner, at])
    side_loads = len(loads)
    for a in range(3):
        at = pl.ds(B, w - 2 * B)
        load(d1.at[a, inner, at], ns[top].at[a, inner, at])

    def columns_of(k, a):
        return c4 if a == 3 else zs[k] if a == 0 else xs[k].at[a - 1]

    def transpose(k, a, n, b):
        scale = (None, None, DOWN2, UP2)[a]
        columns_of(k, a)[n, pl.ds(HALO + b * B, B), :] = scaled(
            ns[k][a, pl.ds(n * B, B), pl.ds(b * B, B)].T, scale)

    for copy in loads[:edge_loads]:
        copy.wait()
    rows, _ = row_plan(levels)
    for k, a, b, at in rows:
        depth, h = depth_of(levels, k), levels[k][2]
        here = pl.ds(b * B, B)
        rows_out[0, pl.ds(at, depth), :] = ns[k][a, pl.ds(0, depth), here]
        rows_out[1, pl.ds(at, depth), :] = ns[k][a, pl.ds(h - depth, depth), here]
    group = iota(1) // 4
    arrays = [(k, a) for k in range(top + 1) for a in range(levels[k][0])]
    for d in range(4):
        step = DIRS[4 + d]
        packed = jnp.zeros((8, B), F32)
        for q, (k, a) in enumerate(arrays):
            _, blocks, h = levels[k]
            at = pl.ds(0 if step[0] < 0 else h - 8, 8)
            if step[1] < 0:
                packed = jnp.where(group == q, turn(ns[k][a, at, pl.ds(0, B)], 4 * q), packed)
            else:
                packed = jnp.where(
                    group == 31 - q, turn(ns[k][a, at, pl.ds((blocks - 1) * B, B)], -4 * q), packed)
        corners_out[d] = packed

    sends = []
    for d, step in enumerate(DIRS):
        if d < 2:
            src, dst = rows_out.at[d], rows_in.at[d]
        elif d < 4:
            src, dst = cols_out.at[d - 2], cols_in.at[d - 2]
        else:
            src, dst = corners_out.at[d - 4], corners_in.at[d - 4]
        sends.append(pltpu.make_async_remote_copy(
            src_ref=src, dst_ref=dst, send_sem=send_sem.at[d], recv_sem=recv_sem.at[d],
            device_id=neighbour(step), device_id_type=MESH))

    def enter():
        pl.semaphore_wait(barrier, len(DIRS))
        for d in (4, 5, 6, 7, 0, 1):
            sends[d].start()

    def enter_sides():
        sends[2].start()
        sends[3].start()

    def enter_all():
        enter()
        enter_sides()

    first_row = r < 1
    fourth = jnp.logical_and(first_row, c < 2)
    third = jnp.logical_or(
        jnp.logical_and(first_row, c >= 2),
        jnp.logical_and(jnp.logical_and(lax.rem(r, 4) < 1, r >= 1), c < 1))
    rest = jnp.logical_not(jnp.logical_or(third, fourth))
    quick = jnp.logical_or(jnp.logical_and(c >= 2, lax.rem(c, 2) < 1), c >= nc - 1)
    at_once = jnp.logical_and(rest, quick)
    second = jnp.logical_and(rest, jnp.logical_not(quick))
    pl.when(at_once)(enter)

    for copy in loads[edge_loads : edge_loads + 2]:
        copy.wait()
    for k in range(top):
        for a in range(levels[k][0]):
            for n in range(row_blocks(levels[k])):
                for b in range(levels[k][1]):
                    transpose(k, a, n, b)
    for copy in loads[edge_loads + 2 : side_loads]:
        copy.wait()
    for a in range(3):
        for n in range(row_blocks(levels[top])):
            for b in (0, levels[top][1] - 1):
                transpose(top, a, n, b)
    columns, _ = column_plan(levels)
    for k, a, n, at in columns:
        depth, w = depth_of(levels, k), levels[k][1] * B
        cols_out[0, pl.ds(at, depth), :] = columns_of(k, a)[n, pl.ds(HALO, depth), :]
        cols_out[1, pl.ds(at, depth), :] = columns_of(k, a)[n, pl.ds(HALO + w - depth, depth), :]

    pl.when(at_once)(enter_sides)
    pl.when(second)(enter_all)

    def details(k):
        for n in range(row_blocks(levels[k])):
            lift_rows(levels[k][1] * B, xs[k].at[0, n], xs[k].at[1, n], ls[k].at[n])
            turn_back(levels[k], n, ls[k].at[n], ws[k], range(2 * levels[k][1]))

    def inner(k, count, s, r, dst):
        start = (-4, 4, 12, 28)[k]
        run = (count - 2 * start) // 8
        at = HALO + start
        lift_runs(run, s, at, r, at, dst.at[pl.ds(HALO + 2 * start, 16 * run), :])

    def chain_columns(k):
        _, blocks, h = levels[k]
        for n in range(row_blocks(levels[k])):
            if k > 0:
                for b in range(blocks):
                    ts[k][n, pl.ds(HALO + b * B, B), :] = lows[k][b, pl.ds(HALO + n * B, B), :].T * UP2
            inner(k, blocks * B, ts[k].at[n], zs[k].at[n], lifted.at[n])

    def chain_rows(k, these):
        h = levels[k][2]
        for j in these:
            for n in range(row_blocks(levels[k])):
                turn_back(levels[k], n, lifted.at[n], us[k], (j,))
            inner(k, h, us[k].at[j], ws[k].at[j], image.at[j] if k == top else lows[k + 1].at[j])

    for k in range(top):
        details(k)
    for k in range(top - 1):
        chain_columns(k)
        chain_rows(k, range(2 * levels[k][1]))
    for copy in loads[side_loads:]:
        copy.wait()
    for a in range(3):
        for n in range(row_blocks(levels[top])):
            for b in range(1, levels[top][1] - 1):
                transpose(top, a, n, b)
    chain_columns(top - 1)
    chain_rows(top - 1, range(2 * levels[top - 1][1]))
    pl.when(third)(enter_all)

    details(top)
    chain_columns(top)
    blocks = levels[top][1]
    chain_rows(top, range(1, blocks))
    pl.when(fourth)(enter_all)

    for k, (_, blocks, h) in enumerate(levels):
        keep = strip_rows(k)
        for a in (0, 3) if k == 0 else (0,):
            for b in range(blocks):
                at = pl.ds(b * B, B)
                ds[at_of(levels, k, a, b), pl.ds(8, keep), :] = ns[k][a, pl.ds(0, keep), at]
                ds[at_of(levels, k, a, b), pl.ds(8 + keep, keep), :] = ns[k][a, pl.ds(h - keep, keep), at]

    sends[2].wait()
    sends[3].wait()
    for k, a, n, at in columns:
        depth, w = depth_of(levels, k), levels[k][1] * B
        columns_of(k, a)[n, pl.ds(HALO + w, depth), :] = cols_in[0, pl.ds(at, depth), :]
        columns_of(k, a)[n, pl.ds(HALO - depth, depth), :] = cols_in[1, pl.ds(at, depth), :]
    for k in (3, 2, 1, 0):
        blocks = levels[k][1]
        w = blocks * B
        for n in range(row_blocks(levels[k])):
            part = ls[k].at[n]
            for at in (HALO - 4, HALO + w - 4):
                lift_runs(1, xs[k].at[0, n], at, xs[k].at[1, n], at, ls[k].at[n, pl.ds(2 * at - HALO, 16), :])
            turn_back(levels[k], n, part, ws[k], (0, 2 * blocks - 1))
            if k < top:
                turn_back_side(levels[k], n, part, edge, ws[k])
            take, left, right = side_takes(levels, k)
            edge[pl.ds(0, take), :] = part[pl.ds(left, take), :]
            edge[pl.ds(take, take), :] = part[pl.ds(2 * w + 16 - right, take), :]
            count = min(B, levels[k][2])
            wcs[k][pl.ds(HALO + n * B, count), :] = edge[...].T[:count]

    chain_rows(top, (*range(levels[top][1], 2 * levels[top][1]), 0))

    for d in (0, 1):
        sends[d].wait()
    offsets = stack_offsets(levels)
    for k, a, b, at in rows:
        depth, base = depth_of(levels, k), offsets[k] + 8 * b
        hn[a, pl.ds(base, depth), :] = rows_in[0, pl.ds(at, depth), :]
        hn[a, pl.ds(base + 8 - depth, depth), :] = rows_in[1, pl.ds(at, depth), :]
    for d in (4, 5, 6, 7):
        sends[d].wait()
    low, bottom = iota(1) < 64, iota(0) < 4
    for q, (k, a) in enumerate(arrays):
        tile = jnp.where(
            bottom,
            jnp.where(low, turn(corners_in[0], -4 * q), turn(corners_in[1], 4 * q)),
            jnp.where(low, turn(corners_in[2], -4 * q), turn(corners_in[3], 4 * q)))
        cn[a, pl.ds(offsets[k], 8), :] = tile
        cn[a, pl.ds(offsets[k] + 8 * (levels[k][1] - 1), 8), :] = tile
    halo_transpose(levels, hn.at[1], cn.at[1], None, sh)
    halo_transpose(levels, hn.at[2], cn.at[2], DOWN2, rh)
    for k, a, b, at in rows:
        if a in (0, 3):
            depth, keep = depth_of(levels, k), strip_rows(k)
            strip = at_of(levels, k, a, b)
            ds[strip, pl.ds(8 + 2 * keep, depth), :] = rows_in[0, pl.ds(at, depth), :]
            ds[strip, pl.ds(8 - depth, depth), :] = rows_in[1, pl.ds(at, depth), :]
            (ct_out if a == 3 else zts[k])[pl.ds(HALO + b * B, B), :] = scaled(
                ds[strip].T, UP2 if a == 3 else None)
    side = cn[0].T
    for k in range(top + 1):
        strip_sides(levels, k, zs[k], side, zts[k])
    strip_sides(levels, 0, c4, cn[3].T * UP2, ct_out)
    lift_rows(B, sh, rh, hd)
    halo_back(levels, range(top + 1), hd, edge, ws)


def strip_kernel(levels, *refs):
    ws, zts, ct, image = refs[:4], refs[4:8], refs[8], refs[9]
    zs, c4, wcs = refs[10:14], refs[14], refs[15:19]
    out = refs[19]
    lows = (None,) + refs[20:23]
    sides = (None,) + refs[23:26]
    ends, us, lifted, edge, th, tc, sd, pair, uc, strip, merged, out_sem, end_sem = refs[26:]
    top = len(levels) - 1
    _, blocks, h = levels[top]
    rows = 2 * h
    cut = 64

    def main(j, start):
        at = pl.ds(cut, rows - 2 * cut)
        return pltpu.make_async_copy(
            image.at[j, pl.ds(HALO + cut, rows - 2 * cut), :], out.at[at, pl.ds(start, B)], out_sem.at[j])

    def flank(side):
        at = pl.ds(cut, rows - 2 * cut)
        start = (0, (2 * blocks - 1) * B)[side]
        return pltpu.make_async_copy(merged.at[side], out.at[at, pl.ds(start, B)],
                                     out_sem.at[(0, 2 * blocks - 1)[side]])

    def send(j, carry):
        main(j, pl.multiple_of(j * B, B)).start()
        return carry

    lax.fori_loop(1, 2 * blocks - 1, send, 0)

    for k, level in enumerate(levels):
        _, nb, h = level
        w = nb * B
        final = k == top
        keep = strip_rows(k)
        size = 2 * keep + 16
        if k == 0:
            t = ct
        else:
            t = th
            for b in range(nb):
                t[pl.ds(HALO + b * B, B), :] = lows[k][b].T * UP2
            side = lows[k][nb].T * UP2
            t[pl.ds(0, 8), :] = side[B - 8 :]
            t[pl.ds(HALO + w, 8), :] = side[:8]
        run = keep // 8
        take, left, right = side_takes(levels, k)
        for n in range(row_blocks(level)):
            if k == 0:
                side_t, second = c4.at[n], HALO + w + 4 - 8 * run
            else:
                tc[n] = sides[k][pl.ds(HALO + n * B, B), :].T * UP2
                side_t, second = tc.at[n], 8 + 2 * keep + 4 - 8 * run
            lift_runs(run, side_t, 4, zs[k].at[n], 4, sd.at[n, 0, pl.ds(0, 16 * run), :])
            lift_runs(run, side_t, second, zs[k].at[n], HALO + w + 4 - 8 * run, sd.at[n, 1, pl.ds(0, 16 * run), :])
            pair[n, pl.ds(0, take), :] = sd[n, 0, pl.ds(left, take), :]
            pair[n, pl.ds(take, take), :] = sd[n, 1, pl.ds(16 * run - right, take), :]
            count = min(B, h)
            uc[pl.ds(HALO + n * B, count), :] = pair[n].T[:count]
        lift_rows(h, uc, wcs[k], strip if final else sides[k + 1])
        if final:
            low = lax.broadcasted_iota(jnp.int32, (rows - 2 * cut, B), 1) < 64
            at = pl.ds(HALO + cut, rows - 2 * cut)
            merged[0] = jnp.where(low, strip[at, :], image[0, at, :])
            merged[1] = jnp.where(low, image[2 * nb - 1, at, :], strip[at, :])
            for side in range(2):
                flank(side).start()
        part = lifted.at[pl.ds(0, 2 * w + 16), :]
        lift_rows(w, t, zts[k], part)
        for j in range(2 * nb):
            us[j] = lifted[pl.ds(HALO + j * B, B), :].T
        if not final:
            edge[0:8, :] = lifted[pl.ds(HALO + 2 * w, 8), :]
            edge[B - 8 : B, :] = lifted[0:8, :]
            us[2 * nb] = edge[...].T
        run = keep // 8

        def strips(j, first, second, level=level, k=k):
            _, _, h = level
            keep = strip_rows(k)
            run = keep // 8
            lift_runs(run, us.at[j], 4, ws[k].at[j], 4, first)
            lift_runs(run, us.at[j], 8 + 2 * keep + 4 - 8 * run, ws[k].at[j], HALO + h + 4 - 8 * run, second)

        if not final:
            following = strip_rows(k + 1)
            made = 16 * run
            for j in range(2 * nb + 1):
                strips(j, ends.at[0, j, pl.ds(0, made), :], ends.at[1, j, pl.ds(0, made), :])
                lows[k + 1][j, pl.ds(0, 8 + following), :] = ends[0, j, pl.ds(0, 8 + following), :]
                lows[k + 1][j, pl.ds(8 + following, 8 + following), :] = ends[
                    1, j, pl.ds(made - 8 - following, 8 + following), :]
        else:
            made = 16 * run

            def end(j, side, start):
                row = (HALO, made - 8 - cut)[side]
                return pltpu.make_async_copy(
                    ends.at[side, j, pl.ds(row, cut), :],
                    out.at[pl.ds((0, rows - cut)[side], cut), pl.ds(start, B)], end_sem.at[side, j])

            def body(j, carry):
                strips(j, ends.at[0, j, pl.ds(0, made), :], ends.at[1, j, pl.ds(0, made), :])
                for side in range(2):
                    end(j, side, pl.multiple_of(j * B, B)).start()
                return carry

            lax.fori_loop(0, 2 * nb, body, 0)
            for j in range(2 * nb):
                if 0 < j < 2 * nb - 1:
                    main(j, j * B).wait()
                for side in range(2):
                    end(j, side, j * B).wait()
            for side in range(2):
                flank(side).wait()


def per_device(coarse, d4, d3, d2, d1):
    levels = []
    for k, x in enumerate((d4, d3, d2, d1)):
        levels.append((4 if k == 0 else 3, x.shape[2] // B, x.shape[1]))
    levels = tuple(levels)
    top = len(levels) - 1
    _, row_count = row_plan(levels)
    _, col_count = column_plan(levels)
    hbm = pl.BlockSpec(memory_space=pltpu.HBM)
    vmem = pl.BlockSpec(memory_space=pltpu.VMEM)
    wide = [2 * b + (0 if k == top else 1) for k, (_, b, _) in enumerate(levels)]
    across = [(row_blocks(l), l[1] * B + 2 * HALO, B) for l in levels]
    strips = [(n, l[2] + 2 * HALO, B) for n, l in zip(wide, levels)]
    stack = (B + 2 * HALO, B)
    blocks, h = levels[top][1], levels[top][2]
    mb = across[top][0]
    long = 2 * blocks * B + 2 * HALO
    tall = [(l[2] + 2 * HALO, B) for l in levels]
    between = pl.pallas_call(
        functools.partial(exchange_kernel, levels),
        out_shape=[pltpu.VMEM(s, F32) for s in (
            strips + [s[1:] for s in across] + [across[0][1:], (2 * blocks, 2 * h + 2 * HALO, B)]
            + across + [across[0]] + tall)],
        in_specs=[hbm] * 5,
        out_specs=[vmem] * 19,
        scratch_shapes=[
            *[pltpu.VMEM((a, max(B, h), b * B), F32) for a, b, h in levels],
            *[pltpu.VMEM((2,) + s, F32) for s in across],
            *[pltpu.VMEM((n, 2 * l[1] * B + 2 * HALO, B), F32) for (n, _, _), l in zip(across, levels)],
            *[pltpu.VMEM(s, F32) for s in strips],
            *[pltpu.VMEM((l[1], l[2] + 2 * HALO, B), F32) for l in levels[1:]],
            *[pltpu.VMEM(s, F32) for s in across[1:]],
            pltpu.VMEM((4, B, B), F32),
            pltpu.VMEM((4, B, B), F32),
            pltpu.VMEM(stack, F32),
            pltpu.VMEM(stack, F32),
            pltpu.VMEM((2 * B + 2 * HALO, B), F32),
            pltpu.VMEM((mb, long, B), F32),
            pltpu.VMEM((B, B), F32),
            pltpu.VMEM((1 + sum(l[1] for l in levels), B, B), F32),
            pltpu.VMEM((2, row_count, B), F32),
            pltpu.VMEM((2, col_count, B), F32),
            pltpu.VMEM((4, 8, B), F32),
            pltpu.VMEM((2, row_count, B), F32),
            pltpu.VMEM((2, col_count, B), F32),
            pltpu.VMEM((4, 8, B), F32),
            pltpu.SemaphoreType.DMA((15,)),
            pltpu.SemaphoreType.DMA((8,)),
            pltpu.SemaphoreType.DMA((8,)),
        ],
        compiler_params=pltpu.CompilerParams(
            collective_id=0, has_side_effects=True, vmem_limit_bytes=41 * 2**20),
    )(*[pltpu.with_memory_space_constraint(x, pltpu.HBM) for x in (coarse, d4, d3, d2, d1)])
    return pl.pallas_call(
        functools.partial(strip_kernel, levels),
        out_shape=jax.ShapeDtypeStruct((2 * h, 2 * blocks * B), F32),
        in_specs=[vmem] * 19,
        out_specs=pl.BlockSpec(memory_space=pl.ANY),
        scratch_shapes=[
            *[pltpu.VMEM((l[1] + 1, B, B), F32) for l in levels[1:]],
            *[pltpu.VMEM(s, F32) for s in tall[1:]],
            pltpu.VMEM((2, 2 * blocks, 16 * (strip_rows(top) // 8), B), F32),
            pltpu.VMEM((2 * blocks, B, B), F32),
            pltpu.VMEM((long, B), F32),
            pltpu.VMEM((B, B), F32),
            pltpu.VMEM(across[top][1:], F32),
            pltpu.VMEM((mb, B, B), F32),
            pltpu.VMEM((mb, 2, 16 * (strip_rows(top) // 8), B), F32),
            pltpu.VMEM((mb, B, B), F32),
            pltpu.VMEM(tall[top], F32),
            pltpu.VMEM((2 * h + 2 * HALO, B), F32),
            pltpu.VMEM((2, 2 * h - 128, B), F32),
            pltpu.SemaphoreType.DMA((2 * blocks,)),
            pltpu.SemaphoreType.DMA((2, 2 * blocks)),
        ],
        compiler_params=pltpu.CompilerParams(vmem_limit_bytes=14 * 2**20),
    )(*between)


def solution(mesh):
    return jax.shard_map(
        per_device,
        mesh=mesh,
        in_specs=(
            P("rows", "cols"),
            P(None, "rows", "cols"),
            P(None, "rows", "cols"),
            P(None, "rows", "cols"),
            P(None, "rows", "cols"),
        ),
        out_specs=P("rows", "cols"),
        check_vma=False,
    )
```

```python
import functools

import jax
import jax.numpy as jnp
from jax import lax
from jax.experimental import pallas as pl
from jax.experimental.pallas import tpu as pltpu
from jax.sharding import PartitionSpec as P

ALPHA = -1.586134342059924
BETA = -0.052980118572961
GAMMA = 0.882911075530934
DELTA = 0.443506852043971
SCALE = 1.149604398860241
UP2 = SCALE * SCALE
DOWN2 = 1.0 / (SCALE * SCALE)

B = 128
HALO = 8
F32 = jnp.float32
MESH = pl.DeviceIdType.MESH

DIRS = ((-1, 0), (1, 0), (0, -1), (0, 1), (-1, -1), (-1, 1), (1, -1), (1, 1))


def iota(axis):
    return lax.broadcasted_iota(jnp.int32, (8, B), axis)


def turn(x, amount):
    amount = amount % B
    return x if amount == 0 else pltpu.roll(x, amount, axis=1)


def row_blocks(level):
    return -(-level[2] // B)


def depth_of(levels, k):
    return 2 if k == len(levels) - 1 else 4


def row_plan(levels):
    plan, at = [], 0
    for k, (arrays, blocks, h) in enumerate(levels):
        for a in range(arrays):
            for b in range(blocks):
                plan.append((k, a, b, at))
                at += depth_of(levels, k)
    return plan, -(-at // 8) * 8


def column_plan(levels):
    plan, at = [], 0
    for k, level in enumerate(levels):
        for a in range(level[0]):
            for n in range(row_blocks(level)):
                plan.append((k, a, n, at))
                at += depth_of(levels, k)
    return plan, -(-at // 8) * 8


def stack_offsets(levels):
    offsets, at = [], 0
    for _, blocks, _ in levels:
        offsets.append(at)
        at += 8 * blocks
    return offsets


def lift_rows(count, s, r, dst):
    lift_runs((count + 8) // 8, s, HALO - 4, r, HALO - 4, dst)


def lift_runs(run, s, s_at, r, r_at, dst):
    def rows(ref, t):
        at = s_at if ref is s else r_at
        return ref[pl.ds(at + t, 8, stride=run), :]

    r0, s1, r1, s2 = {}, {}, {}, {}
    for t in range(-2, run + 2):
        r0[t] = rows(r, t)
        if t < -1:
            continue
        s1[t] = rows(s, t) - DELTA * (r0[t] + r0[t - 1])
        if t < 0:
            continue
        r1[t - 1] = r0[t - 1] - GAMMA * (s1[t - 1] + s1[t])
        if t < 1:
            continue
        n = t - 1
        s2[n] = s1[n] - BETA * (r1[n] + r1[n - 1])
        if n < run:
            dst[pl.ds(2 * n, 8, stride=2 * run), :] = s2[n]
        if n >= 1:
            dst[pl.ds(2 * n - 1, 8, stride=2 * run), :] = r1[n - 1] - ALPHA * (s2[n - 1] + s2[n])


def scaled(x, scale):
    return x if scale is None else x * scale


def turn_back(level, n, lifted, dst, which):
    count = min(B, level[2])
    at = pl.ds(HALO + n * B, count)
    for j in which:
        dst[j, at, :] = lifted[pl.ds(HALO + j * B, B), :].T[:count]


def turn_back_side(level, n, lifted, edge, dst):
    _, blocks, h = level
    count = min(B, h)
    edge[0:8, :] = lifted[pl.ds(HALO + 2 * blocks * B, 8), :]
    edge[B - 8 : B, :] = lifted[0:8, :]
    dst[2 * blocks, pl.ds(HALO + n * B, count), :] = edge[...].T[:count]


def halo_transpose(levels, hn, cn, scale, dst):
    group = iota(1) // 8
    offsets = stack_offsets(levels)
    first = last = None
    for off, (_, blocks, _) in zip(offsets, levels):
        f, l = group == off // 8, group == off // 8 + blocks - 1
        first = f if first is None else first | f
        last = l if last is None else last | l
    t = scaled(hn[...].T, scale)
    ct = scaled(cn[...].T, scale)
    dst[pl.ds(HALO, B), :] = t
    dst[pl.ds(0, 8), :] = jnp.where(first, ct[B - 8 :], turn(t[B - 8 :], 8))
    dst[pl.ds(HALO + B, 8), :] = jnp.where(last, ct[:8], turn(t[:8], -8))


def halo_back(levels, which, lifted, edge, dsts):
    low = iota(1) < 64
    offsets = stack_offsets(levels)
    for j in range(2):
        y = lifted[pl.ds(HALO + j * B, B), :].T
        for k in which:
            _, blocks, h = levels[k]
            for b in range(blocks):
                tile = y[offsets[k] + 8 * b : offsets[k] + 8 * b + 8]
                dsts[k][2 * b + j, pl.ds(0, 8), :] = tile
                dsts[k][2 * b + j, pl.ds(HALO + h, 8), :] = tile
    which = [k for k in which if k < len(levels) - 1]
    if which:
        edge[0:8, :] = lifted[pl.ds(HALO + 2 * B, 8), :]
        edge[B - 8 : B, :] = lifted[0:8, :]
        y = edge[...].T
        for k in which:
            _, blocks, h = levels[k]
            end = offsets[k] + 8 * (blocks - 1)
            tile = jnp.where(low, y[end : end + 8], y[offsets[k] : offsets[k] + 8])
            dsts[k][2 * blocks, pl.ds(0, 8), :] = tile
            dsts[k][2 * blocks, pl.ds(HALO + h, 8), :] = tile


def strip_rows(k):
    return (16, 16, 24, 40)[k]


def strip_sides(levels, k, main, ct, dst):
    _, blocks, h = levels[k]
    keep, off = strip_rows(k), stack_offsets(levels)[k]
    lane = iota(1)
    n = row_blocks(levels[k])
    start = h - keep - B * (n - 1)
    w = blocks * B
    for at, corner, shift in ((0, ct[B - 8 :], off), (HALO + w, ct[:8], off + 8 * (blocks - 1))):
        here = pl.ds(at, 8)
        dst[here, :] = jnp.where(
            lane < 8, turn(corner, -shift),
            jnp.where(
                lane < 8 + keep, turn(main[0, here, :], 8),
                jnp.where(lane < 8 + 2 * keep, turn(main[n - 1, here, :], 8 + keep - start),
                          turn(corner, 8 + 2 * keep - shift))))


def at_of(levels, k, a, b):
    return b if a == 3 else 1 + sum(l[1] for l in levels[:k]) + b


def side_takes(levels, k):
    if k == len(levels) - 1:
        return 64, 8, 72
    take = 8 + strip_rows(k + 1)
    return take, 0, take


def exchange_kernel(levels, *refs):
    coarse, d4, d3, d2, d1 = refs[:5]
    ws, zts, ct_out, image = refs[5:9], refs[9:13], refs[13], refs[14]
    zs, c4, wcs = refs[15:19], refs[19], refs[20:24]
    ns, xs, ls, us = refs[24:28], refs[28:32], refs[32:36], refs[36:40]
    lows, ts = (None,) + refs[40:43], (c4,) + refs[43:46]
    (hn, cn, sh, rh, hd, lifted, edge, ds, rows_out, cols_out, corners_out,
     rows_in, cols_in, corners_in, load_sem, send_sem, recv_sem) = refs[46:]
    nr, nc = lax.axis_size("rows"), lax.axis_size("cols")
    r, c = lax.axis_index("rows"), lax.axis_index("cols")
    top = len(levels) - 1

    def neighbour(step):
        return (lax.rem(r + step[0] + nr, nr), lax.rem(c + step[1] + nc, nc))

    barrier = pltpu.get_barrier_semaphore()
    for step in DIRS:
        pl.semaphore_signal(barrier, inc=1, device_id=neighbour(step), device_id_type=MESH)

    loads = []

    def load(src, dst):
        copy = pltpu.make_async_copy(src, dst, load_sem.at[len(loads)])
        copy.start()
        loads.append(copy)

    h = levels[0][2]
    load(coarse, ns[0].at[3, pl.ds(0, h), :])
    load(d4, ns[0].at[pl.ds(0, 3), pl.ds(0, h), :])
    for k, src in ((1, d3), (2, d2), (3, d1)):
        h = levels[k][2]
        for at in (pl.ds(0, 8), pl.ds(h - 8, 8)):
            load(src.at[:, at, :], ns[k].at[:, at, :])
    edge_loads = len(loads)
    for k, src in ((1, d3), (2, d2)):
        inner = pl.ds(8, levels[k][2] - 16)
        load(src.at[:, inner, :], ns[k].at[:, inner, :])
    _, blocks, h = levels[top]
    w = blocks * B
    inner = pl.ds(8, h - 16)
    for at in (pl.ds(0, B), pl.ds(w - B, B)):
        load(d1.at[:, inner, at], ns[top].at[:, inner, at])
    side_loads = len(loads)
    for a in range(3):
        at = pl.ds(B, w - 2 * B)
        load(d1.at[a, inner, at], ns[top].at[a, inner, at])

    def columns_of(k, a):
        return c4 if a == 3 else zs[k] if a == 0 else xs[k].at[a - 1]

    def transpose(k, a, n, b):
        scale = (None, None, DOWN2, UP2)[a]
        columns_of(k, a)[n, pl.ds(HALO + b * B, B), :] = scaled(
            ns[k][a, pl.ds(n * B, B), pl.ds(b * B, B)].T, scale)

    for copy in loads[:edge_loads]:
        copy.wait()
    rows, _ = row_plan(levels)
    for k, a, b, at in rows:
        depth, h = depth_of(levels, k), levels[k][2]
        here = pl.ds(b * B, B)
        rows_out[0, pl.ds(at, depth), :] = ns[k][a, pl.ds(0, depth), here]
        rows_out[1, pl.ds(at, depth), :] = ns[k][a, pl.ds(h - depth, depth), here]
    group = iota(1) // 4
    arrays = [(k, a) for k in range(top + 1) for a in range(levels[k][0])]
    for d in range(4):
        step = DIRS[4 + d]
        packed = jnp.zeros((8, B), F32)
        for q, (k, a) in enumerate(arrays):
            _, blocks, h = levels[k]
            at = pl.ds(0 if step[0] < 0 else h - 8, 8)
            if step[1] < 0:
                packed = jnp.where(group == q, turn(ns[k][a, at, pl.ds(0, B)], 4 * q), packed)
            else:
                packed = jnp.where(
                    group == 31 - q, turn(ns[k][a, at, pl.ds((blocks - 1) * B, B)], -4 * q), packed)
        corners_out[d] = packed

    sends = []
    for d, step in enumerate(DIRS):
        if d < 2:
            src, dst = rows_out.at[d], rows_in.at[d]
        elif d < 4:
            src, dst = cols_out.at[d - 2], cols_in.at[d - 2]
        else:
            src, dst = corners_out.at[d - 4], corners_in.at[d - 4]
        sends.append(pltpu.make_async_remote_copy(
            src_ref=src, dst_ref=dst, send_sem=send_sem.at[d], recv_sem=recv_sem.at[d],
            device_id=neighbour(step), device_id_type=MESH))

    def enter():
        pl.semaphore_wait(barrier, len(DIRS))
        for d in (4, 5, 6, 7, 0, 1):
            sends[d].start()

    def enter_sides():
        sends[2].start()
        sends[3].start()

    def enter_all():
        enter()
        enter_sides()

    def every(*conditions):
        return functools.reduce(jnp.logical_and, conditions)

    def some(*conditions):
        return functools.reduce(jnp.logical_or, conditions)

    turned, near, odd = lax.rem(r, 4) < 1, c < 2, lax.rem(c, 2) >= 1
    first_row, last_row, last_column = r < 1, r >= nr - 1, c >= nc - 1
    straight, far, even = lax.rem(r, 4) >= 1, c >= 2, lax.rem(c, 2) < 1
    later_row, inner_row, inner_column = r >= 1, r < nr - 1, c < nc - 1
    fifth = every(first_row, near)
    fourth = some(
        every(first_row, far), every(later_row, turned, near),
        every(later_row, turned, odd, inner_column, far), every(straight, near, even, inner_row))
    third = some(
        every(later_row, turned, far, some(even, last_column)), every(straight, near, odd, inner_row))
    at_once = every(straight, far, some(even, last_column))
    second = jnp.logical_not(some(at_once, third, fourth, fifth))
    pl.when(at_once)(enter)

    for copy in loads[edge_loads : edge_loads + 2]:
        copy.wait()
    for k in range(top):
        for a in range(levels[k][0]):
            for n in range(row_blocks(levels[k])):
                for b in range(levels[k][1]):
                    transpose(k, a, n, b)
    for copy in loads[edge_loads + 2 : side_loads]:
        copy.wait()
    for a in range(3):
        for n in range(row_blocks(levels[top])):
            for b in (0, levels[top][1] - 1):
                transpose(top, a, n, b)
    columns, _ = column_plan(levels)
    for k, a, n, at in columns:
        depth, w = depth_of(levels, k), levels[k][1] * B
        cols_out[0, pl.ds(at, depth), :] = columns_of(k, a)[n, pl.ds(HALO, depth), :]
        cols_out[1, pl.ds(at, depth), :] = columns_of(k, a)[n, pl.ds(HALO + w - depth, depth), :]

    pl.when(at_once)(enter_sides)
    pl.when(second)(enter_all)

    def details(k):
        for n in range(row_blocks(levels[k])):
            lift_rows(levels[k][1] * B, xs[k].at[0, n], xs[k].at[1, n], ls[k].at[n])
            turn_back(levels[k], n, ls[k].at[n], ws[k], range(2 * levels[k][1]))

    def inner(k, count, s, r, dst):
        start = (-4, 4, 12, 28)[k]
        run = (count - 2 * start) // 8
        at = HALO + start
        lift_runs(run, s, at, r, at, dst.at[pl.ds(HALO + 2 * start, 16 * run), :])

    def chain_columns(k):
        _, blocks, h = levels[k]
        for n in range(row_blocks(levels[k])):
            if k > 0:
                for b in range(blocks):
                    ts[k][n, pl.ds(HALO + b * B, B), :] = lows[k][b, pl.ds(HALO + n * B, B), :].T * UP2
            inner(k, blocks * B, ts[k].at[n], zs[k].at[n], lifted.at[n])

    def chain_rows(k, these):
        h = levels[k][2]
        for j in these:
            for n in range(row_blocks(levels[k])):
                turn_back(levels[k], n, lifted.at[n], us[k], (j,))
            inner(k, h, us[k].at[j], ws[k].at[j], image.at[j] if k == top else lows[k + 1].at[j])

    for k in range(top):
        details(k)
    for k in range(top - 1):
        chain_columns(k)
        chain_rows(k, range(2 * levels[k][1]))
    pl.when(third)(enter_all)
    for copy in loads[side_loads:]:
        copy.wait()
    for a in range(3):
        for n in range(row_blocks(levels[top])):
            for b in range(1, levels[top][1] - 1):
                transpose(top, a, n, b)
    chain_columns(top - 1)
    chain_rows(top - 1, range(2 * levels[top - 1][1]))
    pl.when(fourth)(enter_all)

    details(top)
    chain_columns(top)
    blocks = levels[top][1]
    chain_rows(top, range(1, blocks))
    pl.when(fifth)(enter_all)

    for k, (_, blocks, h) in enumerate(levels):
        keep = strip_rows(k)
        for a in (0, 3) if k == 0 else (0,):
            for b in range(blocks):
                at = pl.ds(b * B, B)
                ds[at_of(levels, k, a, b), pl.ds(8, keep), :] = ns[k][a, pl.ds(0, keep), at]
                ds[at_of(levels, k, a, b), pl.ds(8 + keep, keep), :] = ns[k][a, pl.ds(h - keep, keep), at]

    sends[2].wait()
    sends[3].wait()
    for k, a, n, at in columns:
        depth, w = depth_of(levels, k), levels[k][1] * B
        columns_of(k, a)[n, pl.ds(HALO + w, depth), :] = cols_in[0, pl.ds(at, depth), :]
        columns_of(k, a)[n, pl.ds(HALO - depth, depth), :] = cols_in[1, pl.ds(at, depth), :]
    for k in (3, 2, 1, 0):
        blocks = levels[k][1]
        w = blocks * B
        for n in range(row_blocks(levels[k])):
            part = ls[k].at[n]
            for at in (HALO - 4, HALO + w - 4):
                lift_runs(1, xs[k].at[0, n], at, xs[k].at[1, n], at, ls[k].at[n, pl.ds(2 * at - HALO, 16), :])
            turn_back(levels[k], n, part, ws[k], (0, 2 * blocks - 1))
            if k < top:
                turn_back_side(levels[k], n, part, edge, ws[k])
            take, left, right = side_takes(levels, k)
            edge[pl.ds(0, take), :] = part[pl.ds(left, take), :]
            edge[pl.ds(take, take), :] = part[pl.ds(2 * w + 16 - right, take), :]
            count = min(B, levels[k][2])
            wcs[k][pl.ds(HALO + n * B, count), :] = edge[...].T[:count]

    chain_rows(top, (*range(levels[top][1], 2 * levels[top][1]), 0))

    for d in (0, 1):
        sends[d].wait()
    offsets = stack_offsets(levels)
    for k, a, b, at in rows:
        depth, base = depth_of(levels, k), offsets[k] + 8 * b
        hn[a, pl.ds(base, depth), :] = rows_in[0, pl.ds(at, depth), :]
        hn[a, pl.ds(base + 8 - depth, depth), :] = rows_in[1, pl.ds(at, depth), :]
    for d in (4, 5, 6, 7):
        sends[d].wait()
    low, bottom = iota(1) < 64, iota(0) < 4
    for q, (k, a) in enumerate(arrays):
        tile = jnp.where(
            bottom,
            jnp.where(low, turn(corners_in[0], -4 * q), turn(corners_in[1], 4 * q)),
            jnp.where(low, turn(corners_in[2], -4 * q), turn(corners_in[3], 4 * q)))
        cn[a, pl.ds(offsets[k], 8), :] = tile
        cn[a, pl.ds(offsets[k] + 8 * (levels[k][1] - 1), 8), :] = tile
    halo_transpose(levels, hn.at[1], cn.at[1], None, sh)
    halo_transpose(levels, hn.at[2], cn.at[2], DOWN2, rh)
    for k, a, b, at in rows:
        if a in (0, 3):
            depth, keep = depth_of(levels, k), strip_rows(k)
            strip = at_of(levels, k, a, b)
            ds[strip, pl.ds(8 + 2 * keep, depth), :] = rows_in[0, pl.ds(at, depth), :]
            ds[strip, pl.ds(8 - depth, depth), :] = rows_in[1, pl.ds(at, depth), :]
            (ct_out if a == 3 else zts[k])[pl.ds(HALO + b * B, B), :] = scaled(
                ds[strip].T, UP2 if a == 3 else None)
    side = cn[0].T
    for k in range(top + 1):
        strip_sides(levels, k, zs[k], side, zts[k])
    strip_sides(levels, 0, c4, cn[3].T * UP2, ct_out)
    lift_rows(B, sh, rh, hd)
    halo_back(levels, range(top + 1), hd, edge, ws)


def strip_kernel(levels, *refs):
    ws, zts, ct, image = refs[:4], refs[4:8], refs[8], refs[9]
    zs, c4, wcs = refs[10:14], refs[14], refs[15:19]
    out = refs[19]
    lows = (None,) + refs[20:23]
    sides = (None,) + refs[23:26]
    ends, us, lifted, edge, th, tc, sd, pair, uc, strip, merged, out_sem, end_sem = refs[26:]
    top = len(levels) - 1
    _, blocks, h = levels[top]
    rows = 2 * h
    cut = 64

    def main(j, start):
        at = pl.ds(cut, rows - 2 * cut)
        return pltpu.make_async_copy(
            image.at[j, pl.ds(HALO + cut, rows - 2 * cut), :], out.at[at, pl.ds(start, B)], out_sem.at[j])

    def flank(side):
        at = pl.ds(cut, rows - 2 * cut)
        start = (0, (2 * blocks - 1) * B)[side]
        return pltpu.make_async_copy(merged.at[side], out.at[at, pl.ds(start, B)],
                                     out_sem.at[(0, 2 * blocks - 1)[side]])

    def send(j, carry):
        main(j, pl.multiple_of(j * B, B)).start()
        return carry

    lax.fori_loop(1, 2 * blocks - 1, send, 0)

    for k, level in enumerate(levels):
        _, nb, h = level
        w = nb * B
        final = k == top
        keep = strip_rows(k)
        size = 2 * keep + 16
        if k == 0:
            t = ct
        else:
            t = th
            for b in range(nb):
                t[pl.ds(HALO + b * B, B), :] = lows[k][b].T * UP2
            side = lows[k][nb].T * UP2
            t[pl.ds(0, 8), :] = side[B - 8 :]
            t[pl.ds(HALO + w, 8), :] = side[:8]
        run = keep // 8
        take, left, right = side_takes(levels, k)
        for n in range(row_blocks(level)):
            if k == 0:
                side_t, second = c4.at[n], HALO + w + 4 - 8 * run
            else:
                tc[n] = sides[k][pl.ds(HALO + n * B, B), :].T * UP2
                side_t, second = tc.at[n], 8 + 2 * keep + 4 - 8 * run
            lift_runs(run, side_t, 4, zs[k].at[n], 4, sd.at[n, 0, pl.ds(0, 16 * run), :])
            lift_runs(run, side_t, second, zs[k].at[n], HALO + w + 4 - 8 * run, sd.at[n, 1, pl.ds(0, 16 * run), :])
            pair[n, pl.ds(0, take), :] = sd[n, 0, pl.ds(left, take), :]
            pair[n, pl.ds(take, take), :] = sd[n, 1, pl.ds(16 * run - right, take), :]
            count = min(B, h)
            uc[pl.ds(HALO + n * B, count), :] = pair[n].T[:count]
        lift_rows(h, uc, wcs[k], strip if final else sides[k + 1])
        if final:
            low = lax.broadcasted_iota(jnp.int32, (rows - 2 * cut, B), 1) < 64
            at = pl.ds(HALO + cut, rows - 2 * cut)
            merged[0] = jnp.where(low, strip[at, :], image[0, at, :])
            merged[1] = jnp.where(low, image[2 * nb - 1, at, :], strip[at, :])
            for side in range(2):
                flank(side).start()
        part = lifted.at[pl.ds(0, 2 * w + 16), :]
        lift_rows(w, t, zts[k], part)
        for j in range(2 * nb):
            us[j] = lifted[pl.ds(HALO + j * B, B), :].T
        if not final:
            edge[0:8, :] = lifted[pl.ds(HALO + 2 * w, 8), :]
            edge[B - 8 : B, :] = lifted[0:8, :]
            us[2 * nb] = edge[...].T
        run = keep // 8

        def strips(j, first, second, level=level, k=k):
            _, _, h = level
            keep = strip_rows(k)
            run = keep // 8
            lift_runs(run, us.at[j], 4, ws[k].at[j], 4, first)
            lift_runs(run, us.at[j], 8 + 2 * keep + 4 - 8 * run, ws[k].at[j], HALO + h + 4 - 8 * run, second)

        if not final:
            following = strip_rows(k + 1)
            made = 16 * run
            for j in range(2 * nb + 1):
                strips(j, ends.at[0, j, pl.ds(0, made), :], ends.at[1, j, pl.ds(0, made), :])
                lows[k + 1][j, pl.ds(0, 8 + following), :] = ends[0, j, pl.ds(0, 8 + following), :]
                lows[k + 1][j, pl.ds(8 + following, 8 + following), :] = ends[
                    1, j, pl.ds(made - 8 - following, 8 + following), :]
        else:
            made = 16 * run

            def end(j, side, start):
                row = (HALO, made - 8 - cut)[side]
                return pltpu.make_async_copy(
                    ends.at[side, j, pl.ds(row, cut), :],
                    out.at[pl.ds((0, rows - cut)[side], cut), pl.ds(start, B)], end_sem.at[side, j])

            def body(j, carry):
                strips(j, ends.at[0, j, pl.ds(0, made), :], ends.at[1, j, pl.ds(0, made), :])
                for side in range(2):
                    end(j, side, pl.multiple_of(j * B, B)).start()
                return carry

            lax.fori_loop(0, 2 * nb, body, 0)
            for j in range(2 * nb):
                if 0 < j < 2 * nb - 1:
                    main(j, j * B).wait()
                for side in range(2):
                    end(j, side, j * B).wait()
            for side in range(2):
                flank(side).wait()


def per_device(coarse, d4, d3, d2, d1):
    levels = []
    for k, x in enumerate((d4, d3, d2, d1)):
        levels.append((4 if k == 0 else 3, x.shape[2] // B, x.shape[1]))
    levels = tuple(levels)
    top = len(levels) - 1
    _, row_count = row_plan(levels)
    _, col_count = column_plan(levels)
    hbm = pl.BlockSpec(memory_space=pltpu.HBM)
    vmem = pl.BlockSpec(memory_space=pltpu.VMEM)
    wide = [2 * b + (0 if k == top else 1) for k, (_, b, _) in enumerate(levels)]
    across = [(row_blocks(l), l[1] * B + 2 * HALO, B) for l in levels]
    strips = [(n, l[2] + 2 * HALO, B) for n, l in zip(wide, levels)]
    stack = (B + 2 * HALO, B)
    blocks, h = levels[top][1], levels[top][2]
    mb = across[top][0]
    long = 2 * blocks * B + 2 * HALO
    tall = [(l[2] + 2 * HALO, B) for l in levels]
    between = pl.pallas_call(
        functools.partial(exchange_kernel, levels),
        out_shape=[pltpu.VMEM(s, F32) for s in (
            strips + [s[1:] for s in across] + [across[0][1:], (2 * blocks, 2 * h + 2 * HALO, B)]
            + across + [across[0]] + tall)],
        in_specs=[hbm] * 5,
        out_specs=[vmem] * 19,
        scratch_shapes=[
            *[pltpu.VMEM((a, max(B, h), b * B), F32) for a, b, h in levels],
            *[pltpu.VMEM((2,) + s, F32) for s in across],
            *[pltpu.VMEM((n, 2 * l[1] * B + 2 * HALO, B), F32) for (n, _, _), l in zip(across, levels)],
            *[pltpu.VMEM(s, F32) for s in strips],
            *[pltpu.VMEM((l[1], l[2] + 2 * HALO, B), F32) for l in levels[1:]],
            *[pltpu.VMEM(s, F32) for s in across[1:]],
            pltpu.VMEM((4, B, B), F32),
            pltpu.VMEM((4, B, B), F32),
            pltpu.VMEM(stack, F32),
            pltpu.VMEM(stack, F32),
            pltpu.VMEM((2 * B + 2 * HALO, B), F32),
            pltpu.VMEM((mb, long, B), F32),
            pltpu.VMEM((B, B), F32),
            pltpu.VMEM((1 + sum(l[1] for l in levels), B, B), F32),
            pltpu.VMEM((2, row_count, B), F32),
            pltpu.VMEM((2, col_count, B), F32),
            pltpu.VMEM((4, 8, B), F32),
            pltpu.VMEM((2, row_count, B), F32),
            pltpu.VMEM((2, col_count, B), F32),
            pltpu.VMEM((4, 8, B), F32),
            pltpu.SemaphoreType.DMA((15,)),
            pltpu.SemaphoreType.DMA((8,)),
            pltpu.SemaphoreType.DMA((8,)),
        ],
        compiler_params=pltpu.CompilerParams(
            collective_id=0, has_side_effects=True, vmem_limit_bytes=41 * 2**20),
    )(*[pltpu.with_memory_space_constraint(x, pltpu.HBM) for x in (coarse, d4, d3, d2, d1)])
    return pl.pallas_call(
        functools.partial(strip_kernel, levels),
        out_shape=jax.ShapeDtypeStruct((2 * h, 2 * blocks * B), F32),
        in_specs=[vmem] * 19,
        out_specs=pl.BlockSpec(memory_space=pl.ANY),
        scratch_shapes=[
            *[pltpu.VMEM((l[1] + 1, B, B), F32) for l in levels[1:]],
            *[pltpu.VMEM(s, F32) for s in tall[1:]],
            pltpu.VMEM((2, 2 * blocks, 16 * (strip_rows(top) // 8), B), F32),
            pltpu.VMEM((2 * blocks, B, B), F32),
            pltpu.VMEM((long, B), F32),
            pltpu.VMEM((B, B), F32),
            pltpu.VMEM(across[top][1:], F32),
            pltpu.VMEM((mb, B, B), F32),
            pltpu.VMEM((mb, 2, 16 * (strip_rows(top) // 8), B), F32),
            pltpu.VMEM((mb, B, B), F32),
            pltpu.VMEM(tall[top], F32),
            pltpu.VMEM((2 * h + 2 * HALO, B), F32),
            pltpu.VMEM((2, 2 * h - 128, B), F32),
            pltpu.SemaphoreType.DMA((2 * blocks,)),
            pltpu.SemaphoreType.DMA((2, 2 * blocks)),
        ],
        compiler_params=pltpu.CompilerParams(vmem_limit_bytes=14 * 2**20),
    )(*between)


def solution(mesh):
    return jax.shard_map(
        per_device,
        mesh=mesh,
        in_specs=(
            P("rows", "cols"),
            P(None, "rows", "cols"),
            P(None, "rows", "cols"),
            P(None, "rows", "cols"),
            P(None, "rows", "cols"),
        ),
        out_specs=P("rows", "cols"),
        check_vma=False,
    )
```

```python
import functools

import jax
import jax.numpy as jnp
from jax import lax
from jax.experimental import pallas as pl
from jax.experimental.pallas import tpu as pltpu
from jax.sharding import PartitionSpec as P

ALPHA = -1.586134342059924
BETA = -0.052980118572961
GAMMA = 0.882911075530934
DELTA = 0.443506852043971
SCALE = 1.149604398860241
UP2 = SCALE * SCALE
DOWN2 = 1.0 / (SCALE * SCALE)

B = 128
HALO = 8
F32 = jnp.float32
MESH = pl.DeviceIdType.MESH

DIRS = ((-1, 0), (1, 0), (0, -1), (0, 1), (-1, -1), (-1, 1), (1, -1), (1, 1))


def iota(axis):
    return lax.broadcasted_iota(jnp.int32, (8, B), axis)


def turn(x, amount):
    amount = amount % B
    return x if amount == 0 else pltpu.roll(x, amount, axis=1)


def row_blocks(level):
    return -(-level[2] // B)


def depth_of(levels, k):
    return 2 if k == len(levels) - 1 else 4


def row_depth(levels, k, a, d):
    back = len(levels) - 1 - k
    if d == 0:
        return (2, 3, 4, 4)[back]
    return (1, 2, 2, 2)[back] if a in (0, 3) else (2, 3, 3, 3)[back]


def row_plan(levels, d):
    plan, at = [], 0
    for k, (arrays, blocks, h) in enumerate(levels):
        for a in range(arrays):
            for b in range(blocks):
                depth = row_depth(levels, k, a, d)
                plan.append((k, a, b, at, depth))
                at += depth
    return plan, -(-at // 8) * 8


def column_plan(levels):
    plan, at = [], 0
    for k, level in enumerate(levels):
        for a in range(level[0]):
            for n in range(row_blocks(level)):
                plan.append((k, a, n, at))
                at += depth_of(levels, k)
    return plan, -(-at // 8) * 8


def stack_offsets(levels):
    offsets, at = [], 0
    for _, blocks, _ in levels:
        offsets.append(at)
        at += 8 * blocks
    return offsets


def lift_rows(count, s, r, dst):
    lift_runs((count + 8) // 8, s, HALO - 4, r, HALO - 4, dst)


def lift_runs(run, s, s_at, r, r_at, dst):
    def rows(ref, t):
        at = s_at if ref is s else r_at
        return ref[pl.ds(at + t, 8, stride=run), :]

    r0, s1, r1, s2 = {}, {}, {}, {}
    for t in range(-2, run + 2):
        r0[t] = rows(r, t)
        if t < -1:
            continue
        s1[t] = rows(s, t) - DELTA * (r0[t] + r0[t - 1])
        if t < 0:
            continue
        r1[t - 1] = r0[t - 1] - GAMMA * (s1[t - 1] + s1[t])
        if t < 1:
            continue
        n = t - 1
        s2[n] = s1[n] - BETA * (r1[n] + r1[n - 1])
        if n < run:
            dst[pl.ds(2 * n, 8, stride=2 * run), :] = s2[n]
        if n >= 1:
            dst[pl.ds(2 * n - 1, 8, stride=2 * run), :] = r1[n - 1] - ALPHA * (s2[n - 1] + s2[n])


def scaled(x, scale):
    return x if scale is None else x * scale


def turn_back(level, n, lifted, dst, which):
    count = min(B, level[2])
    at = pl.ds(HALO + n * B, count)
    for j in which:
        dst[j, at, :] = lifted[pl.ds(HALO + j * B, B), :].T[:count]


def turn_back_side(level, n, lifted, edge, dst):
    _, blocks, h = level
    count = min(B, h)
    edge[0:8, :] = lifted[pl.ds(HALO + 2 * blocks * B, 8), :]
    edge[B - 8 : B, :] = lifted[0:8, :]
    dst[2 * blocks, pl.ds(HALO + n * B, count), :] = edge[...].T[:count]


def halo_transpose(levels, hn, cn, scale, dst):
    group = iota(1) // 8
    offsets = stack_offsets(levels)
    first = last = None
    for off, (_, blocks, _) in zip(offsets, levels):
        f, l = group == off // 8, group == off // 8 + blocks - 1
        first = f if first is None else first | f
        last = l if last is None else last | l
    t = scaled(hn[...].T, scale)
    ct = scaled(cn[...].T, scale)
    dst[pl.ds(HALO, B), :] = t
    dst[pl.ds(0, 8), :] = jnp.where(first, ct[B - 8 :], turn(t[B - 8 :], 8))
    dst[pl.ds(HALO + B, 8), :] = jnp.where(last, ct[:8], turn(t[:8], -8))


def halo_back(levels, which, lifted, edge, dsts):
    low = iota(1) < 64
    offsets = stack_offsets(levels)
    for j in range(2):
        y = lifted[pl.ds(HALO + j * B, B), :].T
        for k in which:
            _, blocks, h = levels[k]
            for b in range(blocks):
                tile = y[offsets[k] + 8 * b : offsets[k] + 8 * b + 8]
                dsts[k][2 * b + j, pl.ds(0, 8), :] = tile
                dsts[k][2 * b + j, pl.ds(HALO + h, 8), :] = tile
    which = [k for k in which if k < len(levels) - 1]
    if which:
        edge[0:8, :] = lifted[pl.ds(HALO + 2 * B, 8), :]
        edge[B - 8 : B, :] = lifted[0:8, :]
        y = edge[...].T
        for k in which:
            _, blocks, h = levels[k]
            end = offsets[k] + 8 * (blocks - 1)
            tile = jnp.where(low, y[end : end + 8], y[offsets[k] : offsets[k] + 8])
            dsts[k][2 * blocks, pl.ds(0, 8), :] = tile
            dsts[k][2 * blocks, pl.ds(HALO + h, 8), :] = tile


def strip_rows(k):
    return (16, 16, 24, 40)[k]


def strip_sides(levels, k, main, ct, dst):
    _, blocks, h = levels[k]
    keep, off = strip_rows(k), stack_offsets(levels)[k]
    lane = iota(1)
    n = row_blocks(levels[k])
    start = h - keep - B * (n - 1)
    w = blocks * B
    for at, corner, shift in ((0, ct[B - 8 :], off), (HALO + w, ct[:8], off + 8 * (blocks - 1))):
        here = pl.ds(at, 8)
        dst[here, :] = jnp.where(
            lane < 8, turn(corner, -shift),
            jnp.where(
                lane < 8 + keep, turn(main[0, here, :], 8),
                jnp.where(lane < 8 + 2 * keep, turn(main[n - 1, here, :], 8 + keep - start),
                          turn(corner, 8 + 2 * keep - shift))))


def at_of(levels, k, a, b):
    return b if a == 3 else 1 + sum(l[1] for l in levels[:k]) + b


def side_takes(levels, k):
    if k == len(levels) - 1:
        return 64, 8, 72
    take = 8 + strip_rows(k + 1)
    return take, 0, take


def exchange_kernel(levels, *refs):
    coarse, d4, d3, d2, d1 = refs[:5]
    ws, zts, ct_out, image = refs[5:9], refs[9:13], refs[13], refs[14]
    zs, c4, wcs = refs[15:19], refs[19], refs[20:24]
    ns, xs, ls, us = refs[24:28], refs[28:32], refs[32:36], refs[36:40]
    lows, ts = (None,) + refs[40:43], (c4,) + refs[43:46]
    (hn, cn, sh, rh, hd, lifted, edge, ds, rows_out, cols_out, corners_out,
     rows_in, cols_in, corners_in, load_sem, send_sem, recv_sem) = refs[46:]
    nr, nc = lax.axis_size("rows"), lax.axis_size("cols")
    r, c = lax.axis_index("rows"), lax.axis_index("cols")
    top = len(levels) - 1

    def neighbour(step):
        return (lax.rem(r + step[0] + nr, nr), lax.rem(c + step[1] + nc, nc))

    barrier = pltpu.get_barrier_semaphore()
    for step in DIRS:
        pl.semaphore_signal(barrier, inc=1, device_id=neighbour(step), device_id_type=MESH)

    loads = []

    def load(src, dst):
        copy = pltpu.make_async_copy(src, dst, load_sem.at[len(loads)])
        copy.start()
        loads.append(copy)

    h = levels[0][2]
    load(coarse, ns[0].at[3, pl.ds(0, h), :])
    load(d4, ns[0].at[pl.ds(0, 3), pl.ds(0, h), :])
    for k, src in ((1, d3), (2, d2), (3, d1)):
        h = levels[k][2]
        for at in (pl.ds(0, 8), pl.ds(h - 8, 8)):
            load(src.at[:, at, :], ns[k].at[:, at, :])
    edge_loads = len(loads)
    for k, src in ((1, d3), (2, d2)):
        inner = pl.ds(8, levels[k][2] - 16)
        load(src.at[:, inner, :], ns[k].at[:, inner, :])
    _, blocks, h = levels[top]
    w = blocks * B
    inner = pl.ds(8, h - 16)
    for at in (pl.ds(0, B), pl.ds(w - B, B)):
        load(d1.at[:, inner, at], ns[top].at[:, inner, at])
    side_loads = len(loads)
    for a in range(3):
        at = pl.ds(B, w - 2 * B)
        load(d1.at[a, inner, at], ns[top].at[a, inner, at])

    def columns_of(k, a):
        return c4 if a == 3 else zs[k] if a == 0 else xs[k].at[a - 1]

    def transpose(k, a, n, b):
        scale = (None, None, DOWN2, UP2)[a]
        columns_of(k, a)[n, pl.ds(HALO + b * B, B), :] = scaled(
            ns[k][a, pl.ds(n * B, B), pl.ds(b * B, B)].T, scale)

    for copy in loads[:edge_loads]:
        copy.wait()
    for d in range(2):
        for k, a, b, at, depth in row_plan(levels, d)[0]:
            first = 0 if d == 0 else levels[k][2] - depth
            rows_out[d, pl.ds(at, depth), :] = ns[k][a, pl.ds(first, depth), pl.ds(b * B, B)]
    group = iota(1) // 4
    arrays = [(k, a) for k in range(top + 1) for a in range(levels[k][0])]
    for d in range(4):
        step = DIRS[4 + d]
        packed = jnp.zeros((8, B), F32)
        for q, (k, a) in enumerate(arrays):
            _, blocks, h = levels[k]
            at = pl.ds(0 if step[0] < 0 else h - 8, 8)
            if step[1] < 0:
                packed = jnp.where(group == q, turn(ns[k][a, at, pl.ds(0, B)], 4 * q), packed)
            else:
                packed = jnp.where(
                    group == 31 - q, turn(ns[k][a, at, pl.ds((blocks - 1) * B, B)], -4 * q), packed)
        corners_out[d] = packed

    sends = []
    for d, step in enumerate(DIRS):
        if d < 2:
            sent = pl.ds(0, row_plan(levels, d)[1])
            src, dst = rows_out.at[d, sent, :], rows_in.at[d, sent, :]
        elif d < 4:
            src, dst = cols_out.at[d - 2], cols_in.at[d - 2]
        else:
            src, dst = corners_out.at[d - 4], corners_in.at[d - 4]
        sends.append(pltpu.make_async_remote_copy(
            src_ref=src, dst_ref=dst, send_sem=send_sem.at[d], recv_sem=recv_sem.at[d],
            device_id=neighbour(step), device_id_type=MESH))

    def enter():
        pl.semaphore_wait(barrier, len(DIRS))
        for d in (4, 5, 6, 7, 0, 1):
            sends[d].start()

    def enter_sides():
        sends[2].start()
        sends[3].start()

    def enter_all():
        enter()
        enter_sides()

    def every(*conditions):
        return functools.reduce(jnp.logical_and, conditions)

    def some(*conditions):
        return functools.reduce(jnp.logical_or, conditions)

    turned, near, odd = lax.rem(r, 4) < 1, c < 2, lax.rem(c, 2) >= 1
    first_row, last_row, last_column = r < 1, r >= nr - 1, c >= nc - 1
    straight, far, even = lax.rem(r, 4) >= 1, c >= 2, lax.rem(c, 2) < 1
    later_row, inner_row, inner_column = r >= 1, r < nr - 1, c < nc - 1
    fifth = every(first_row, near)
    fourth = some(
        every(first_row, far), every(later_row, turned, near),
        every(later_row, turned, odd, inner_column, far), every(straight, near, even, inner_row))
    third = some(
        every(later_row, turned, far, some(even, last_column)), every(straight, near, odd, inner_row))
    at_once = every(straight, far, some(even, last_column))
    second = jnp.logical_not(some(at_once, third, fourth, fifth))
    pl.when(at_once)(enter)

    for copy in loads[edge_loads : edge_loads + 2]:
        copy.wait()
    for k in range(top):
        for a in range(levels[k][0]):
            for n in range(row_blocks(levels[k])):
                for b in range(levels[k][1]):
                    transpose(k, a, n, b)
    for copy in loads[edge_loads + 2 : side_loads]:
        copy.wait()
    for a in range(3):
        for n in range(row_blocks(levels[top])):
            for b in (0, levels[top][1] - 1):
                transpose(top, a, n, b)
    columns, _ = column_plan(levels)
    for k, a, n, at in columns:
        depth, w = depth_of(levels, k), levels[k][1] * B
        cols_out[0, pl.ds(at, depth), :] = columns_of(k, a)[n, pl.ds(HALO, depth), :]
        cols_out[1, pl.ds(at, depth), :] = columns_of(k, a)[n, pl.ds(HALO + w - depth, depth), :]

    pl.when(at_once)(enter_sides)
    pl.when(second)(enter_all)

    def details(k):
        for n in range(row_blocks(levels[k])):
            lift_rows(levels[k][1] * B, xs[k].at[0, n], xs[k].at[1, n], ls[k].at[n])
            turn_back(levels[k], n, ls[k].at[n], ws[k], range(2 * levels[k][1]))

    def inner(k, count, s, r, dst):
        start = (-4, 4, 12, 28)[k]
        run = (count - 2 * start) // 8
        at = HALO + start
        lift_runs(run, s, at, r, at, dst.at[pl.ds(HALO + 2 * start, 16 * run), :])

    def chain_columns(k):
        _, blocks, h = levels[k]
        for n in range(row_blocks(levels[k])):
            if k > 0:
                for b in range(blocks):
                    ts[k][n, pl.ds(HALO + b * B, B), :] = lows[k][b, pl.ds(HALO + n * B, B), :].T * UP2
            inner(k, blocks * B, ts[k].at[n], zs[k].at[n], lifted.at[n])

    def chain_rows(k, these):
        h = levels[k][2]
        for j in these:
            for n in range(row_blocks(levels[k])):
                turn_back(levels[k], n, lifted.at[n], us[k], (j,))
            inner(k, h, us[k].at[j], ws[k].at[j], image.at[j] if k == top else lows[k + 1].at[j])

    for k in range(top):
        details(k)
    for k in range(top - 1):
        chain_columns(k)
        chain_rows(k, range(2 * levels[k][1]))
    pl.when(third)(enter_all)
    for copy in loads[side_loads:]:
        copy.wait()
    for a in range(3):
        for n in range(row_blocks(levels[top])):
            for b in range(1, levels[top][1] - 1):
                transpose(top, a, n, b)
    chain_columns(top - 1)
    chain_rows(top - 1, range(2 * levels[top - 1][1]))
    pl.when(fourth)(enter_all)

    details(top)
    chain_columns(top)
    blocks = levels[top][1]
    chain_rows(top, range(1, blocks))
    pl.when(fifth)(enter_all)

    for k, (_, blocks, h) in enumerate(levels):
        keep = strip_rows(k)
        for a in (0, 3) if k == 0 else (0,):
            for b in range(blocks):
                at = pl.ds(b * B, B)
                ds[at_of(levels, k, a, b), pl.ds(8, keep), :] = ns[k][a, pl.ds(0, keep), at]
                ds[at_of(levels, k, a, b), pl.ds(8 + keep, keep), :] = ns[k][a, pl.ds(h - keep, keep), at]

    sends[2].wait()
    sends[3].wait()
    for k, a, n, at in columns:
        depth, w = depth_of(levels, k), levels[k][1] * B
        columns_of(k, a)[n, pl.ds(HALO + w, depth), :] = cols_in[0, pl.ds(at, depth), :]
        columns_of(k, a)[n, pl.ds(HALO - depth, depth), :] = cols_in[1, pl.ds(at, depth), :]
    for k in (3, 2, 1, 0):
        blocks = levels[k][1]
        w = blocks * B
        for n in range(row_blocks(levels[k])):
            part = ls[k].at[n]
            for at in (HALO - 4, HALO + w - 4):
                lift_runs(1, xs[k].at[0, n], at, xs[k].at[1, n], at, ls[k].at[n, pl.ds(2 * at - HALO, 16), :])
            turn_back(levels[k], n, part, ws[k], (0, 2 * blocks - 1))
            if k < top:
                turn_back_side(levels[k], n, part, edge, ws[k])
            take, left, right = side_takes(levels, k)
            edge[pl.ds(0, take), :] = part[pl.ds(left, take), :]
            edge[pl.ds(take, take), :] = part[pl.ds(2 * w + 16 - right, take), :]
            count = min(B, levels[k][2])
            wcs[k][pl.ds(HALO + n * B, count), :] = edge[...].T[:count]

    chain_rows(top, (*range(levels[top][1], 2 * levels[top][1]), 0))

    for d in (0, 1):
        sends[d].wait()
    offsets = stack_offsets(levels)
    for d in range(2):
        for k, a, b, at, depth in row_plan(levels, d)[0]:
            incoming = rows_in[d, pl.ds(at, depth), :]
            if a in (0, 3):
                first = 8 + 2 * strip_rows(k) if d == 0 else 8 - depth
                ds[at_of(levels, k, a, b), pl.ds(first, depth), :] = incoming
            else:
                first = offsets[k] + 8 * b + (0 if d == 0 else 8 - depth)
                hn[a, pl.ds(first, depth), :] = incoming
    for d in (4, 5, 6, 7):
        sends[d].wait()
    low, bottom = iota(1) < 64, iota(0) < 4
    for q, (k, a) in enumerate(arrays):
        tile = jnp.where(
            bottom,
            jnp.where(low, turn(corners_in[0], -4 * q), turn(corners_in[1], 4 * q)),
            jnp.where(low, turn(corners_in[2], -4 * q), turn(corners_in[3], 4 * q)))
        cn[a, pl.ds(offsets[k], 8), :] = tile
        cn[a, pl.ds(offsets[k] + 8 * (levels[k][1] - 1), 8), :] = tile
    halo_transpose(levels, hn.at[1], cn.at[1], None, sh)
    halo_transpose(levels, hn.at[2], cn.at[2], DOWN2, rh)
    for k in range(top + 1):
        for a in (0, 3) if k == 0 else (0,):
            for b in range(levels[k][1]):
                (ct_out if a == 3 else zts[k])[pl.ds(HALO + b * B, B), :] = scaled(
                    ds[at_of(levels, k, a, b)].T, UP2 if a == 3 else None)
    side = cn[0].T
    for k in range(top + 1):
        strip_sides(levels, k, zs[k], side, zts[k])
    strip_sides(levels, 0, c4, cn[3].T * UP2, ct_out)
    lift_rows(B, sh, rh, hd)
    halo_back(levels, range(top + 1), hd, edge, ws)


def strip_kernel(levels, *refs):
    ws, zts, ct, image = refs[:4], refs[4:8], refs[8], refs[9]
    zs, c4, wcs = refs[10:14], refs[14], refs[15:19]
    out = refs[19]
    lows = (None,) + refs[20:23]
    sides = (None,) + refs[23:26]
    ends, us, lifted, edge, th, tc, sd, pair, uc, strip, merged, out_sem, end_sem = refs[26:]
    top = len(levels) - 1
    _, blocks, h = levels[top]
    rows = 2 * h
    cut = 64

    def main(j, start):
        at = pl.ds(cut, rows - 2 * cut)
        return pltpu.make_async_copy(
            image.at[j, pl.ds(HALO + cut, rows - 2 * cut), :], out.at[at, pl.ds(start, B)], out_sem.at[j])

    def flank(side):
        at = pl.ds(cut, rows - 2 * cut)
        start = (0, (2 * blocks - 1) * B)[side]
        return pltpu.make_async_copy(merged.at[side], out.at[at, pl.ds(start, B)],
                                     out_sem.at[(0, 2 * blocks - 1)[side]])

    def send(j, carry):
        main(j, pl.multiple_of(j * B, B)).start()
        return carry

    lax.fori_loop(1, 2 * blocks - 1, send, 0)

    for k, level in enumerate(levels):
        _, nb, h = level
        w = nb * B
        final = k == top
        keep = strip_rows(k)
        size = 2 * keep + 16
        if k == 0:
            t = ct
        else:
            t = th
            for b in range(nb):
                t[pl.ds(HALO + b * B, B), :] = lows[k][b].T * UP2
            side = lows[k][nb].T * UP2
            t[pl.ds(0, 8), :] = side[B - 8 :]
            t[pl.ds(HALO + w, 8), :] = side[:8]
        run = keep // 8
        take, left, right = side_takes(levels, k)
        for n in range(row_blocks(level)):
            if k == 0:
                side_t, second = c4.at[n], HALO + w + 4 - 8 * run
            else:
                tc[n] = sides[k][pl.ds(HALO + n * B, B), :].T * UP2
                side_t, second = tc.at[n], 8 + 2 * keep + 4 - 8 * run
            lift_runs(run, side_t, 4, zs[k].at[n], 4, sd.at[n, 0, pl.ds(0, 16 * run), :])
            lift_runs(run, side_t, second, zs[k].at[n], HALO + w + 4 - 8 * run, sd.at[n, 1, pl.ds(0, 16 * run), :])
            pair[n, pl.ds(0, take), :] = sd[n, 0, pl.ds(left, take), :]
            pair[n, pl.ds(take, take), :] = sd[n, 1, pl.ds(16 * run - right, take), :]
            count = min(B, h)
            uc[pl.ds(HALO + n * B, count), :] = pair[n].T[:count]
        lift_rows(h, uc, wcs[k], strip if final else sides[k + 1])
        if final:
            low = lax.broadcasted_iota(jnp.int32, (rows - 2 * cut, B), 1) < 64
            at = pl.ds(HALO + cut, rows - 2 * cut)
            merged[0] = jnp.where(low, strip[at, :], image[0, at, :])
            merged[1] = jnp.where(low, image[2 * nb - 1, at, :], strip[at, :])
            for side in range(2):
                flank(side).start()
        part = lifted.at[pl.ds(0, 2 * w + 16), :]
        lift_rows(w, t, zts[k], part)
        for j in range(2 * nb):
            us[j] = lifted[pl.ds(HALO + j * B, B), :].T
        if not final:
            edge[0:8, :] = lifted[pl.ds(HALO + 2 * w, 8), :]
            edge[B - 8 : B, :] = lifted[0:8, :]
            us[2 * nb] = edge[...].T
        run = keep // 8

        def strips(j, first, second, level=level, k=k):
            _, _, h = level
            keep = strip_rows(k)
            run = keep // 8
            lift_runs(run, us.at[j], 4, ws[k].at[j], 4, first)
            lift_runs(run, us.at[j], 8 + 2 * keep + 4 - 8 * run, ws[k].at[j], HALO + h + 4 - 8 * run, second)

        if not final:
            following = strip_rows(k + 1)
            made = 16 * run
            for j in range(2 * nb + 1):
                strips(j, ends.at[0, j, pl.ds(0, made), :], ends.at[1, j, pl.ds(0, made), :])
                lows[k + 1][j, pl.ds(0, 8 + following), :] = ends[0, j, pl.ds(0, 8 + following), :]
                lows[k + 1][j, pl.ds(8 + following, 8 + following), :] = ends[
                    1, j, pl.ds(made - 8 - following, 8 + following), :]
        else:
            made = 16 * run

            def end(j, side, start):
                row = (HALO, made - 8 - cut)[side]
                return pltpu.make_async_copy(
                    ends.at[side, j, pl.ds(row, cut), :],
                    out.at[pl.ds((0, rows - cut)[side], cut), pl.ds(start, B)], end_sem.at[side, j])

            def body(j, carry):
                strips(j, ends.at[0, j, pl.ds(0, made), :], ends.at[1, j, pl.ds(0, made), :])
                for side in range(2):
                    end(j, side, pl.multiple_of(j * B, B)).start()
                return carry

            lax.fori_loop(0, 2 * nb, body, 0)
            for j in range(2 * nb):
                if 0 < j < 2 * nb - 1:
                    main(j, j * B).wait()
                for side in range(2):
                    end(j, side, j * B).wait()
            for side in range(2):
                flank(side).wait()


def per_device(coarse, d4, d3, d2, d1):
    levels = []
    for k, x in enumerate((d4, d3, d2, d1)):
        levels.append((4 if k == 0 else 3, x.shape[2] // B, x.shape[1]))
    levels = tuple(levels)
    top = len(levels) - 1
    row_count = max(row_plan(levels, d)[1] for d in range(2))
    _, col_count = column_plan(levels)
    hbm = pl.BlockSpec(memory_space=pltpu.HBM)
    vmem = pl.BlockSpec(memory_space=pltpu.VMEM)
    wide = [2 * b + (0 if k == top else 1) for k, (_, b, _) in enumerate(levels)]
    across = [(row_blocks(l), l[1] * B + 2 * HALO, B) for l in levels]
    strips = [(n, l[2] + 2 * HALO, B) for n, l in zip(wide, levels)]
    stack = (B + 2 * HALO, B)
    blocks, h = levels[top][1], levels[top][2]
    mb = across[top][0]
    long = 2 * blocks * B + 2 * HALO
    tall = [(l[2] + 2 * HALO, B) for l in levels]
    between = pl.pallas_call(
        functools.partial(exchange_kernel, levels),
        out_shape=[pltpu.VMEM(s, F32) for s in (
            strips + [s[1:] for s in across] + [across[0][1:], (2 * blocks, 2 * h + 2 * HALO, B)]
            + across + [across[0]] + tall)],
        in_specs=[hbm] * 5,
        out_specs=[vmem] * 19,
        scratch_shapes=[
            *[pltpu.VMEM((a, max(B, h), b * B), F32) for a, b, h in levels],
            *[pltpu.VMEM((2,) + s, F32) for s in across],
            *[pltpu.VMEM((n, 2 * l[1] * B + 2 * HALO, B), F32) for (n, _, _), l in zip(across, levels)],
            *[pltpu.VMEM(s, F32) for s in strips],
            *[pltpu.VMEM((l[1], l[2] + 2 * HALO, B), F32) for l in levels[1:]],
            *[pltpu.VMEM(s, F32) for s in across[1:]],
            pltpu.VMEM((4, B, B), F32),
            pltpu.VMEM((4, B, B), F32),
            pltpu.VMEM(stack, F32),
            pltpu.VMEM(stack, F32),
            pltpu.VMEM((2 * B + 2 * HALO, B), F32),
            pltpu.VMEM((mb, long, B), F32),
            pltpu.VMEM((B, B), F32),
            pltpu.VMEM((1 + sum(l[1] for l in levels), B, B), F32),
            pltpu.VMEM((2, row_count, B), F32),
            pltpu.VMEM((2, col_count, B), F32),
            pltpu.VMEM((4, 8, B), F32),
            pltpu.VMEM((2, row_count, B), F32),
            pltpu.VMEM((2, col_count, B), F32),
            pltpu.VMEM((4, 8, B), F32),
            pltpu.SemaphoreType.DMA((15,)),
            pltpu.SemaphoreType.DMA((8,)),
            pltpu.SemaphoreType.DMA((8,)),
        ],
        compiler_params=pltpu.CompilerParams(
            collective_id=0, has_side_effects=True, vmem_limit_bytes=41 * 2**20),
    )(*[pltpu.with_memory_space_constraint(x, pltpu.HBM) for x in (coarse, d4, d3, d2, d1)])
    return pl.pallas_call(
        functools.partial(strip_kernel, levels),
        out_shape=jax.ShapeDtypeStruct((2 * h, 2 * blocks * B), F32),
        in_specs=[vmem] * 19,
        out_specs=pl.BlockSpec(memory_space=pl.ANY),
        scratch_shapes=[
            *[pltpu.VMEM((l[1] + 1, B, B), F32) for l in levels[1:]],
            *[pltpu.VMEM(s, F32) for s in tall[1:]],
            pltpu.VMEM((2, 2 * blocks, 16 * (strip_rows(top) // 8), B), F32),
            pltpu.VMEM((2 * blocks, B, B), F32),
            pltpu.VMEM((long, B), F32),
            pltpu.VMEM((B, B), F32),
            pltpu.VMEM(across[top][1:], F32),
            pltpu.VMEM((mb, B, B), F32),
            pltpu.VMEM((mb, 2, 16 * (strip_rows(top) // 8), B), F32),
            pltpu.VMEM((mb, B, B), F32),
            pltpu.VMEM(tall[top], F32),
            pltpu.VMEM((2 * h + 2 * HALO, B), F32),
            pltpu.VMEM((2, 2 * h - 128, B), F32),
            pltpu.SemaphoreType.DMA((2 * blocks,)),
            pltpu.SemaphoreType.DMA((2, 2 * blocks)),
        ],
        compiler_params=pltpu.CompilerParams(vmem_limit_bytes=14 * 2**20),
    )(*between)


def solution(mesh):
    return jax.shard_map(
        per_device,
        mesh=mesh,
        in_specs=(
            P("rows", "cols"),
            P(None, "rows", "cols"),
            P(None, "rows", "cols"),
            P(None, "rows", "cols"),
            P(None, "rows", "cols"),
        ),
        out_specs=P("rows", "cols"),
        check_vma=False,
    )
```
